128 devices in a mesh: seq: 32 (over x, y_lo, z), dp: 4 (over y_hi, core).
Axes of the slice: x: 4, y: 4 (y_hi: 2, y_lo: 2; y = y_hi * 2 + y_lo), z: 4, core: 2. Of those that a mesh axis runs over, the one named last changes fastest.
Arguments:
- conv_input: bfloat16 [4, 8192, 2816], P('dp', 'seq'), may hold values from -6 to 6
- gate_input: bfloat16 [4, 8192, 2560], P('dp', 'seq'), may hold values from -6 to 6
- step_input: float32 [4, 40, 8192], P('dp', None, 'seq'), may hold values from -7.5 to 8192
- filter_taps: float32 [4, 2816], replicated, may hold values from -3 to 3
- filter_bias: float32 [2816], replicated, may hold values from -0.5 to 0.5
- step_bias: float32 [40], replicated, may hold values from -1 to 1
- decay_log: float32 [40], replicated, may hold values from -13 to 3
- skip_gain: float32 [40], replicated, may hold values from 0.5 to 1.5
- norm_weight: float32 [2560], replicated, may hold values from 0.5 to 1.5
- output_weight: bfloat16 [2560, 1280], P('dp'), may hold values from -0.125 to 0.125
- output_grad: bfloat16 [4, 8192, 1280], P('dp', 'seq'), may hold values from -6 to 6
Outputs:
- input_grad: bfloat16 [4, 8192, 2816], P('dp', 'seq')
- gate_grad: bfloat16 [4, 8192, 2560], P('dp', 'seq')
- step_grad: float32 [4, 40, 8192], P('dp', None, 'seq')
- weight_grad: float32 [2560, 1280], P('dp')
- filter_grads: float32 [5, 2816], replicated
- norm_grad: float32 [2560], replicated
- head_grads: float32 [3, 40], replicated
The draws below stay inside these ranges and needn't reach their ends.
All inputs are finite; a program needn't handle non-finite values.
Results may differ from the reference program's by a relative error of at most 0.0029.
Values may be sent and summed in bfloat16 or wider, within the bound.
A program may use at most 192 MiB of HBM per device.

```python
import jax
import jax.numpy as jnp
from jax import lax

HEADS = 40
HEAD_DIM = 64
STATE = 128
WIDTH = 1280
SPAN = 256
KERNEL = 4
TOKENS_DEV = 256
INNER = 2560
CHANNELS = 2816
SEQ_LEN = 8192
BATCH = 4


def head_rates(key):
    folded = jax.random.fold_in(key, 4099)
    slow_key, fast_key, pick_key = jax.random.split(folded, 3)
    slow_rate = jax.random.uniform(slow_key, (HEADS,), jnp.float32, 10.0, 30.0) / (0.03 * SEQ_LEN)
    fast_rate = 1.0 / (0.03 * jax.random.uniform(fast_key, (HEADS,), jnp.float32, 30.0, 50.0))
    share = 0.5
    chosen = jax.random.uniform(pick_key, (HEADS,), jnp.float32) < share
    return jnp.where(chosen, fast_rate, slow_rate)


def draw_decay_log(key, part):
    return jnp.log(head_rates(key))


def draw_step_input(key, part):
    rates = head_rates(key)
    folded = jax.random.fold_in(key, 8191)
    noise_key, block_key, place_key, loss_key = jax.random.split(folded, 4)
    noise = jax.random.uniform(noise_key, (BATCH, HEADS, SEQ_LEN), jnp.float32, -5.5, -2.5)
    levels = jax.random.uniform(block_key, (BATCH, HEADS, SEQ_LEN // TOKENS_DEV, 1), jnp.float32, -1.0, 1.0)
    spread = jnp.broadcast_to(levels, (BATCH, HEADS, SEQ_LEN // TOKENS_DEV, TOKENS_DEV)).reshape(BATCH, HEADS, SEQ_LEN)
    places = jax.random.randint(place_key, (BATCH, 2), 0, SEQ_LEN)
    marked = jnp.any(jnp.arange(SEQ_LEN)[None, None, :] == places[:, :, None], axis=1)
    losses = jax.random.uniform(loss_key, (BATCH, HEADS, 1), jnp.float32, 0.2, 0.45)
    jumps = -jnp.log(1.0 - losses) / rates[None, :, None]
    return jnp.where(marked[:, None, :], jumps, noise + spread)


def block_levels(rng, extent, cuts, least, high):
    loudness = 1.0
    for dim, parts in cuts:
        draws = jax.random.uniform(jax.random.fold_in(jax.random.fold_in(rng, 6), dim), (parts,), jnp.float32, least / len(cuts), high / len(cuts))
        loudness = loudness * jnp.repeat(jnp.exp(draws), extent[dim] // parts).reshape((-1,) + (1,) * (len(extent) - 1 - dim))
    return loudness


def scatter_about(stream_key, shape, scale, limit, cuts=(), kind=jnp.bfloat16):
    loudness = block_levels(stream_key, shape, cuts, -0.22, 0.18) if cuts else 1.0
    values = jax.random.normal(stream_key, shape, jnp.float32) * scale * loudness
    return jnp.minimum(jnp.maximum(values, -limit), limit).astype(kind)


def setup_inputs(seed: int = 0) -> dict:
    streams_of = jax.random.split(jax.random.key(seed), 12)
    return {
        "conv_input": scatter_about(streams_of[0], (BATCH, SEQ_LEN, CHANNELS), 1.0, 6.0, ((0, 4), (1, 32))),
        "gate_input": scatter_about(streams_of[1], (BATCH, SEQ_LEN, INNER), 1.0, 6.0, ((0, 4), (1, 32))),
        "step_input": draw_step_input(jax.random.fold_in(streams_of[11], 71), 0),
        "filter_taps": scatter_about(streams_of[3], (KERNEL, CHANNELS), KERNEL ** -0.5, 3.0, (), jnp.float32),
        "filter_bias": jnp.clip(jax.random.uniform(streams_of[4], (CHANNELS,), jnp.float32, -0.5, 0.5), -0.5, 0.5),
        "step_bias": jnp.clip(jax.random.uniform(streams_of[5], (HEADS,), jnp.float32, -1.0, 1.0), -1.0, 1.0),
        "decay_log": draw_decay_log(jax.random.fold_in(streams_of[11], 71), 0),
        "skip_gain": jnp.clip(jax.random.uniform(streams_of[7], (HEADS,), jnp.float32, 0.5, 1.5), 0.5, 1.5),
        "norm_weight": jnp.clip(1.0 + 0.1 * jax.random.normal(streams_of[8], (INNER,), jnp.float32), 0.5, 1.5),
        "output_weight": scatter_about(streams_of[9], (INNER, WIDTH), INNER ** -0.5, 0.125, ((0, 4),)),
        "output_grad": scatter_about(streams_of[10], (BATCH, SEQ_LEN, WIDTH), 1.0, 6.0, ((0, 4), (1, 32))),
    }


HIGHEST = lax.Precision.HIGHEST
MASKED = -1e+30
EPSILON = 1e-05

def block_step(skip_gain, carried, slices):
    activated, block_steps, block_rates = slices
    length = activated.shape[0]
    values = activated[:, :INNER].reshape(length, HEADS, HEAD_DIM)
    key_side = activated[:, INNER:INNER + STATE]
    query_side = activated[:, INNER + STATE:]
    cumsums = jnp.cumsum(block_rates, axis=1)
    scaled = values * block_steps.T[:, :, None]
    to_end = jnp.exp(cumsums[:, -1:] - cumsums)
    block_state = jnp.einsum('hs,shp,sn->hpn', to_end, scaled, key_side, precision=HIGHEST)
    scores = jnp.einsum('tn,sn->ts', query_side, key_side, precision=HIGHEST)
    differences = cumsums[:, :, None] - cumsums[:, None, :]
    causal = jnp.tril(jnp.ones((length, length), dtype=bool))
    weights = scores[None] * jnp.exp(jnp.where(causal[None], differences, MASKED))
    inside = jnp.einsum('hts,shp->thp', weights, scaled, precision=HIGHEST)
    from_state = jnp.einsum('tn,hpn->thp', query_side, carried, precision=HIGHEST) * jnp.exp(cumsums).T[:, :, None]
    result = inside + from_state + skip_gain[:, None] * values
    updated = jnp.exp(cumsums[:, -1])[:, None, None] * carried + block_state
    return (updated, result.reshape(length, INNER))

def layer_forward(raw_rows, gate_rows, step_rows, filter_taps, filter_bias, step_bias, decay_log, skip_gain, norm_weight):
    length = raw_rows.shape[0]
    padded = jnp.concatenate([jnp.zeros((KERNEL - 1, CHANNELS), jnp.float32), raw_rows], axis=0)
    filtered = filter_bias + filter_taps[0] * padded[0:length]
    for offset in range(1, KERNEL):
        filtered = filtered + filter_taps[offset] * padded[offset:offset + length]
    activated = jax.nn.silu(filtered)
    step_sizes = jax.nn.softplus(step_rows + step_bias[:, None])
    decay_rates = step_sizes * (-jnp.exp(decay_log))[:, None]
    blocks = length // SPAN
    pieces = (activated.reshape(blocks, SPAN, CHANNELS), step_sizes.reshape(HEADS, blocks, SPAN).transpose(1, 0, 2), decay_rates.reshape(HEADS, blocks, SPAN).transpose(1, 0, 2))
    stepper = jax.checkpoint(lambda carried, slices: block_step(skip_gain, carried, slices))
    _, outputs = lax.scan(stepper, jnp.zeros((HEADS, HEAD_DIM, STATE), jnp.float32), pieces)
    scanned = outputs.reshape(length, INNER)
    gated = scanned * jax.nn.silu(gate_rows)
    inverse_rms = lax.rsqrt(lax.optimization_barrier(jnp.mean(gated * gated, axis=1, keepdims=True)) + EPSILON)
    return gated * inverse_rms * norm_weight

def reference(conv_input, gate_input, step_input, filter_taps, filter_bias, step_bias, decay_log, skip_gain, norm_weight, output_weight, output_grad):

    def one_sequence(slices):
        raw_rows, gate_rows, step_rows, cotangent = slices
        normed, pullback = jax.vjp(layer_forward, raw_rows.astype(jnp.float32), gate_rows.astype(jnp.float32), step_rows, filter_taps, filter_bias, step_bias, decay_log, skip_gain, norm_weight)
        normed_low = normed.astype(jnp.bfloat16)
        normed_grad = jnp.dot(cotangent, output_weight.T, preferred_element_type=jnp.float32)
        weight_term = jnp.dot(normed_low.T, cotangent, preferred_element_type=jnp.float32)
        return tuple(pullback(normed_grad)) + (weight_term,)
    results = lax.map(one_sequence, (conv_input, gate_input, step_input, output_grad))
    input_grad = results[0].astype(jnp.bfloat16)
    gate_grad = results[1].astype(jnp.bfloat16)
    step_grad = results[2]
    filter_grads = jnp.concatenate([lax.optimization_barrier(jnp.sum(results[3], axis=0)), lax.optimization_barrier(jnp.sum(results[4], axis=0))[None]], axis=0)
    head_grads = jnp.stack([lax.optimization_barrier(jnp.sum(results[5], axis=0)), lax.optimization_barrier(jnp.sum(results[6], axis=0)), lax.optimization_barrier(jnp.sum(results[7], axis=0))])
    norm_grad = lax.optimization_barrier(jnp.sum(results[8], axis=0))
    weight_grad = lax.optimization_barrier(jnp.sum(results[9], axis=0))
    return (input_grad, gate_grad, step_grad, weight_grad, filter_grads, norm_grad, head_grads)
```

```python
import functools

import jax
import jax.numpy as jnp
from jax import lax
from jax.experimental import pallas as pl
from jax.experimental.pallas import tpu as pltpu
from jax.sharding import PartitionSpec as P

HEADS = 40
HEAD_DIM = 64
STATE = 128
INNER = 2560
CHANNELS = 2816
WIDTH = 1280
TOKENS = 256
TAPS = 4
PAIRS = 20
HALF = 1280
CHUNK = HALF + 128
SEQ = 32
DP = 4
ROWS = INNER // DP
PIECE = 208
MASKED = -1e30
EPSILON = 1e-05

F32 = jnp.float32
BF16 = jnp.bfloat16
MESH = pl.DeviceIdType.MESH
NN = ((1,), (0,))
NT = ((1,), (1,))
TN = ((0,), (0,))


def mm(a, b, dims):
    return lax.dot_general(a, b, (dims, ((), ())), preferred_element_type=F32)


def split(x):
    high = x.astype(BF16)
    return high, (x - high.astype(F32)).astype(BF16)


def dot3(a, b, dims):
    return mm(a[0], b[0], dims) + mm(a[0], b[1], dims) + mm(a[1], b[0], dims)


def iota(shape, dim):
    return lax.broadcasted_iota(jnp.int32, shape, dim)


def lanes(p):
    return pl.ds(pl.multiple_of(p * 128, 128), 128)


def rates_of(step_ref, bias_ref, log_ref):
    raw = step_ref[...] + bias_ref[...]
    sizes = jnp.maximum(raw, 0.0) + jnp.log1p(jnp.exp(-jnp.abs(raw)))
    gain = -jnp.exp(log_ref[...])
    rates = sizes * gain
    lane = iota(rates.shape, 1)
    cums = rates
    shift = 1
    while shift < TOKENS:
        cums = cums + jnp.where(lane >= shift, pltpu.roll(cums, shift, 1), 0.0)
        shift *= 2
    return raw, sizes, gain, rates, cums


def turned(x):
    return jnp.transpose(jnp.concatenate([x, jnp.zeros((128 - HEADS, TOKENS), F32)], axis=0))


def widen(columns, p):
    first = iota((TOKENS, 128), 1) < HEAD_DIM
    return jnp.where(first, columns[:, 2 * p : 2 * p + 1], columns[:, 2 * p + 1 : 2 * p + 2])


def head_sum(v, p):
    into = (iota((128, 128), 1) == 2 * p + iota((128, 128), 0) // HEAD_DIM).astype(BF16)
    high, low = split(v)
    return mm(high, into, NN) + mm(low, into, NN)


def sigmoid(x):
    return 1.0 / (1.0 + jnp.exp(-x))


def filtered_of(x_ref, halo_ref, taps_ref, bias_ref, ext_ref, cols):
    ext_ref[0:8, :] = halo_ref[:, cols].astype(F32)
    ext_ref[8 : 8 + TOKENS, :] = x_ref[:, cols].astype(F32)
    total = bias_ref[:, cols] + taps_ref[0:1, cols] * ext_ref[5 : 5 + TOKENS, :]
    for k in range(1, TAPS):
        total = total + taps_ref[k : k + 1, cols] * ext_ref[5 + k : 5 + k + TOKENS, :]
    return total


def write_decays(pay_ref, cums_turned):
    decays = jnp.exp(cums_turned[TOKENS - 1 : TOKENS, :])
    for half in range(2):
        pay_ref[half, :, HALF:] = jnp.broadcast_to(decays, (STATE, 128))


def first_kernel(x_ref, halo_ref, taps_ref, fbias_ref, step_ref, sbias_ref, dlog_ref, act_ref, pay_ref, ext_ref):
    def activate(j, carry):
        cols = lanes(j)
        f = filtered_of(x_ref, halo_ref, taps_ref, fbias_ref, ext_ref, cols)
        act_ref[:, cols] = f * sigmoid(f)
        return carry

    lax.fori_loop(0, CHANNELS // 128, activate, 0)
    _, sizes, _, _, cums = rates_of(step_ref, sbias_ref, dlog_ref)
    to_end = turned(jnp.exp(cums[:, TOKENS - 1 :] - cums) * sizes)
    key_turned = split(jnp.transpose(act_ref[:, INNER : INNER + STATE]))
    for p in range(PAIRS):
        a = act_ref[:, p * 128 : p * 128 + 128] * widen(to_end, p)
        half, at = divmod(p, PAIRS // 2)
        pay_ref[half, :, at * 128 : at * 128 + 128] = dot3(key_turned, split(a), NN)
    write_decays(pay_ref, turned(cums))


def middle_kernel(
    dp_ref, act_ref, gate_ref, step_ref, sbias_ref, dlog_ref, skip_ref, weight_ref, ent_ref, cot_ref,
    w0_ref, w1_ref, w2_ref, w3_ref,
    low_ref, ggate_ref, pay_ref, dy_ref, dx_ref, dq_ref, dk_ref, dcum_ref, dnorm_ref, dskip_ref,
    col_ref, cum_ref, stepx_ref, expx_ref, scores_ref, turn_ref, scan_ref, ng_ref, acc_ref, dsc_ref,
):
    me = dp_ref[0]
    for k, w_ref in enumerate((w0_ref, w1_ref, w2_ref, w3_ref)):
        at = pl.multiple_of(jnp.bitwise_xor(me, k) * ROWS, 128)
        ng_ref[:, pl.ds(at, ROWS)] = mm(cot_ref[...], w_ref[...], NT)
    _, sizes, _, _, cums = rates_of(step_ref, sbias_ref, dlog_ref)
    for h in range(HEADS):
        cum_ref[h] = cums[h : h + 1, :]
    cum_t = turned(cums)
    size_t = turned(sizes)
    exp_t = jnp.exp(cum_t)
    for h in range(HEADS):
        col_ref[h] = jnp.broadcast_to(cum_t[:, h : h + 1], (TOKENS, 128))
    for p in range(PAIRS):
        stepx_ref[:, p * 128 : p * 128 + 128] = widen(size_t, p)
        expx_ref[:, p * 128 : p * 128 + 128] = widen(exp_t, p)
    write_decays(pay_ref, cum_t)
    key = act_ref[:, INNER : INNER + STATE]
    query = act_ref[:, INNER + STATE :]
    key_s, query_s = split(key), split(query)
    query_turned = split(jnp.transpose(query))
    scores_ref[...] = dot3(query_s, key_s, NT)
    turn_ref[...] = dot3(key_s, query_s, NT)
    first = iota((TOKENS, 128), 1) < HEAD_DIM
    down = iota((TOKENS, TOKENS), 0)
    across = iota((TOKENS, TOKENS), 1)

    def column(h):
        c = col_ref[h]
        return jnp.concatenate([c, c], axis=1)

    acc_ref[...] = jnp.zeros_like(acc_ref)

    def forward(p, carry):
        cols = lanes(p)
        half = p // (PAIRS // 2)
        values = act_ref[:, cols]
        high, low = split(values * stepx_ref[:, cols])
        both = jnp.concatenate([high, low], axis=1)
        parts = []
        for i in range(2):
            h = 2 * p + i
            e = jnp.exp(jnp.where(down >= across, column(h) - cum_ref[h], MASKED))
            wh, wl = split(scores_ref[...] * e)
            r = mm(wh, both, NN)
            parts.append(r[:, :128] + r[:, 128:] + mm(wl, high, NN))
        state = split(ent_ref[half, :, lanes(p - half * (PAIRS // 2))])
        scanned = (
            jnp.where(first, parts[0], parts[1])
            + dot3(query_s, state, NN) * expx_ref[:, cols]
            + skip_ref[:, cols] * values
        )
        scan_ref[:, cols] = scanned
        gate = gate_ref[:, cols].astype(F32)
        gated = scanned * (gate * sigmoid(gate))
        acc_ref[...] += gated * gated
        return carry

    lax.fori_loop(0, PAIRS, forward, 0)
    inverse = lax.rsqrt(jnp.sum(acc_ref[...], axis=1, keepdims=True) / INNER + EPSILON)
    acc_ref[...] = jnp.zeros_like(acc_ref)

    def norm(p, carry):
        cols = lanes(p)
        gate = gate_ref[:, cols].astype(F32)
        gated = scan_ref[:, cols] * (gate * sigmoid(gate))
        weight = weight_ref[:, cols]
        unit = gated * inverse
        low_ref[:, cols] = (unit * weight).astype(BF16)
        ng = ng_ref[:, cols]
        dnorm_ref[:, cols] = jnp.sum(ng * unit, axis=0, keepdims=True)
        acc_ref[...] += ng * weight * gated
        return carry

    lax.fori_loop(0, PAIRS, norm, 0)
    lean = jnp.sum(acc_ref[...], axis=1, keepdims=True) * (inverse * inverse * inverse) / INNER
    dsc_ref[...] = jnp.zeros_like(dsc_ref)
    dq_ref[...] = jnp.zeros_like(dq_ref)
    dcum_ref[...] = jnp.zeros_like(dcum_ref)
    dskip_ref[...] = jnp.zeros_like(dskip_ref)

    def backward(p, carry):
        cols = lanes(p)
        half = p // (PAIRS // 2)
        inner = lanes(p - half * (PAIRS // 2))
        gate = gate_ref[:, cols].astype(F32)
        gain = sigmoid(gate)
        silu = gate * gain
        scanned = scan_ref[:, cols]
        dgated = inverse * (ng_ref[:, cols] * weight_ref[:, cols]) - scanned * silu * lean
        ggate_ref[:, cols] = (dgated * scanned * (gain * (1.0 + gate * (1.0 - gain)))).astype(BF16)
        dy = dgated * silu
        dy_ref[:, cols] = dy
        dh, dl = split(dy)
        both = jnp.concatenate([dh, dl], axis=1)
        twice = jnp.concatenate([dh, dh], axis=1)
        values = act_ref[:, cols]
        scaled = values * stepx_ref[:, cols]
        parts = []
        for i in range(2):
            h = 2 * p + i
            e = jnp.exp(jnp.where(across >= down, cum_ref[h] - column(h), MASKED))
            wh, wl = split(turn_ref[...] * e)
            r = mm(wh, both, NN)
            parts.append(r[:, :128] + r[:, 128:] + mm(wl, dh, NN))
            own = first if i == 0 else jnp.logical_not(first)
            xh, xl = split(jnp.where(own, scaled, 0.0))
            dw = mm(jnp.concatenate([xh, xl], axis=1), twice, NT) + mm(xh, dl, NT)
            dsc_ref[...] += dw * e
        dx = jnp.where(first, parts[0], parts[1])
        dx_ref[:, cols] = dx
        z = split(dy * expx_ref[:, cols])
        pay_ref[half, :, inner] = dot3(query_turned, z, NN)
        dq_ref[...] += dot3(z, split(ent_ref[half, :, inner]), NT)
        skipped = dy * values
        dcum_ref[...] += head_sum(dy * scanned - skipped * skip_ref[:, cols] - scaled * dx, p)
        dskip_ref[...] += head_sum(jnp.sum(skipped.reshape(TOKENS // 8, 8, 128), axis=0), p)
        return carry

    lax.fori_loop(0, PAIRS, backward, 0)
    dsc = dsc_ref[...]
    dk_ref[...] = dot3(split(dsc), query_s, NN)
    dq_ref[...] += dot3(split(jnp.transpose(dsc)), key_s, NN)


def last_kernel(
    x_ref, halo_ref, taps_ref, fbias_ref, act_ref, step_ref, sbias_ref, dlog_ref, skip_ref, ent_ref, end_ref,
    dy_ref, dx_ref, dq_ref, dk_ref, dcum_ref, dskip_ref,
    gin_ref, tail_ref, ret_ref, gstep_ref, gfilt_ref, ghead_ref,
    ext_ref, dfilt_ref, stepx_ref, endx_ref, dact_ref, dstep_ref, zsum_ref, ded_ref, dkey_ref,
):
    raw, sizes, gain, rates, cums = rates_of(step_ref, sbias_ref, dlog_ref)
    size_t = turned(sizes)
    end_t = turned(jnp.exp(cums[:, TOKENS - 1 :] - cums))
    for p in range(PAIRS):
        stepx_ref[:, p * 128 : p * 128 + 128] = widen(size_t, p)
        endx_ref[:, p * 128 : p * 128 + 128] = widen(end_t, p)
    key_s = split(act_ref[:, INNER : INNER + STATE])
    dstep_ref[...] = jnp.zeros_like(dstep_ref)
    zsum_ref[...] = jnp.zeros_like(zsum_ref)
    ded_ref[...] = jnp.zeros_like(ded_ref)
    dkey_ref[...] = dk_ref[...]

    def pair(p, carry):
        cols = lanes(p)
        half = p // (PAIRS // 2)
        inner = lanes(p - half * (PAIRS // 2))
        values = act_ref[:, cols]
        step = stepx_ref[:, cols]
        ending = endx_ref[:, cols]
        end = end_ref[half, :, inner]
        end_s = split(end)
        z = dot3(key_s, end_s, NN) * ending
        dx = dx_ref[:, cols] + z
        dact_ref[:, cols] = dx * step + skip_ref[:, cols] * dy_ref[:, cols]
        dstep_ref[...] += head_sum(dx * values, p)
        scaled = values * step
        zsum_ref[...] += head_sum(scaled * z, p)
        dkey_ref[...] += dot3(split(scaled * ending), end_s, NT)
        both = end * ent_ref[half, :, inner]
        ded_ref[...] += head_sum(jnp.sum(both.reshape(STATE // 8, 8, 128), axis=0), p)
        return carry

    lax.fori_loop(0, PAIRS, pair, 0)
    dact_ref[:, INNER : INNER + STATE] = dkey_ref[...]
    dact_ref[:, INNER + STATE :] = dq_ref[...]
    zsum = zsum_ref[...]
    cum_t = turned(cums)
    decays = jnp.exp(cum_t[TOKENS - 1 :, :])
    final = jnp.sum(zsum, axis=0, keepdims=True) + decays * jnp.sum(ded_ref[...], axis=0, keepdims=True)
    row = iota((TOKENS, 128), 0)
    dcum = dcum_ref[...] - zsum + jnp.where(row == TOKENS - 1, final, 0.0)
    shift = 1
    while shift < TOKENS:
        dcum = dcum + jnp.where(row < TOKENS - shift, pltpu.roll(dcum, TOKENS - shift, 0), 0.0)
        shift *= 2
    gain_t = turned(jnp.broadcast_to(gain, (HEADS, TOKENS)))
    draw = (dstep_ref[...] + dcum * gain_t) * turned(sigmoid(raw))
    gstep_ref[...] = jnp.transpose(draw)[:HEADS, :]
    ghead_ref[0:1, :] = jnp.sum(draw, axis=0, keepdims=True)
    ghead_ref[1:2, :] = jnp.sum(dcum * turned(rates), axis=0, keepdims=True)
    ghead_ref[2:3, :] = jnp.sum(dskip_ref[...], axis=0, keepdims=True)
    ghead_ref[3:8, :] = jnp.zeros((5, 128), F32)
    dfilt_ref[0:8, :] = jnp.zeros((8, 128), F32)
    dfilt_ref[8 + TOKENS :, :] = jnp.zeros((8, 128), F32)

    def filters(j, carry):
        cols = lanes(j)
        f = filtered_of(x_ref, halo_ref, taps_ref, fbias_ref, ext_ref, cols)
        s = sigmoid(f)
        dfilt = dact_ref[:, cols] * (s * (1.0 + f * (1.0 - s)))
        dfilt_ref[8 : 8 + TOKENS, :] = dfilt
        dx = taps_ref[TAPS - 1 : TAPS, cols] * dfilt
        back = taps_ref[0:1, cols] * dfilt_ref[8:16, :]
        for k in range(TAPS):
            gfilt_ref[k : k + 1, cols] = jnp.sum(dfilt * ext_ref[5 + k : 5 + k + TOKENS, :], axis=0, keepdims=True)
            if k < TAPS - 1:
                dx = dx + taps_ref[k : k + 1, cols] * dfilt_ref[11 - k : 11 - k + TOKENS, :]
            if 0 < k < TAPS - 1:
                back = back + taps_ref[k : k + 1, cols] * dfilt_ref[8 - k : 16 - k, :]
        gfilt_ref[TAPS : TAPS + 1, cols] = jnp.sum(dfilt, axis=0, keepdims=True)
        gin_ref[:, cols] = dx.astype(BF16)
        tail_ref[:, cols] = dx[TOKENS - 8 :, :]
        ret_ref[:, cols] = back
        return carry

    lax.fori_loop(0, CHANNELS // 128, filters, 0)


def outer_kernel(l0, l1, l2, l3, g0, g1, g2, g3, out_ref):
    lows = [jnp.transpose(r[...]) for r in (l0, l1, l2, l3)]
    cots = (g0, g1, g2, g3)

    for j in range(WIDTH // 256):
        total = mm(lows[0], cots[0][:, j * 256 : j * 256 + 256], NN)
        for k in range(1, DP):
            total = total + mm(lows[k], cots[k][:, j * 256 : j * 256 + 256], NN)
        for i in range(2):
            at = (2 * j + i) * ROWS
            out_ref[at : at + ROWS, :] = total[:, i * 128 : i * 128 + 128].astype(BF16)
    out_ref[10 * ROWS :, :] = jnp.zeros((SEQ * PIECE - 10 * ROWS, 128), BF16)


def greet(seq, dp, with_dp):
    barrier = pltpu.get_barrier_semaphore()

    def hello(i, carry):
        peer = lax.rem(seq + i, SEQ)
        pl.semaphore_signal(barrier, inc=1, device_id=(peer, dp), device_id_type=MESH)
        return carry

    lax.fori_loop(1, SEQ, hello, 0)
    count = SEQ - 1
    if with_dp:
        for k in range(1, DP):
            other = lax.rem(dp + k, DP)
            pl.semaphore_signal(barrier, inc=1, device_id=(seq, other), device_id_type=MESH)
        count += DP - 1
    pl.semaphore_wait(barrier, count)


def to_peer(src, dst, send, recv, device):
    return pltpu.make_async_remote_copy(
        src_ref=src, dst_ref=dst, send_sem=send, recv_sem=recv, device_id=device, device_id_type=MESH
    )


def scan_kernel(reverse, pay_ref, out_ref, recv, outgoing, coef, sems):
    seq, dp = lax.axis_index("seq"), lax.axis_index("dp")
    greet(seq, dp, False)

    def each_peer(act):
        def step(i, carry):
            act(i, lax.rem(seq + i, SEQ))
            return carry

        lax.fori_loop(1, SEQ, step, 0)

    def spread(i, peer):
        return to_peer(pay_ref.at[peer], recv.at[seq], sems.at[0, i], sems.at[1, seq], (peer, dp))

    def spread_here(i, peer):
        return to_peer(pay_ref.at[peer], recv.at[peer], sems.at[0, i], sems.at[1, peer], (peer, dp))

    each_peer(lambda i, peer: spread(i, peer).start())
    recv[seq] = pay_ref[seq]
    each_peer(lambda i, peer: spread_here(i, peer).wait_recv())

    decays = jnp.concatenate([recv[k, 0:1, HALF:] for k in range(SEQ)], axis=0)
    head = (seq // (SEQ // 2)) * (HEADS // 2) + iota((128, HALF), 1) // HEAD_DIM
    into = (iota((128, HALF), 0) == head).astype(F32)
    wide = lax.dot_general(
        decays, into, (NN, ((), ())), preferred_element_type=F32, precision=lax.Precision.HIGHEST
    )
    for k in range(SEQ):
        coef[k] = wide[k : k + 1, :]

    def scan(j, state):
        k = SEQ - 1 - j if reverse else j
        outgoing[k] = state
        return coef[k] * state + recv[k, :, :HALF]

    lax.fori_loop(0, SEQ, scan, jnp.zeros((8, HALF), F32))

    def back(i, peer):
        return to_peer(outgoing.at[peer], out_ref.at[seq], sems.at[2, i], sems.at[3, seq], (peer, dp))

    def back_here(i, peer):
        return to_peer(outgoing.at[peer], out_ref.at[peer], sems.at[2, i], sems.at[3, peer], (peer, dp))

    each_peer(lambda i, peer: back(i, peer).start())
    out_ref[seq] = outgoing[seq]
    each_peer(lambda i, peer: back_here(i, peer).wait_recv())
    each_peer(lambda i, peer: spread(i, peer).wait_send())
    each_peer(lambda i, peer: back(i, peer).wait_send())


def sum_kernel(wide_ref, small_ref, wout_ref, sout_ref, wrecv, srecv, wown, sown, sdp, wacc, sems, dsems):
    seq, dp = lax.axis_index("seq"), lax.axis_index("dp")
    greet(seq, dp, True)

    def each_peer(act):
        def step(i, carry):
            act(i, lax.rem(seq + i, SEQ))
            return carry

        lax.fori_loop(1, SEQ, step, 0)

    def out(src, dst, row):
        return lambda i, peer: to_peer(src.at[peer], dst.at[seq], sems.at[row, i], sems.at[row + 1, seq], (peer, dp))

    def out_here(src, dst, row):
        return lambda i, peer: to_peer(src.at[peer], dst.at[peer], sems.at[row, i], sems.at[row + 1, peer], (peer, dp))

    def all_of(src, dst, row):
        return lambda i, peer: to_peer(src, dst.at[seq], sems.at[row, i], sems.at[row + 1, seq], (peer, dp))

    def all_here(src, dst, row):
        return lambda i, peer: to_peer(src, dst.at[peer], sems.at[row, i], sems.at[row + 1, peer], (peer, dp))

    each_peer(lambda i, peer: out(small_ref, srecv, 0)(i, peer).start())
    each_peer(lambda i, peer: out(wide_ref, wrecv, 2)(i, peer).start())
    srecv[seq] = small_ref[seq]
    wrecv[seq] = wide_ref[seq]
    each_peer(lambda i, peer: out_here(small_ref, srecv, 0)(i, peer).wait_recv())
    sdp[dp] = lax.fori_loop(0, SEQ, lambda k, total: total + srecv[k], jnp.zeros((8, 128), F32))

    def across(k):
        other = lax.rem(dp + k, DP)
        return to_peer(sdp.at[dp], sdp.at[dp], dsems.at[0, k], dsems.at[1, dp], (seq, other))

    def across_here(k):
        other = lax.rem(dp + k, DP)
        return to_peer(sdp.at[dp], sdp.at[other], dsems.at[0, k], dsems.at[1, other], (seq, other))

    for k in range(1, DP):
        across(k).start()
    for k in range(1, DP):
        across_here(k).wait_recv()
    sown[...] = sdp[0] + sdp[1] + sdp[2] + sdp[3]
    each_peer(lambda i, peer: all_of(sown, sout_ref, 4)(i, peer).start())
    sout_ref[seq] = sown[...]

    each_peer(lambda i, peer: out_here(wide_ref, wrecv, 2)(i, peer).wait_recv())
    wacc[...] = jnp.zeros_like(wacc)

    def add(k, carry):
        wacc[...] += wrecv[k].astype(F32)
        return carry

    lax.fori_loop(0, SEQ, add, 0)
    wown[...] = wacc[...].astype(BF16)
    each_peer(lambda i, peer: all_of(wown, wout_ref, 6)(i, peer).start())
    wout_ref[seq] = wown[...]
    each_peer(lambda i, peer: all_here(sown, sout_ref, 4)(i, peer).wait_recv())
    each_peer(lambda i, peer: all_here(wown, wout_ref, 6)(i, peer).wait_recv())
    for k in range(1, DP):
        across(k).wait_send()
    each_peer(lambda i, peer: out(small_ref, srecv, 0)(i, peer).wait_send())
    each_peer(lambda i, peer: out(wide_ref, wrecv, 2)(i, peer).wait_send())
    each_peer(lambda i, peer: all_of(sown, sout_ref, 4)(i, peer).wait_send())
    each_peer(lambda i, peer: all_of(wown, wout_ref, 6)(i, peer).wait_send())


VMEM = pl.BlockSpec(memory_space=pltpu.VMEM)
SMEM = pl.BlockSpec(memory_space=pltpu.SMEM)


def call(kernel, outs, scratch, args, specs=None, collective=None, flops=0, traffic=0, name=None):
    params = dict(vmem_limit_bytes=60 * 2**20)
    if collective is not None:
        params.update(collective_id=collective, has_side_effects=True)
    return pl.pallas_call(
        kernel,
        out_shape=[jax.ShapeDtypeStruct(shape, kind) for shape, kind in outs],
        in_specs=specs or [VMEM] * len(args),
        out_specs=[VMEM] * len(outs),
        scratch_shapes=scratch,
        compiler_params=pltpu.CompilerParams(**params),
        cost_estimate=pl.CostEstimate(flops=flops, bytes_accessed=traffic, transcendentals=0),
        name=name,
    )(*args)


def vmem(*shape, kind=F32):
    return pltpu.VMEM(shape, kind)


def state_scan(payload, reverse, collective):
    (out,) = call(
        functools.partial(scan_kernel, reverse),
        [((SEQ, 8, HALF), F32)],
        [vmem(SEQ, 8, CHUNK), vmem(SEQ, 8, HALF), vmem(SEQ, 1, HALF), pltpu.SemaphoreType.DMA((4, SEQ))],
        (payload.reshape(SEQ, 8, CHUNK),),
        collective=collective,
        flops=30_000_000_000,
        name="scan_back" if reverse else "scan_on",
    )
    return out.reshape(2, STATE, HALF)


def moved(value, bits):
    return lax.ppermute(value, "dp", [(d, d ^ bits) for d in range(DP)])


def body(
    conv_input, gate_input, step_input, filter_taps, filter_bias, step_bias, decay_log, skip_gain, norm_weight,
    output_weight, output_grad,
):
    raw_rows, gate_rows, step_rows, cotangent = conv_input[0], gate_input[0], step_input[0], output_grad[0]
    dp = lax.axis_index("dp")
    crossing = [(s * DP + d, (s ^ 4) * DP + (d ^ 2)) for s in range(SEQ) for d in range(DP)]
    halo = lax.ppermute(raw_rows[-8:], "seq", [(s, s + 1) for s in range(SEQ - 1)])
    weight_2 = lax.ppermute(output_weight, ("seq", "dp"), crossing)
    weight_1 = moved(output_weight, 1)
    weight_3 = moved(weight_2, 1)
    cot_1, cot_2 = moved(cotangent, 1), moved(cotangent, 2)
    cot_3 = moved(cot_2, 1)

    fbias = filter_bias[None]
    heads = (step_rows, step_bias[:, None], decay_log[:, None])
    skip = jnp.repeat(skip_gain, HEAD_DIM)[None]
    act, payload = call(
        first_kernel,
        [((TOKENS, CHANNELS), F32), ((2, STATE, CHUNK), F32)],
        [vmem(TOKENS + 8, 128)],
        (raw_rows, halo, filter_taps, fbias, *heads),
        flops=5_000_000_000,
        name="first",
    )
    entering = state_scan(payload, False, 0)
    wide = (TOKENS, INNER)
    small = (TOKENS, STATE)
    low, gate_grad, payload, dy, dx, dq, dk, dcum, dnorm, dskip = call(
        middle_kernel,
        [(wide, BF16), (wide, BF16), ((2, STATE, CHUNK), F32), (wide, F32), (wide, F32), (small, F32), (small, F32),
         (small, F32), ((1, INNER), F32), ((8, 128), F32)],
        [vmem(HEADS, TOKENS, 128), vmem(HEADS, 1, TOKENS), vmem(*wide), vmem(*wide), vmem(TOKENS, TOKENS),
         vmem(TOKENS, TOKENS), vmem(*wide), vmem(*wide), vmem(TOKENS, 128), vmem(TOKENS, TOKENS)],
        (dp[None].astype(jnp.int32), act, gate_rows, *heads, skip, norm_weight[None], entering, cotangent,
         output_weight, weight_1, weight_2, weight_3),
        specs=[SMEM] + [VMEM] * 13,
        flops=20_000_000_000,
        name="middle",
    )
    lows = [
        lax.dynamic_slice_in_dim(low, jnp.bitwise_xor(dp, k) * ROWS, ROWS, axis=1) for k in range(DP)
    ]
    lows = [lows[0]] + [moved(lows[k], k) for k in range(1, DP)]
    ending = state_scan(payload, True, 1)
    (partial,) = call(
        outer_kernel, [((SEQ * PIECE, 128), BF16)], [], (*lows, cotangent, cot_1, cot_2, cot_3),
        flops=4_000_000_000, name="outer",
    )
    gin, tail, back, gstep, gfilt, ghead = call(
        last_kernel,
        [((TOKENS, CHANNELS), BF16), ((8, CHANNELS), F32), ((8, CHANNELS), F32), ((HEADS, TOKENS), F32),
         ((TAPS + 1, CHANNELS), F32), ((8, 128), F32)],
        [vmem(TOKENS + 8, 128), vmem(TOKENS + 16, 128), vmem(*wide), vmem(*wide), vmem(TOKENS, CHANNELS),
         vmem(*small), vmem(*small), vmem(8, 128), vmem(*small)],
        (raw_rows, halo, filter_taps, fbias, act, *heads, skip, entering, ending, dy, dx, dq, dk, dcum, dskip),
        flops=8_000_000_000,
        name="last",
    )
    returned = lax.ppermute(back, "seq", [(s + 1, s) for s in range(SEQ - 1)])
    parts = jnp.concatenate([gfilt.ravel(), dnorm.ravel(), ghead[:3, :HEADS].ravel()])
    count = parts.shape[0]
    parts = jnp.concatenate([parts, jnp.zeros((SEQ * 1024 - count,), F32)]).reshape(SEQ, 8, 128)
    wsum, ssum = call(
        sum_kernel,
        [((SEQ, PIECE, 128), BF16), ((SEQ, 8, 128), F32)],
        [vmem(SEQ, PIECE, 128, kind=BF16), vmem(SEQ, 8, 128), vmem(PIECE, 128, kind=BF16), vmem(8, 128),
         vmem(DP, 8, 128), vmem(PIECE, 128), pltpu.SemaphoreType.DMA((8, SEQ)), pltpu.SemaphoreType.DMA((2, DP))],
        (partial.reshape(SEQ, PIECE, 128), parts),
        collective=2,
        flops=30_000_000_000,
        name="sums",
    )
    weight_grad = wsum.reshape(SEQ * PIECE, 128)[: 10 * ROWS].reshape(10, ROWS, 128).transpose(1, 0, 2)
    weight_grad = weight_grad.reshape(ROWS, WIDTH).astype(F32)
    sums = ssum.ravel()
    filters, norms = (TAPS + 1) * CHANNELS, INNER
    filter_grads = sums[:filters].reshape(TAPS + 1, CHANNELS)
    norm_grad = sums[filters : filters + norms]
    head_grads = sums[filters + norms : count].reshape(3, HEADS)
    tail = jnp.concatenate([tail[:5], tail[5:] + returned[:3]], axis=0).astype(BF16)
    input_grad = lax.dynamic_update_slice(gin, tail, (TOKENS - 8, 0))
    return input_grad[None], gate_grad[None], gstep[None], weight_grad, filter_grads, norm_grad, head_grads


def solution(mesh):
    tokens, by_head, rows = P("dp", "seq", None), P("dp", None, "seq"), P("dp", None)
    return jax.shard_map(
        body,
        mesh=mesh,
        in_specs=(tokens, tokens, by_head, P(), P(), P(), P(), P(), P(), rows, tokens),
        out_specs=(tokens, tokens, by_head, rows, P(), P(), P()),
        check_vma=False,
    )
```

```python
import jax
import jax.numpy as jnp
from jax import lax
from jax.experimental import pallas as pl
from jax.experimental.pallas import tpu as pltpu
from jax.sharding import PartitionSpec as P

HEADS = 40
HEAD_DIM = 64
STATE = 128
INNER = 2560
CHANNELS = 2816
WIDTH = 1280
TOKENS = 256
TAPS = 4
PAIRS = 20
HALF = 1280
CHUNK = HALF + 128
SEQ = 32
DP = 4
ROWS = INNER // DP
EDGE = 16
PIECE = 208
MASKED = -1e30
EPSILON = 1e-05

F32 = jnp.float32
BF16 = jnp.bfloat16
MESH = pl.DeviceIdType.MESH
NN = ((1,), (0,))
NT = ((1,), (1,))
TN = ((0,), (0,))


def mm(a, b, dims):
    return lax.dot_general(a, b, (dims, ((), ())), preferred_element_type=F32)


def split(x):
    high = x.astype(BF16)
    return high, (x - high.astype(F32)).astype(BF16)


def dot3(a, b, dims):
    return mm(a[0], b[0], dims) + mm(a[0], b[1], dims) + mm(a[1], b[0], dims)


def iota(shape, dim):
    return lax.broadcasted_iota(jnp.int32, shape, dim)


def lanes(p):
    return pl.ds(pl.multiple_of(p * 128, 128), 128)


def turned(x):
    return jnp.transpose(jnp.concatenate([x, jnp.zeros((128 - HEADS, TOKENS), F32)], axis=0))


def rates_of(step_ref, table_ref):
    columns = jnp.transpose(jnp.concatenate([table_ref[7:9, :128], jnp.zeros((126, 128), F32)], axis=0))
    raw = step_ref[...] + columns[:HEADS, 0:1]
    sizes = jnp.maximum(raw, 0.0) + jnp.log1p(jnp.exp(-jnp.abs(raw)))
    gain = -jnp.exp(columns[:HEADS, 1:2])
    rates = sizes * gain
    lane = iota(rates.shape, 1)
    cums = rates
    shift = 1
    while shift < TOKENS:
        cums = cums + jnp.where(lane >= shift, pltpu.roll(cums, shift, 1), 0.0)
        shift *= 2
    return raw, sizes, gain, rates, cums


def widen(columns, p):
    first = iota((TOKENS, 128), 1) < HEAD_DIM
    return jnp.where(first, columns[:, 2 * p : 2 * p + 1], columns[:, 2 * p + 1 : 2 * p + 2])


def head_sum(v, p):
    into = (iota((128, 128), 1) == 2 * p + iota((128, 128), 0) // HEAD_DIM).astype(BF16)
    high, low = split(v)
    return mm(high, into, NN) + mm(low, into, NN)


def sigmoid(x):
    return 1.0 / (1.0 + jnp.exp(-x))


def filtered_of(x_ref, table_ref, ext_ref, edge, cols):
    ext_ref[0:EDGE, :] = edge
    ext_ref[EDGE : EDGE + TOKENS, :] = x_ref[:, cols].astype(F32)
    total = table_ref[TAPS : TAPS + 1, cols]
    for k in range(TAPS):
        at = EDGE - TAPS + 1 + k
        total = total + table_ref[k : k + 1, cols] * ext_ref[at : at + TOKENS, :]
    return total


def write_decays(pay_ref, cums_turned):
    decays = jnp.exp(cums_turned[TOKENS - 1 : TOKENS, :])
    for c in range(SEQ):
        pay_ref[c, :, HALF:] = jnp.broadcast_to(decays, (8, 128))


def write_state(pay_ref, p, state):
    half = p // (PAIRS // 2)
    at = lanes(p - half * (PAIRS // 2))
    for c in range(SEQ // 2):
        pay_ref[half * (SEQ // 2) + c, :, at] = state[c * 8 : c * 8 + 8, :]


def read_state(ref, p):
    half = p // (PAIRS // 2)
    at = lanes(p - half * (PAIRS // 2))
    return jnp.concatenate([ref[half * (SEQ // 2) + c, :, at] for c in range(SEQ // 2)], axis=0)


def to_peer(src, dst, send, recv, device):
    return pltpu.make_async_remote_copy(
        src_ref=src, dst_ref=dst, send_sem=send, recv_sem=recv, device_id=device, device_id_type=MESH
    )


def greet(seq, dp, others):
    barrier = pltpu.get_barrier_semaphore()

    def hello(i, carry):
        peer = lax.rem(seq + i, SEQ)
        pl.semaphore_signal(barrier, inc=1, device_id=(peer, dp), device_id_type=MESH)
        return carry

    lax.fori_loop(1, SEQ, hello, 0)
    for other in others:
        pl.semaphore_signal(barrier, inc=1, device_id=other, device_id_type=MESH)
    pl.semaphore_wait(barrier, SEQ - 1 + len(others))


def each_peer(seq, act):
    def step(i, carry):
        act(i, lax.rem(seq + i, SEQ))
        return carry

    lax.fori_loop(1, SEQ, step, 0)


class Scatter:
    def __init__(self, seq, dp, src, dst, sems, row, whole=False):
        self.seq, self.dp, self.src, self.dst, self.sems, self.row, self.whole = seq, dp, src, dst, sems, row, whole

    def copy(self, i, peer, slot):
        src = self.src if self.whole else self.src.at[peer]
        sems = self.sems
        return to_peer(src, self.dst.at[slot], sems.at[self.row, i], sems.at[self.row + 1, slot], (peer, self.dp))

    def start(self):
        each_peer(self.seq, lambda i, peer: self.copy(i, peer, self.seq).start())
        self.dst[self.seq] = self.src[...] if self.whole else self.src[self.seq]

    def received(self):
        each_peer(self.seq, lambda i, peer: self.copy(i, peer, peer).wait_recv())

    def sent(self):
        each_peer(self.seq, lambda i, peer: self.copy(i, peer, self.seq).wait_send())


def scan_chunks(seq, reverse, recv, outgoing, coef):
    decays = jnp.concatenate([recv[k, 0:1, HALF:] for k in range(SEQ)], axis=0)
    head = (seq // (SEQ // 2)) * (HEADS // 2) + iota((128, HALF), 1) // HEAD_DIM
    into = (iota((128, HALF), 0) == head).astype(F32)
    wide = lax.dot_general(
        decays, into, (NN, ((), ())), preferred_element_type=F32, precision=lax.Precision.HIGHEST
    )
    for k in range(SEQ):
        coef[k] = wide[k : k + 1, :]

    def scan(j, state):
        k = SEQ - 1 - j if reverse else j
        outgoing[k] = state
        return coef[k] * state + recv[k, :, :HALF]

    lax.fori_loop(0, SEQ, scan, jnp.zeros((8, HALF), F32))


def place():
    seq, dp = lax.axis_index("seq"), lax.axis_index("dp")
    partner = dp + 1 - 2 * lax.rem(dp, 2)
    across = lax.rem(dp + 2, DP)
    return seq, dp, partner, across


def forward_kernel(
    x_ref, table_ref, step_ref, cot_ref, w_ref,
    act_ref, inside_ref, ng_ref, ent_ref, halo_ref,
    edge_ref, ext_ref, pay_ref, recv, outgoing, coef, wrecv, col_ref, cum_ref, stepx_ref, scores_ref, sems, wsems, hsems,
):
    seq, dp, partner, across = place()
    beside = seq + 4 - 8 * lax.rem(seq // 4, 2)
    after, before = lax.rem(seq + 1, SEQ), lax.rem(seq + SEQ - 1, SEQ)
    greet(seq, dp, [(seq, partner), (beside, across)])
    last_rows = x_ref.at[pl.ds(TOKENS - EDGE, EDGE)]
    halo = to_peer(last_rows, edge_ref, hsems.at[0], hsems.at[1], (after, dp))
    halo.start()
    quarter = ROWS // 4

    def piece(q):
        return pl.ds(q * quarter, quarter)

    cross = [
        to_peer(w_ref.at[piece(q)], wrecv.at[1, piece(q)], wsems.at[0, q], wsems.at[1, q], (beside, across))
        for q in range(4)
    ]
    relay = [
        to_peer(wrecv.at[1, piece(q)], wrecv.at[2, piece(q)], wsems.at[2, q], wsems.at[3, q], (seq, partner))
        for q in range(4)
    ]
    near = to_peer(w_ref, wrecv.at[0], wsems.at[4, 0], wsems.at[5, 0], (seq, partner))
    for copy in cross:
        copy.start()
    near.start()
    _, sizes, _, _, cums = rates_of(step_ref, table_ref)
    cum_t = turned(cums)
    size_t = turned(sizes)
    end_t = turned(jnp.exp(cums[:, TOKENS - 1 :] - cums) * sizes)
    write_decays(pay_ref, cum_t)
    halo.wait_recv()
    halo_ref[...] = jnp.where(seq > 0, edge_ref[...].astype(F32), 0.0)

    def activate(j, carry):
        cols = lanes(j)
        f = filtered_of(x_ref, table_ref, ext_ref, halo_ref[:, cols], cols)
        act_ref[:, cols] = f * sigmoid(f)
        return carry

    lax.fori_loop(0, CHANNELS // 128, activate, 0)
    key = act_ref[:, INNER : INNER + STATE]
    key_turned = split(jnp.transpose(key))
    for p in range(PAIRS):
        a = act_ref[:, p * 128 : p * 128 + 128] * widen(end_t, p)
        write_state(pay_ref, p, dot3(key_turned, split(a), NN))
    out = Scatter(seq, dp, pay_ref, recv, sems, 0)
    out.start()

    for h in range(HEADS):
        cum_ref[h] = cums[h : h + 1, :]
        col_ref[h] = jnp.broadcast_to(cum_t[:, h : h + 1], (TOKENS, 128))
    for p in range(PAIRS):
        stepx_ref[:, p * 128 : p * 128 + 128] = widen(size_t, p)
    query = act_ref[:, INNER + STATE :]
    scores_ref[...] = dot3(split(query), split(key), NT)
    first = iota((TOKENS, 128), 1) < HEAD_DIM
    causal = iota((TOKENS, TOKENS), 0) >= iota((TOKENS, TOKENS), 1)

    def forward(p, carry):
        cols = lanes(p)
        high, low = split(act_ref[:, cols] * stepx_ref[:, cols])
        both = jnp.concatenate([high, low], axis=1)
        parts = []
        for i in range(2):
            h = 2 * p + i
            c = col_ref[h]
            e = jnp.exp(jnp.where(causal, jnp.concatenate([c, c], axis=1) - cum_ref[h], MASKED))
            wh, wl = split(scores_ref[...] * e)
            r = mm(wh, both, NN)
            parts.append(r[:, :128] + r[:, 128:] + mm(wl, high, NN))
        inside_ref[:, cols] = jnp.where(first, parts[0], parts[1])
        return carry

    def normed_grad(block, weights):
        at = pl.multiple_of(block * ROWS, 128)
        ng_ref[:, pl.ds(at, ROWS)] = mm(cot_ref[...], weights[...], NT)

    lax.fori_loop(0, PAIRS, forward, 0)
    normed_grad(dp, w_ref)
    out.received()
    scan_chunks(seq, False, recv, outgoing, coef)
    back = Scatter(seq, dp, outgoing, ent_ref, sems, 2)
    back.start()
    near.wait_recv()
    normed_grad(partner, wrecv.at[0])
    for q in range(4):
        cross[q].wait_recv()
        relay[q].start()
    normed_grad(across, wrecv.at[1])
    for copy in relay:
        copy.wait_recv()
    normed_grad(DP - 1 - dp, wrecv.at[2])
    back.received()
    for copy in [halo, near, *cross, *relay]:
        copy.wait_send()
    out.sent()
    back.sent()


def backward_kernel(
    act_ref, gate_ref, table_ref, step_ref, ent_ref, inside_ref, ng_ref, cot_ref,
    ggate_ref, dy_ref, dx_ref, dq_ref, dk_ref, dcum_ref, dnorm_ref, dskip_ref, end_ref, part_ref,
    pay_ref, recv, outgoing, coef, low_ref, lrecv, crecv, col_ref, cum_ref, stepx_ref, expx_ref, turn_ref, scan_ref,
    acc_ref, dsc_ref, sems, dsems,
):
    seq, dp, partner, across = place()
    corner = DP - 1 - dp
    greet(seq, dp, [(seq, partner), (seq, across), (seq, corner)])
    near = to_peer(cot_ref, crecv.at[0], dsems.at[0, 0], dsems.at[1, 0], (seq, partner))
    cross = to_peer(cot_ref, crecv.at[1], dsems.at[0, 1], dsems.at[1, 1], (seq, across))
    relay = to_peer(crecv.at[1], crecv.at[2], dsems.at[0, 2], dsems.at[1, 2], (seq, partner))
    near.start()
    cross.start()

    _, sizes, _, _, cums = rates_of(step_ref, table_ref)
    cum_t = turned(cums)
    size_t = turned(sizes)
    exp_t = jnp.exp(cum_t)
    write_decays(pay_ref, cum_t)
    for p in range(PAIRS):
        expx_ref[:, p * 128 : p * 128 + 128] = widen(exp_t, p)
    query = act_ref[:, INNER + STATE :]
    query_s = split(query)
    query_turned = split(jnp.transpose(query))
    acc_ref[...] = jnp.zeros_like(acc_ref)

    def forward(p, carry):
        cols = lanes(p)
        carried = dot3(query_s, split(read_state(ent_ref, p)), NN) * expx_ref[:, cols]
        scanned = inside_ref[:, cols] + carried + table_ref[6:7, cols] * act_ref[:, cols]
        scan_ref[:, cols] = scanned
        gate = gate_ref[:, cols].astype(F32)
        gated = scanned * (gate * sigmoid(gate))
        acc_ref[...] += gated * gated
        return carry

    lax.fori_loop(0, PAIRS, forward, 0)
    inverse = lax.rsqrt(jnp.sum(acc_ref[...], axis=1, keepdims=True) / INNER + EPSILON)
    acc_ref[...] = jnp.zeros_like(acc_ref)

    def norm(p, carry):
        cols = lanes(p)
        gate = gate_ref[:, cols].astype(F32)
        gated = scan_ref[:, cols] * (gate * sigmoid(gate))
        weight = table_ref[5:6, cols]
        unit = gated * inverse
        block = p // 5
        low_ref[block, :, lanes(p - block * 5)] = (unit * weight).astype(BF16)
        ng = ng_ref[:, cols]
        dnorm_ref[:, cols] = jnp.sum(ng * unit, axis=0, keepdims=True)
        acc_ref[...] += ng * weight * gated
        return carry

    lax.fori_loop(0, PAIRS, norm, 0)
    lows = [
        to_peer(low_ref.at[other], lrecv.at[k], dsems.at[2, k], dsems.at[3, k], (seq, other))
        for k, other in enumerate((partner, across, corner))
    ]
    for copy in lows:
        copy.start()
    lean = jnp.sum(acc_ref[...], axis=1, keepdims=True) * (inverse * inverse * inverse) / INNER

    def cotangents(p, carry):
        cols = lanes(p)
        gate = gate_ref[:, cols].astype(F32)
        gain = sigmoid(gate)
        silu = gate * gain
        scanned = scan_ref[:, cols]
        dgated = inverse * (ng_ref[:, cols] * table_ref[5:6, cols]) - scanned * silu * lean
        ggate_ref[:, cols] = (dgated * scanned * (gain * (1.0 + gate * (1.0 - gain)))).astype(BF16)
        dy = dgated * silu
        dy_ref[:, cols] = dy
        write_state(pay_ref, p, dot3(query_turned, split(dy * expx_ref[:, cols]), NN))
        return carry

    lax.fori_loop(0, PAIRS, cotangents, 0)
    out = Scatter(seq, dp, pay_ref, recv, sems, 0)
    out.start()

    for h in range(HEADS):
        cum_ref[h] = cums[h : h + 1, :]
        col_ref[h] = jnp.broadcast_to(cum_t[:, h : h + 1], (TOKENS, 128))
    for p in range(PAIRS):
        stepx_ref[:, p * 128 : p * 128 + 128] = widen(size_t, p)
    key_s = split(act_ref[:, INNER : INNER + STATE])
    turn_ref[...] = dot3(key_s, query_s, NT)
    first = iota((TOKENS, 128), 1) < HEAD_DIM
    causal = iota((TOKENS, TOKENS), 1) >= iota((TOKENS, TOKENS), 0)
    for ref in (dsc_ref, dq_ref, dcum_ref, dskip_ref):
        ref[...] = jnp.zeros_like(ref)

    def backward(p, carry):
        cols = lanes(p)
        dy = dy_ref[:, cols]
        dh, dl = split(dy)
        both = jnp.concatenate([dh, dl], axis=1)
        twice = jnp.concatenate([dh, dh], axis=1)
        values = act_ref[:, cols]
        scaled = values * stepx_ref[:, cols]
        parts = []
        for i in range(2):
            h = 2 * p + i
            c = col_ref[h]
            e = jnp.exp(jnp.where(causal, cum_ref[h] - jnp.concatenate([c, c], axis=1), MASKED))
            wh, wl = split(turn_ref[...] * e)
            r = mm(wh, both, NN)
            parts.append(r[:, :128] + r[:, 128:] + mm(wl, dh, NN))
            own = first if i == 0 else jnp.logical_not(first)
            xh, xl = split(jnp.where(own, scaled, 0.0))
            dw = mm(jnp.concatenate([xh, xl], axis=1), twice, NT) + mm(xh, dl, NT)
            dsc_ref[...] += dw * e
        dx = jnp.where(first, parts[0], parts[1])
        dx_ref[:, cols] = dx
        dq_ref[...] += dot3(split(dy * expx_ref[:, cols]), split(read_state(ent_ref, p)), NT)
        skipped = dy * values
        dcum_ref[...] += head_sum(dy * scan_ref[:, cols] - skipped * table_ref[6:7, cols] - scaled * dx, p)
        dskip_ref[...] += head_sum(jnp.sum(skipped.reshape(TOKENS // 8, 8, 128), axis=0), p)
        return carry

    lax.fori_loop(0, PAIRS, backward, 0)
    out.received()
    scan_chunks(seq, True, recv, outgoing, coef)
    back = Scatter(seq, dp, outgoing, end_ref, sems, 2)
    back.start()
    cross.wait_recv()
    relay.start()
    dsc = dsc_ref[...]
    dk_ref[...] = dot3(split(dsc), query_s, NN)
    dq_ref[...] += dot3(split(jnp.transpose(dsc)), key_s, NN)
    near.wait_recv()
    for copy in lows:
        copy.wait_recv()
    relay.wait_recv()
    left = [jnp.transpose(block) for block in (low_ref[dp], lrecv[0], lrecv[1], lrecv[2])]
    right = [cot_ref, crecv.at[0], crecv.at[1], crecv.at[2]]
    for j in range(WIDTH // 256):
        total = mm(left[0], right[0][:, j * 256 : j * 256 + 256], NN)
        for k in range(1, DP):
            total = total + mm(left[k], right[k][:, j * 256 : j * 256 + 256], NN)
        for i in range(2):
            at = (2 * j + i) * ROWS
            part_ref[at : at + ROWS, :] = total[:, i * 128 : i * 128 + 128].astype(BF16)
    part_ref[10 * ROWS :, :] = jnp.zeros((SEQ * PIECE - 10 * ROWS, 128), BF16)
    back.received()
    for copy in [near, cross, relay, *lows]:
        copy.wait_send()
    out.sent()
    back.sent()


def last_kernel(
    x_ref, halo_ref, table_ref, act_ref, step_ref, ent_ref, end_ref, dy_ref, dx_ref, dq_ref, dk_ref, dcum_ref,
    dnorm_ref, dskip_ref, wide_ref,
    gin_ref, gstep_ref, gfilt_ref, gnorm_ref, ghead_ref, gweight_ref,
    ext_ref, dfilt_ref, stepx_ref, endx_ref, dact_ref, dstep_ref, zsum_ref, ded_ref, dkey_ref,
    tail_ref, ret_ref, rrecv, small_ref, srecv, sall, sown, sdp, wrecv, wall, wown, wacc, sems, dsems, hsems,
):
    seq, dp, partner, across = place()
    after, before = lax.rem(seq + 1, SEQ), lax.rem(seq + SEQ - 1, SEQ)
    greet(seq, dp, [(seq, lax.rem(dp + k, DP)) for k in range(1, DP)])
    spread = Scatter(seq, dp, wide_ref, wrecv, sems, 2)
    spread.start()

    raw, sizes, gain, rates, cums = rates_of(step_ref, table_ref)
    size_t = turned(sizes)
    end_t = turned(jnp.exp(cums[:, TOKENS - 1 :] - cums))
    for p in range(PAIRS):
        stepx_ref[:, p * 128 : p * 128 + 128] = widen(size_t, p)
        endx_ref[:, p * 128 : p * 128 + 128] = widen(end_t, p)
    key_s = split(act_ref[:, INNER : INNER + STATE])
    for ref in (dstep_ref, zsum_ref, ded_ref):
        ref[...] = jnp.zeros_like(ref)
    dkey_ref[...] = dk_ref[...]

    def pair(p, carry):
        cols = lanes(p)
        values = act_ref[:, cols]
        step = stepx_ref[:, cols]
        ending = endx_ref[:, cols]
        end = read_state(end_ref, p)
        end_s = split(end)
        z = dot3(key_s, end_s, NN) * ending
        dx = dx_ref[:, cols] + z
        dact_ref[:, cols] = dx * step + table_ref[6:7, cols] * dy_ref[:, cols]
        dstep_ref[...] += head_sum(dx * values, p)
        scaled = values * step
        zsum_ref[...] += head_sum(scaled * z, p)
        dkey_ref[...] += dot3(split(scaled * ending), end_s, NT)
        both = end * read_state(ent_ref, p)
        ded_ref[...] += head_sum(jnp.sum(both.reshape(STATE // 8, 8, 128), axis=0), p)
        return carry

    lax.fori_loop(0, PAIRS, pair, 0)
    dact_ref[:, INNER : INNER + STATE] = dkey_ref[...]
    dact_ref[:, INNER + STATE :] = dq_ref[...]
    dfilt_ref[0:8, :] = jnp.zeros((8, 128), F32)
    dfilt_ref[8 + TOKENS :, :] = jnp.zeros((8, 128), F32)
    small_ref[...] = jnp.zeros_like(small_ref)

    def filters(j, carry):
        cols = lanes(j)
        f = filtered_of(x_ref, table_ref, ext_ref, halo_ref[:, cols], cols)
        s = sigmoid(f)
        dfilt = dact_ref[:, cols] * (s * (1.0 + f * (1.0 - s)))
        dfilt_ref[8 : 8 + TOKENS, :] = dfilt
        dx = table_ref[TAPS - 1 : TAPS, cols] * dfilt
        back = table_ref[0:1, cols] * dfilt_ref[8:16, :]
        for k in range(TAPS):
            at = EDGE - TAPS + 1 + k
            small_ref[j, k : k + 1, :] = jnp.sum(dfilt * ext_ref[at : at + TOKENS, :], axis=0, keepdims=True)
            if k < TAPS - 1:
                dx = dx + table_ref[k : k + 1, cols] * dfilt_ref[11 - k : 11 - k + TOKENS, :]
            if 0 < k < TAPS - 1:
                back = back + table_ref[k : k + 1, cols] * dfilt_ref[8 - k : 16 - k, :]
        small_ref[j, TAPS : TAPS + 1, :] = jnp.sum(dfilt, axis=0, keepdims=True)
        gin_ref[:, cols] = dx.astype(BF16)
        tail_ref[:, cols] = dx[TOKENS - EDGE :, :]
        ret_ref[:, cols] = back
        return carry

    lax.fori_loop(0, CHANNELS // 128, filters, 0)
    halo = to_peer(ret_ref, rrecv, hsems.at[0], hsems.at[1], (before, dp))
    halo.start()
    zsum = zsum_ref[...]
    decays = jnp.exp(turned(cums)[TOKENS - 1 :, :])
    final = jnp.sum(zsum, axis=0, keepdims=True) + decays * jnp.sum(ded_ref[...], axis=0, keepdims=True)
    row = iota((TOKENS, 128), 0)
    dcum = dcum_ref[...] - zsum + jnp.where(row == TOKENS - 1, final, 0.0)
    shift = 1
    while shift < TOKENS:
        dcum = dcum + jnp.where(row < TOKENS - shift, pltpu.roll(dcum, TOKENS - shift, 0), 0.0)
        shift *= 2
    gain_t = turned(jnp.broadcast_to(gain, (HEADS, TOKENS)))
    draw = (dstep_ref[...] + dcum * gain_t) * turned(sigmoid(raw))
    gstep_ref[...] = jnp.transpose(draw)[:HEADS, :]
    for p in range(PAIRS):
        small_ref[p, 5:6, :] = dnorm_ref[:, p * 128 : p * 128 + 128]
    tiles = CHANNELS // 128
    small_ref[tiles, 0:1, :] = jnp.sum(draw, axis=0, keepdims=True)
    small_ref[tiles, 1:2, :] = jnp.sum(dcum * turned(rates), axis=0, keepdims=True)
    small_ref[tiles, 2:3, :] = jnp.sum(dskip_ref[...], axis=0, keepdims=True)
    narrow = Scatter(seq, dp, small_ref, srecv, sems, 0)
    narrow.start()

    spread.received()
    wacc[...] = jnp.zeros_like(wacc)

    def add(k, carry):
        wacc[...] += wrecv[k].astype(F32)
        return carry

    lax.fori_loop(0, SEQ, add, 0)
    wown[...] = wacc[...].astype(BF16)
    wide_all = Scatter(seq, dp, wown, wall, sems, 6, whole=True)
    wide_all.start()

    narrow.received()
    sdp[dp] = lax.fori_loop(0, SEQ, lambda k, total: total + srecv[k], jnp.zeros((8, 128), F32))

    def exchange(k, slot):
        return to_peer(sdp.at[dp], sdp.at[slot], dsems.at[0, k], dsems.at[1, slot], (seq, lax.rem(dp + k, DP)))

    for k in range(1, DP):
        exchange(k, dp).start()
    for k in range(1, DP):
        exchange(k, lax.rem(dp + k, DP)).wait_recv()
    sown[...] = sdp[0] + sdp[1] + sdp[2] + sdp[3]
    narrow_all = Scatter(seq, dp, sown, sall, sems, 4, whole=True)
    narrow_all.start()
    halo.wait_recv()
    fix = jnp.where(seq < SEQ - 1, rrecv[...], 0.0)
    zeros = jnp.zeros((EDGE - TAPS + 1, CHANNELS), F32)
    fix = jnp.concatenate([zeros, fix[: TAPS - 1, :]], axis=0)
    gin_ref[TOKENS - EDGE :, :] = (tail_ref[...] + fix).astype(BF16)
    narrow_all.received()
    for j in range(tiles):
        gfilt_ref[:, j * 128 : j * 128 + 128] = sall[j, 0 : TAPS + 1, :]
    for p in range(PAIRS):
        gnorm_ref[:, p * 128 : p * 128 + 128] = sall[p, 5:6, :]
    ghead_ref[...] = sall[tiles]
    wide_all.received()
    for j in range(WIDTH // 128):
        for c in range(ROWS // 16):
            chunk, at = divmod(j * ROWS + c * 16, PIECE)
            gweight_ref[c * 16 : c * 16 + 16, j * 128 : j * 128 + 128] = wall[chunk, at : at + 16, :].astype(F32)
    halo.wait_send()
    for k in range(1, DP):
        exchange(k, dp).wait_send()
    for scatter in (spread, narrow, wide_all, narrow_all):
        scatter.sent()


VMEM = pl.BlockSpec(memory_space=pltpu.VMEM)


def call(kernel, outs, scratch, args, collective, name):
    return pl.pallas_call(
        kernel,
        out_shape=[jax.ShapeDtypeStruct(shape, kind) for shape, kind in outs],
        in_specs=[VMEM] * len(args),
        out_specs=[VMEM] * len(outs),
        scratch_shapes=scratch,
        compiler_params=pltpu.CompilerParams(
            vmem_limit_bytes=62 * 2**20, collective_id=collective, has_side_effects=True
        ),
        name=name,
    )(*args)


def vmem(*shape, kind=F32):
    return pltpu.VMEM(shape, kind)


def padded(row):
    return jnp.pad(row, (0, CHANNELS - row.shape[0]))[None]


def body(
    conv_input, gate_input, step_input, filter_taps, filter_bias, step_bias, decay_log, skip_gain, norm_weight,
    output_weight, output_grad,
):
    raw_rows, gate_rows, step_rows, cotangent = conv_input[0], gate_input[0], step_input[0], output_grad[0]
    skips = jnp.broadcast_to(skip_gain[:, None], (HEADS, HEAD_DIM)).reshape(INNER)
    rows = [filter_taps, filter_bias[None], *map(padded, (norm_weight, skips, step_bias, decay_log))]
    table = jnp.concatenate([*rows, jnp.zeros((7, CHANNELS), F32)], axis=0)
    dma = pltpu.SemaphoreType.DMA
    wide, small, square = (TOKENS, INNER), (TOKENS, STATE), (TOKENS, TOKENS)
    chunks, states = (SEQ, 8, CHUNK), (SEQ, 8, HALF)
    scan = [vmem(*chunks), vmem(*chunks), vmem(*states), vmem(SEQ, 1, HALF)]
    columns = [vmem(HEADS, TOKENS, 128), vmem(HEADS, 1, TOKENS)]
    act, inside, normed_grad, entering, halo = call(
        forward_kernel,
        [((TOKENS, CHANNELS), F32), (wide, F32), (wide, F32), (states, F32), ((EDGE, CHANNELS), F32)],
        [vmem(EDGE, CHANNELS, kind=BF16), vmem(TOKENS + EDGE, 128), *scan, vmem(DP - 1, ROWS, WIDTH, kind=BF16),
         *columns, vmem(*wide), vmem(*square), dma((4, SEQ)), dma((6, 4)), dma((2,))],
        (raw_rows, table, step_rows, cotangent, output_weight),
        0, "forward",
    )
    gate_grad, dy, dx, dq, dk, dcum, dnorm, dskip, ending, partial = call(
        backward_kernel,
        [(wide, BF16), (wide, F32), (wide, F32), (small, F32), (small, F32), (small, F32), ((1, INNER), F32),
         ((8, 128), F32), (states, F32), ((SEQ * PIECE, 128), BF16)],
        [*scan, vmem(DP, TOKENS, ROWS, kind=BF16), vmem(DP - 1, TOKENS, ROWS, kind=BF16),
         vmem(DP - 1, TOKENS, WIDTH, kind=BF16), *columns, vmem(*wide), vmem(*wide), vmem(*square), vmem(*wide),
         vmem(*small), vmem(*square), dma((4, SEQ)), dma((4, DP - 1))],
        (act, gate_rows, table, step_rows, entering, inside, normed_grad, cotangent),
        1, "backward",
    )
    gin, gstep, gfilt, gnorm, ghead, gweight = call(
        last_kernel,
        [((TOKENS, CHANNELS), BF16), ((HEADS, TOKENS), F32), ((TAPS + 1, CHANNELS), F32), ((1, INNER), F32),
         ((8, 128), F32), ((ROWS, WIDTH), F32)],
        [vmem(TOKENS + EDGE, 128), vmem(TOKENS + 16, 128), vmem(*wide), vmem(*wide), vmem(TOKENS, CHANNELS),
         vmem(*small), vmem(*small), vmem(8, 128), vmem(*small), vmem(EDGE, CHANNELS), vmem(8, CHANNELS),
         vmem(8, CHANNELS), vmem(SEQ, 8, 128), vmem(SEQ, 8, 128), vmem(SEQ, 8, 128), vmem(8, 128), vmem(DP, 8, 128),
         vmem(SEQ, PIECE, 128, kind=BF16), vmem(SEQ, PIECE, 128, kind=BF16), vmem(PIECE, 128, kind=BF16),
         vmem(PIECE, 128), dma((8, SEQ)), dma((2, DP)), dma((2,))],
        (raw_rows, halo, table, act, step_rows, entering, ending, dy, dx, dq, dk, dcum, dnorm, dskip,
         partial.reshape(SEQ, PIECE, 128)),
        2, "last",
    )
    return gin[None], gate_grad[None], gstep[None], gweight, gfilt, gnorm[0], ghead[:3, :HEADS]


def solution(mesh):
    tokens, by_head, rows = P("dp", "seq", None), P("dp", None, "seq"), P("dp", None)
    return jax.shard_map(
        body,
        mesh=mesh,
        in_specs=(tokens, tokens, by_head, P(), P(), P(), P(), P(), P(), rows, tokens),
        out_specs=(tokens, tokens, by_head, rows, P(), P(), P()),
        check_vma=False,
    )
```

```python
import jax
import jax.numpy as jnp
from jax import lax
from jax.experimental import pallas as pl
from jax.experimental.pallas import tpu as pltpu
from jax.sharding import PartitionSpec as P

HEADS = 40
HEAD_DIM = 64
STATE = 128
INNER = 2560
CHANNELS = 2816
WIDTH = 1280
TOKENS = 256
TAPS = 4
PAIRS = 20
HALF = 1280
SEQ = 32
DP = 4
ROWS = INNER // DP
EDGE = 16
PIECE = 208
MASKED = -1e30
EPSILON = 1e-05

F32 = jnp.float32
BF16 = jnp.bfloat16
MESH = pl.DeviceIdType.MESH
NN = ((1,), (0,))
NT = ((1,), (1,))
TN = ((0,), (0,))


def mm(a, b, dims):
    return lax.dot_general(a, b, (dims, ((), ())), preferred_element_type=F32)


def split(x):
    high = x.astype(BF16)
    return high, (x - high.astype(F32)).astype(BF16)


def dot3(a, b, dims):
    return mm(a[0], b[0], dims) + mm(a[0], b[1], dims) + mm(a[1], b[0], dims)


def iota(shape, dim):
    return lax.broadcasted_iota(jnp.int32, shape, dim)


def lanes(p):
    return pl.ds(pl.multiple_of(p * 128, 128), 128)


def turned(x):
    return jnp.transpose(jnp.concatenate([x, jnp.zeros((128 - HEADS, TOKENS), F32)], axis=0))


def rates_of(step_ref, table_ref):
    columns = jnp.transpose(jnp.concatenate([table_ref[7:9, :128], jnp.zeros((126, 128), F32)], axis=0))
    raw = step_ref[...] + columns[:HEADS, 0:1]
    sizes = jnp.maximum(raw, 0.0) + jnp.log1p(jnp.exp(-jnp.abs(raw)))
    gain = -jnp.exp(columns[:HEADS, 1:2])
    rates = sizes * gain
    lane = iota(rates.shape, 1)
    cums = rates
    shift = 1
    while shift < TOKENS:
        cums = cums + jnp.where(lane >= shift, pltpu.roll(cums, shift, 1), 0.0)
        shift *= 2
    return raw, sizes, gain, rates, cums


def widen(columns, p):
    first = iota((TOKENS, 128), 1) < HEAD_DIM
    return jnp.where(first, columns[:, 2 * p : 2 * p + 1], columns[:, 2 * p + 1 : 2 * p + 2])


def head_sum(v, p):
    into = (iota((128, 128), 1) == 2 * p + iota((128, 128), 0) // HEAD_DIM).astype(BF16)
    high, low = split(v)
    return mm(high, into, NN) + mm(low, into, NN)


def sigmoid(x):
    return 1.0 / (1.0 + jnp.exp(-x))


def filtered_of(x_ref, table_ref, ext_ref, edge, cols):
    ext_ref[0:EDGE, :] = edge
    ext_ref[EDGE : EDGE + TOKENS, :] = x_ref[:, cols].astype(F32)
    total = table_ref[TAPS : TAPS + 1, cols]
    for k in range(TAPS):
        at = EDGE - TAPS + 1 + k
        total = total + table_ref[k : k + 1, cols] * ext_ref[at : at + TOKENS, :]
    return total


def write_state(pay_ref, p, state):
    half = p // (PAIRS // 2)
    at = lanes(p - half * (PAIRS // 2))
    for c in range(SEQ // 2):
        pay_ref[half * (SEQ // 2) + c, :, at] = state[c * 8 : c * 8 + 8, :]


def read_state(ref, p):
    half = p // (PAIRS // 2)
    at = lanes(p - half * (PAIRS // 2))
    return jnp.concatenate([ref[half * (SEQ // 2) + c, :, at] for c in range(SEQ // 2)], axis=0)


def to_peer(src, dst, send, recv, device):
    return pltpu.make_async_remote_copy(
        src_ref=src, dst_ref=dst, send_sem=send, recv_sem=recv, device_id=device, device_id_type=MESH
    )


def greet(seq, dp, others):
    barrier = pltpu.get_barrier_semaphore()

    def hello(i, carry):
        peer = lax.rem(seq + i, SEQ)
        pl.semaphore_signal(barrier, inc=1, device_id=(peer, dp), device_id_type=MESH)
        return carry

    lax.fori_loop(1, SEQ, hello, 0)
    for other in others:
        pl.semaphore_signal(barrier, inc=1, device_id=other, device_id_type=MESH)
    pl.semaphore_wait(barrier, SEQ - 1 + len(others))


def each_peer(seq, act):
    def step(i, carry):
        act(i, lax.rem(seq + i, SEQ))
        return carry

    lax.fori_loop(1, SEQ, step, 0)


class Scatter:
    def __init__(self, seq, dp, src, dst, sems, row, whole=False):
        self.seq, self.dp, self.src, self.dst, self.sems, self.row, self.whole = seq, dp, src, dst, sems, row, whole

    def copy(self, i, peer, slot):
        src = self.src if self.whole else self.src.at[peer]
        sems = self.sems
        return to_peer(src, self.dst.at[slot], sems.at[self.row, i], sems.at[self.row + 1, slot], (peer, self.dp))

    def start(self):
        each_peer(self.seq, lambda i, peer: self.copy(i, peer, self.seq).start())
        self.dst[self.seq] = self.src[...] if self.whole else self.src[self.seq]

    def received(self):
        each_peer(self.seq, lambda i, peer: self.copy(i, peer, peer).wait_recv())

    def sent(self):
        each_peer(self.seq, lambda i, peer: self.copy(i, peer, self.seq).wait_send())


def coefficients(seq, drecv, coef):
    decays = jnp.concatenate([drecv[k, 0:1, :] for k in range(SEQ)], axis=0)
    head = (seq // (SEQ // 2)) * (HEADS // 2) + iota((128, HALF), 1) // HEAD_DIM
    into = (iota((128, HALF), 0) == head).astype(F32)
    wide = lax.dot_general(
        decays, into, (NN, ((), ())), preferred_element_type=F32, precision=lax.Precision.HIGHEST
    )
    for k in range(SEQ):
        coef[k] = wide[k : k + 1, :]


def scan_chunks(reverse, recv, outgoing, coef):
    def scan(j, state):
        k = SEQ - 1 - j if reverse else j
        outgoing[k] = state.astype(outgoing.dtype)
        return coef[k] * state + recv[k].astype(F32)

    lax.fori_loop(0, SEQ, scan, jnp.zeros((8, HALF), F32))


def place():
    seq, dp = lax.axis_index("seq"), lax.axis_index("dp")
    partner = dp + 1 - 2 * lax.rem(dp, 2)
    across = lax.rem(dp + 2, DP)
    return seq, dp, partner, across


def kernel(
    x_ref, gate_ref, table_ref, step_ref, cot_ref, w_ref,
    gin_ref, ggate_ref, gstep_ref, gfilt_ref, gnorm_ref, ghead_ref, gweight_ref,
    edge_ref, halo_ref, ext_ref, dfilt_ref, act_ref, scan_ref, ng_ref, stepx_ref, expx_ref, col_ref, cum_ref,
    scores_ref, turn_ref, dsc_ref, acc_ref, dq_ref, dk_ref, dcum_ref, dskip_ref, dstep_ref, zsum_ref, ded_ref,
    drecv, down_ref, coef, pay_ref, recv, outgoing, ent_ref, pay2_ref, recv2, outgoing2, end_ref,
    wblocks, low_ref, lrecv, crecv, part_ref, wrecv, wall, wown, wacc,
    tail_ref, ret_ref, rrecv, small_ref, srecv, sall, sown, sdp, sems, wsems, dsems, hsems, xsems,
):
    seq, dp, partner, across = place()
    corner = DP - 1 - dp
    beside = seq + 4 - 8 * lax.rem(seq // 4, 2)
    after, before = lax.rem(seq + 1, SEQ), lax.rem(seq + SEQ - 1, SEQ)
    greet(seq, dp, [(seq, partner), (seq, across), (seq, corner), (beside, across)])
    last_rows = x_ref.at[pl.ds(TOKENS - EDGE, EDGE)]
    halo = to_peer(last_rows, edge_ref, hsems.at[0], hsems.at[1], (after, dp))
    halo.start()
    quarter = ROWS // 4

    def piece(q):
        return pl.ds(q * quarter, quarter)

    cross = [
        to_peer(w_ref.at[piece(q)], wblocks.at[1, piece(q)], wsems.at[0, q], wsems.at[1, q], (beside, across))
        for q in range(4)
    ]
    relay = [
        to_peer(wblocks.at[1, piece(q)], wblocks.at[2, piece(q)], wsems.at[2, q], wsems.at[3, q], (seq, partner))
        for q in range(4)
    ]
    near = to_peer(w_ref, wblocks.at[0], wsems.at[4, 0], wsems.at[5, 0], (seq, partner))
    for copy in cross:
        copy.start()
    near.start()
    raw, sizes, gain, rates, cums = rates_of(step_ref, table_ref)
    cum_t = turned(cums)
    size_t = turned(sizes)
    decays = jnp.exp(cum_t[TOKENS - 1 :, :])
    down_ref[...] = jnp.broadcast_to(decays, (8, 128))
    decay_all = Scatter(seq, dp, down_ref, drecv, sems, 0, whole=True)
    decay_all.start()
    to_end = turned(jnp.exp(cums[:, TOKENS - 1 :] - cums))
    end_t = to_end * size_t
    halo.wait_recv()
    halo_ref[...] = jnp.where(seq > 0, edge_ref[...].astype(F32), 0.0)

    def activate(j, carry):
        cols = lanes(j)
        f = filtered_of(x_ref, table_ref, ext_ref, halo_ref[:, cols], cols)
        act_ref[:, cols] = f * sigmoid(f)
        return carry

    lax.fori_loop(0, CHANNELS // 128, activate, 0)
    key = act_ref[:, INNER : INNER + STATE]
    key_turned = split(jnp.transpose(key))
    for p in range(PAIRS):
        a = act_ref[:, p * 128 : p * 128 + 128] * widen(end_t, p)
        write_state(pay_ref, p, dot3(key_turned, split(a), NN))
    out = Scatter(seq, dp, pay_ref, recv, sems, 2)
    out.start()

    exp_t = jnp.exp(cum_t)
    for h in range(HEADS):
        cum_ref[h] = cums[h : h + 1, :]
        col_ref[h] = jnp.broadcast_to(cum_t[:, h : h + 1], (TOKENS, 128))
    for p in range(PAIRS):
        stepx_ref[:, p * 128 : p * 128 + 128] = widen(size_t, p)
        expx_ref[:, p * 128 : p * 128 + 128] = widen(exp_t, p)
    query = act_ref[:, INNER + STATE :]
    key_s, query_s = split(key), split(query)
    query_turned = split(jnp.transpose(query))
    scores_ref[...] = dot3(query_s, key_s, NT)
    first = iota((TOKENS, 128), 1) < HEAD_DIM
    rows, columns = iota((TOKENS, TOKENS), 0), iota((TOKENS, TOKENS), 1)

    def inside(p, carry):
        cols = lanes(p)
        high, low = split(act_ref[:, cols] * stepx_ref[:, cols])
        both = jnp.concatenate([high, low], axis=1)
        parts = []
        for i in range(2):
            h = 2 * p + i
            c = col_ref[h]
            e = jnp.exp(jnp.where(rows >= columns, jnp.concatenate([c, c], axis=1) - cum_ref[h], MASKED))
            wh, wl = split(scores_ref[...] * e)
            r = mm(wh, both, NN)
            parts.append(r[:, :128] + r[:, 128:] + mm(wl, high, NN))
        scan_ref[:, cols] = jnp.where(first, parts[0], parts[1])
        return carry

    def normed_grad(block, weights):
        at = pl.multiple_of(block * ROWS, 128)
        ng_ref[:, pl.ds(at, ROWS)] = mm(cot_ref[...], weights[...], NT)

    lax.fori_loop(0, PAIRS, inside, 0)
    normed_grad(dp, w_ref)
    decay_all.received()
    coefficients(seq, drecv, coef)
    out.received()
    scan_chunks(False, recv, outgoing, coef)
    back = Scatter(seq, dp, outgoing, ent_ref, sems, 4)
    back.start()
    near.wait_recv()
    normed_grad(partner, wblocks.at[0])
    for q in range(4):
        cross[q].wait_recv()
        relay[q].start()
    cot_near = to_peer(cot_ref, crecv.at[0], dsems.at[0, 0], dsems.at[1, 0], (seq, partner))
    cot_cross = to_peer(cot_ref, crecv.at[1], dsems.at[0, 1], dsems.at[1, 1], (seq, across))
    cot_relay = to_peer(crecv.at[1], crecv.at[2], dsems.at[0, 2], dsems.at[1, 2], (seq, partner))
    cot_near.start()
    cot_cross.start()
    normed_grad(across, wblocks.at[1])
    turn_ref[...] = dot3(key_s, query_s, NT)
    for copy in relay:
        copy.wait_recv()
    normed_grad(corner, wblocks.at[2])
    for ref in (acc_ref, dsc_ref, dq_ref, dcum_ref, dskip_ref, dstep_ref, zsum_ref, ded_ref, small_ref):
        ref[...] = jnp.zeros_like(ref)
    back.received()

    def forward(p, carry):
        cols = lanes(p)
        carried = dot3(query_s, split(read_state(ent_ref, p)), NN) * expx_ref[:, cols]
        scanned = scan_ref[:, cols] + carried + table_ref[6:7, cols] * act_ref[:, cols]
        scan_ref[:, cols] = scanned
        gate = gate_ref[:, cols].astype(F32)
        gated = scanned * (gate * sigmoid(gate))
        acc_ref[...] += gated * gated
        return carry

    lax.fori_loop(0, PAIRS, forward, 0)
    inverse = lax.rsqrt(jnp.sum(acc_ref[...], axis=1, keepdims=True) / INNER + EPSILON)
    acc_ref[...] = jnp.zeros_like(acc_ref)

    def norm(p, carry):
        cols = lanes(p)
        gate = gate_ref[:, cols].astype(F32)
        gated = scan_ref[:, cols] * (gate * sigmoid(gate))
        weight = table_ref[5:6, cols]
        unit = gated * inverse
        block = p // 5
        low_ref[block, :, lanes(p - block * 5)] = (unit * weight).astype(BF16)
        ng = ng_ref[:, cols]
        small_ref[p, 5:6, :] = jnp.sum(ng * unit, axis=0, keepdims=True)
        acc_ref[...] += ng * weight * gated
        return carry

    lax.fori_loop(0, PAIRS, norm, 0)
    lows = [
        to_peer(low_ref.at[other], lrecv.at[k], dsems.at[2, k], dsems.at[3, k], (seq, other))
        for k, other in enumerate((partner, across, corner))
    ]
    for copy in lows:
        copy.start()
    lean = jnp.sum(acc_ref[...], axis=1, keepdims=True) * (inverse * inverse * inverse) / INNER

    def cotangents(p, carry):
        cols = lanes(p)
        gate = gate_ref[:, cols].astype(F32)
        sloped = sigmoid(gate)
        silu = gate * sloped
        scanned = scan_ref[:, cols]
        dgated = inverse * (ng_ref[:, cols] * table_ref[5:6, cols]) - scanned * silu * lean
        ggate_ref[:, cols] = (dgated * scanned * (sloped * (1.0 + gate * (1.0 - sloped)))).astype(BF16)
        dy = dgated * silu
        ng_ref[:, cols] = dy
        write_state(pay2_ref, p, dot3(query_turned, split(dy * expx_ref[:, cols]), NN))
        return carry

    lax.fori_loop(0, PAIRS, cotangents, 0)
    out2 = Scatter(seq, dp, pay2_ref, recv2, sems, 6)
    out2.start()

    def backward(p, carry):
        cols = lanes(p)
        dy = ng_ref[:, cols]
        dh, dl = split(dy)
        both = jnp.concatenate([dh, dl], axis=1)
        twice = jnp.concatenate([dh, dh], axis=1)
        values = act_ref[:, cols]
        scaled = values * stepx_ref[:, cols]
        parts = []
        for i in range(2):
            h = 2 * p + i
            c = col_ref[h]
            e = jnp.exp(jnp.where(columns >= rows, cum_ref[h] - jnp.concatenate([c, c], axis=1), MASKED))
            wh, wl = split(turn_ref[...] * e)
            r = mm(wh, both, NN)
            parts.append(r[:, :128] + r[:, 128:] + mm(wl, dh, NN))
            own = first if i == 0 else jnp.logical_not(first)
            xh, xl = split(jnp.where(own, scaled, 0.0))
            dw = mm(jnp.concatenate([xh, xl], axis=1), twice, NT) + mm(xh, dl, NT)
            dsc_ref[...] += dw * e
        dx = jnp.where(first, parts[0], parts[1])
        dq_ref[...] += dot3(split(dy * expx_ref[:, cols]), split(read_state(ent_ref, p)), NT)
        skipped = dy * values
        dcum_ref[...] += head_sum(dy * scan_ref[:, cols] - skipped * table_ref[6:7, cols] - scaled * dx, p)
        dskip_ref[...] += head_sum(jnp.sum(skipped.reshape(TOKENS // 8, 8, 128), axis=0), p)
        scan_ref[:, cols] = dx
        return carry

    lax.fori_loop(0, PAIRS, backward, 0)
    for p in range(PAIRS):
        expx_ref[:, p * 128 : p * 128 + 128] = widen(to_end, p)
    cot_cross.wait_recv()
    cot_relay.start()
    out2.received()
    scan_chunks(True, recv2, outgoing2, coef)
    back2 = Scatter(seq, dp, outgoing2, end_ref, sems, 8)
    back2.start()
    dsc = dsc_ref[...]
    dk_ref[...] = dot3(split(dsc), query_s, NN)
    dq_ref[...] += dot3(split(jnp.transpose(dsc)), key_s, NN)
    cot_near.wait_recv()
    for copy in lows:
        copy.wait_recv()
    cot_relay.wait_recv()
    left = [jnp.transpose(block) for block in (low_ref[dp], lrecv[0], lrecv[1], lrecv[2])]
    right = [cot_ref, crecv.at[0], crecv.at[1], crecv.at[2]]
    for j in range(WIDTH // 256):
        total = mm(left[0], right[0][:, j * 256 : j * 256 + 256], NN)
        for k in range(1, DP):
            total = total + mm(left[k], right[k][:, j * 256 : j * 256 + 256], NN)
        for i in range(2):
            for c in range(ROWS // 16):
                chunk, at = divmod((2 * j + i) * ROWS + c * 16, PIECE)
                part_ref[chunk, at : at + 16, :] = total[c * 16 : c * 16 + 16, i * 128 : i * 128 + 128].astype(BF16)
    for c in range(10 * ROWS, SEQ * PIECE, 16):
        chunk, at = divmod(c, PIECE)
        part_ref[chunk, at : at + 16, :] = jnp.zeros((16, 128), BF16)
    spread = Scatter(seq, dp, part_ref, wrecv, sems, 10)
    spread.start()
    back2.received()

    def pair(p, carry):
        cols = lanes(p)
        values = act_ref[:, cols]
        step = stepx_ref[:, cols]
        ending = expx_ref[:, cols]
        end = read_state(end_ref, p)
        end_s = split(end)
        z = dot3(key_s, end_s, NN) * ending
        dx = scan_ref[:, cols] + z
        act_ref[:, cols] = dx * step + table_ref[6:7, cols] * ng_ref[:, cols]
        dstep_ref[...] += head_sum(dx * values, p)
        scaled = values * step
        zsum_ref[...] += head_sum(scaled * z, p)
        dk_ref[...] += dot3(split(scaled * ending), end_s, NT)
        both = end * read_state(ent_ref, p)
        ded_ref[...] += head_sum(jnp.sum(both.reshape(STATE // 8, 8, 128), axis=0), p)
        return carry

    lax.fori_loop(0, PAIRS, pair, 0)
    act_ref[:, INNER : INNER + STATE] = dk_ref[...]
    act_ref[:, INNER + STATE :] = dq_ref[...]
    dfilt_ref[0:8, :] = jnp.zeros((8, 128), F32)
    dfilt_ref[8 + TOKENS :, :] = jnp.zeros((8, 128), F32)

    def filters(j, carry):
        cols = lanes(j)
        f = filtered_of(x_ref, table_ref, ext_ref, halo_ref[:, cols], cols)
        s = sigmoid(f)
        dfilt = act_ref[:, cols] * (s * (1.0 + f * (1.0 - s)))
        dfilt_ref[8 : 8 + TOKENS, :] = dfilt
        dx = table_ref[TAPS - 1 : TAPS, cols] * dfilt
        lead = table_ref[0:1, cols] * dfilt_ref[8:16, :]
        for k in range(TAPS):
            at = EDGE - TAPS + 1 + k
            small_ref[j, k : k + 1, :] = jnp.sum(dfilt * ext_ref[at : at + TOKENS, :], axis=0, keepdims=True)
            if k < TAPS - 1:
                dx = dx + table_ref[k : k + 1, cols] * dfilt_ref[11 - k : 11 - k + TOKENS, :]
            if 0 < k < TAPS - 1:
                lead = lead + table_ref[k : k + 1, cols] * dfilt_ref[8 - k : 16 - k, :]
        small_ref[j, TAPS : TAPS + 1, :] = jnp.sum(dfilt, axis=0, keepdims=True)
        gin_ref[:, cols] = dx.astype(BF16)
        tail_ref[:, cols] = dx[TOKENS - EDGE :, :]
        ret_ref[:, cols] = lead
        return carry

    lax.fori_loop(0, CHANNELS // 128, filters, 0)
    returned = to_peer(ret_ref, rrecv, hsems.at[2], hsems.at[3], (before, dp))
    returned.start()
    zsum = zsum_ref[...]
    final = jnp.sum(zsum, axis=0, keepdims=True) + decays * jnp.sum(ded_ref[...], axis=0, keepdims=True)
    row = iota((TOKENS, 128), 0)
    dcum = dcum_ref[...] - zsum + jnp.where(row == TOKENS - 1, final, 0.0)
    shift = 1
    while shift < TOKENS:
        dcum = dcum + jnp.where(row < TOKENS - shift, pltpu.roll(dcum, TOKENS - shift, 0), 0.0)
        shift *= 2
    gain_t = turned(jnp.broadcast_to(gain, (HEADS, TOKENS)))
    draw = (dstep_ref[...] + dcum * gain_t) * turned(sigmoid(raw))
    gstep_ref[...] = jnp.transpose(draw)[:HEADS, :]
    tiles = CHANNELS // 128
    small_ref[tiles, 0:1, :] = jnp.sum(draw, axis=0, keepdims=True)
    small_ref[tiles, 1:2, :] = jnp.sum(dcum * turned(rates), axis=0, keepdims=True)
    small_ref[tiles, 2:3, :] = jnp.sum(dskip_ref[...], axis=0, keepdims=True)
    narrow = Scatter(seq, dp, small_ref, srecv, sems, 14)
    narrow.start()

    spread.received()
    wacc[...] = jnp.zeros_like(wacc)

    def add(k, carry):
        wacc[...] += wrecv[k].astype(F32)
        return carry

    lax.fori_loop(0, SEQ, add, 0)
    wown[...] = wacc[...].astype(BF16)
    wide_all = Scatter(seq, dp, wown, wall, sems, 12, whole=True)
    wide_all.start()

    narrow.received()
    sdp[dp] = lax.fori_loop(0, SEQ, lambda k, total: total + srecv[k], jnp.zeros((8, 128), F32))

    def exchange(k, slot):
        return to_peer(sdp.at[dp], sdp.at[slot], xsems.at[0, k], xsems.at[1, slot], (seq, lax.rem(dp + k, DP)))

    for k in range(1, DP):
        exchange(k, dp).start()
    for k in range(1, DP):
        exchange(k, lax.rem(dp + k, DP)).wait_recv()
    sown[...] = sdp[0] + sdp[1] + sdp[2] + sdp[3]
    narrow_all = Scatter(seq, dp, sown, sall, sems, 16, whole=True)
    narrow_all.start()
    returned.wait_recv()
    fix = jnp.where(seq < SEQ - 1, rrecv[...], 0.0)
    zeros = jnp.zeros((EDGE - TAPS + 1, CHANNELS), F32)
    fix = jnp.concatenate([zeros, fix[: TAPS - 1, :]], axis=0)
    gin_ref[TOKENS - EDGE :, :] = (tail_ref[...] + fix).astype(BF16)
    narrow_all.received()
    for j in range(tiles):
        gfilt_ref[:, j * 128 : j * 128 + 128] = sall[j, 0 : TAPS + 1, :]
    for p in range(PAIRS):
        gnorm_ref[:, p * 128 : p * 128 + 128] = sall[p, 5:6, :]
    ghead_ref[...] = sall[tiles]
    wide_all.received()
    for j in range(WIDTH // 128):
        for c in range(ROWS // 16):
            chunk, at = divmod(j * ROWS + c * 16, PIECE)
            gweight_ref[c * 16 : c * 16 + 16, j * 128 : j * 128 + 128] = wall[chunk, at : at + 16, :]
    for copy in [halo, near, *cross, *relay, cot_near, cot_cross, cot_relay, *lows, returned]:
        copy.wait_send()
    for k in range(1, DP):
        exchange(k, dp).wait_send()
    for scatter in (decay_all, out, back, out2, back2, spread, narrow, wide_all, narrow_all):
        scatter.sent()


VMEM = pl.BlockSpec(memory_space=pltpu.VMEM)


def vmem(*shape, kind=F32):
    return pltpu.VMEM(shape, kind)


def padded(row):
    return jnp.pad(row, (0, CHANNELS - row.shape[0]))[None]


SENT = F32


def body(
    conv_input, gate_input, step_input, filter_taps, filter_bias, step_bias, decay_log, skip_gain, norm_weight,
    output_weight, output_grad,
):
    skips = jnp.broadcast_to(skip_gain[:, None], (HEADS, HEAD_DIM)).reshape(INNER)
    rows = [filter_taps, filter_bias[None], *map(padded, (norm_weight, skips, step_bias, decay_log))]
    table = jnp.concatenate([*rows, jnp.zeros((7, CHANNELS), F32)], axis=0)
    args = (conv_input[0], gate_input[0], table, step_input[0], output_grad[0], output_weight)
    dma = pltpu.SemaphoreType.DMA
    wide, small, square = (TOKENS, INNER), (TOKENS, STATE), (TOKENS, TOKENS)
    states, pieces, tiles = (SEQ, 8, HALF), (SEQ, PIECE, 128), (SEQ, 8, 128)
    scan = [vmem(*states, kind=SENT)] * 4
    outs = [
        ((TOKENS, CHANNELS), BF16), (wide, BF16), ((HEADS, TOKENS), F32), ((TAPS + 1, CHANNELS), F32),
        ((1, INNER), F32), ((8, 128), F32), ((ROWS, WIDTH), BF16),
    ]
    gin, ggate, gstep, gfilt, gnorm, ghead, gweight = pl.pallas_call(
        kernel,
        out_shape=[jax.ShapeDtypeStruct(shape, kind) for shape, kind in outs],
        in_specs=[VMEM] * len(args),
        out_specs=[VMEM] * len(outs),
        scratch_shapes=[
            vmem(EDGE, CHANNELS, kind=BF16), vmem(EDGE, CHANNELS), vmem(TOKENS + EDGE, 128), vmem(TOKENS + 16, 128),
            vmem(TOKENS, CHANNELS), vmem(*wide), vmem(*wide), vmem(*wide), vmem(*wide),
            vmem(HEADS, TOKENS, 128), vmem(HEADS, 1, TOKENS), vmem(*square), vmem(*square), vmem(*square),
            *[vmem(*small)] * 4, vmem(8, 128), *[vmem(*small)] * 2, vmem(8, 128),
            vmem(*tiles), vmem(8, 128), vmem(SEQ, 1, HALF), *scan, *scan,
            vmem(DP - 1, ROWS, WIDTH, kind=BF16), vmem(DP, TOKENS, ROWS, kind=BF16),
            vmem(DP - 1, TOKENS, ROWS, kind=BF16), vmem(DP - 1, TOKENS, WIDTH, kind=BF16),
            *[vmem(*pieces, kind=BF16)] * 3, vmem(PIECE, 128, kind=BF16), vmem(PIECE, 128),
            vmem(EDGE, CHANNELS), *[vmem(8, CHANNELS)] * 2, *[vmem(*tiles)] * 3, vmem(8, 128), vmem(DP, 8, 128),
            dma((18, SEQ)), dma((6, 4)), dma((4, DP - 1)), dma((4,)), dma((2, DP)),
        ],
        compiler_params=pltpu.CompilerParams(
            vmem_limit_bytes=63 * 2**20, collective_id=0, has_side_effects=True
        ),
        name="layer_backward",
    )(*args)
    return gin[None], ggate[None], gstep[None], gweight.astype(F32), gfilt, gnorm[0], ghead[:3, :HEADS]


def solution(mesh):
    tokens, by_head, rows = P("dp", "seq", None), P("dp", None, "seq"), P("dp", None)
    return jax.shard_map(
        body,
        mesh=mesh,
        in_specs=(tokens, tokens, by_head, P(), P(), P(), P(), P(), P(), rows, tokens),
        out_specs=(tokens, tokens, by_head, rows, P(), P(), P()),
        check_vma=False,
    )
```

```python
import jax
import jax.numpy as jnp
from jax import lax
from jax.experimental import pallas as pl
from jax.experimental.pallas import tpu as pltpu
from jax.sharding import PartitionSpec as P

HEADS = 40
HEAD_DIM = 64
STATE = 128
INNER = 2560
CHANNELS = 2816
WIDTH = 1280
TOKENS = 256
TAPS = 4
PAIRS = 20
GROUPS = 4
EACH = PAIRS // GROUPS
SPREAD = INNER // GROUPS
BAND = 16
BANDS = STATE // BAND
SEQ = 32
DP = 4
ROWS = INNER // DP
EDGE = 16
PIECE = 208
MASKED = -1e30
EPSILON = 1e-05

F32 = jnp.float32
BF16 = jnp.bfloat16
MESH = pl.DeviceIdType.MESH
NN = ((1,), (0,))
NT = ((1,), (1,))
TN = ((0,), (0,))


def mm(a, b, dims):
    return lax.dot_general(a, b, (dims, ((), ())), preferred_element_type=F32)


def split(x):
    high = x.astype(BF16)
    return high, (x - high.astype(F32)).astype(BF16)


def dot3(a, b, dims):
    return mm(a[0], b[0], dims) + mm(a[0], b[1], dims) + mm(a[1], b[0], dims)


def iota(shape, dim):
    return lax.broadcasted_iota(jnp.int32, shape, dim)


def lanes(p):
    return pl.ds(pl.multiple_of(p * 128, 128), 128)


def turned(x):
    return jnp.transpose(jnp.concatenate([x, jnp.zeros((128 - HEADS, TOKENS), F32)], axis=0))


def rates_of(step_ref, heads_ref):
    columns = jnp.transpose(jnp.pad(heads_ref[...], ((0, 125), (0, 128 - HEADS))))
    raw = step_ref[...] + columns[:HEADS, 0:1]
    sizes = jnp.maximum(raw, 0.0) + jnp.log1p(jnp.exp(-jnp.abs(raw)))
    gain = -jnp.exp(columns[:HEADS, 1:2])
    rates = sizes * gain
    lane = iota(rates.shape, 1)
    cums = rates
    shift = 1
    while shift < TOKENS:
        cums = cums + jnp.where(lane >= shift, pltpu.roll(cums, shift, 1), 0.0)
        shift *= 2
    return raw, sizes, gain, rates, cums


def widen(columns, p):
    first = iota((TOKENS, 128), 1) < HEAD_DIM
    return jnp.where(first, columns[:, 2 * p : 2 * p + 1], columns[:, 2 * p + 1 : 2 * p + 2])


def head_sum(v, p):
    into = (iota((128, 128), 1) == 2 * p + iota((128, 128), 0) // HEAD_DIM).astype(BF16)
    high, low = split(v)
    return mm(high, into, NN) + mm(low, into, NN)


def sigmoid(x):
    return 1.0 / (1.0 + jnp.exp(-x))


def filtered_of(x_ref, table_ref, ext_ref, edge, cols):
    ext_ref[0:EDGE, :] = edge
    ext_ref[EDGE : EDGE + TOKENS, :] = x_ref[:, cols].astype(F32)
    total = table_ref[TAPS : TAPS + 1, cols]
    for k in range(TAPS):
        at = EDGE - TAPS + 1 + k
        total = total + table_ref[k : k + 1, cols] * ext_ref[at : at + TOKENS, :]
    return total


def write_state(pay_ref, p, state):
    group = p // EACH
    at = lanes(p - group * EACH)
    for c in range(BANDS):
        pay_ref[group * BANDS + c, :, at] = state[c * BAND : c * BAND + BAND, :]


def read_state(ref, p):
    group = p // EACH
    at = lanes(p - group * EACH)
    return jnp.concatenate([ref[group * BANDS + c, :, at] for c in range(BANDS)], axis=0)


def to_peer(src, dst, send, recv, device):
    return pltpu.make_async_remote_copy(
        src_ref=src, dst_ref=dst, send_sem=send, recv_sem=recv, device_id=device, device_id_type=MESH
    )


def greet(seq, dp, others):
    barrier = pltpu.get_barrier_semaphore()

    def hello(i, carry):
        peer = lax.rem(seq + i, SEQ)
        pl.semaphore_signal(barrier, inc=1, device_id=(peer, dp), device_id_type=MESH)
        return carry

    lax.fori_loop(1, SEQ, hello, 0)
    for other in others:
        pl.semaphore_signal(barrier, inc=1, device_id=other, device_id_type=MESH)
    return lambda: pl.semaphore_wait(barrier, SEQ - 1 + len(others))


def each_peer(seq, act):
    def step(i, carry):
        act(i, lax.rem(seq + i, SEQ))
        return carry

    lax.fori_loop(1, SEQ, step, 0)


class Scatter:
    def __init__(self, seq, dp, src, dst, sems, row, whole=False, pick=lambda peer: peer):
        self.seq, self.dp, self.src, self.dst, self.sems, self.row = seq, dp, src, dst, sems, row
        self.whole, self.pick = whole, pick

    def copy(self, i, peer, slot):
        src = self.src if self.whole else self.src.at[self.pick(peer)]
        sems = self.sems
        return to_peer(src, self.dst.at[slot], sems.at[self.row, i], sems.at[self.row + 1, slot], (peer, self.dp))

    def keep(self):
        self.dst[self.seq] = self.src[...] if self.whole else self.src[self.pick(self.seq)]

    def start(self):
        each_peer(self.seq, lambda i, peer: self.copy(i, peer, self.seq).start())
        self.keep()

    def received(self):
        each_peer(self.seq, lambda i, peer: self.copy(i, peer, peer).wait_recv())

    def sent(self):
        each_peer(self.seq, lambda i, peer: self.copy(i, peer, self.seq).wait_send())

    def in_group(self, group, act):
        def step(c, carry):
            peer = group * BANDS + c

            @pl.when(peer != self.seq)
            def _():
                act(lax.rem(peer - self.seq + SEQ, SEQ), peer)

            return carry

        lax.fori_loop(0, BANDS, step, 0)

    def start_group(self, group):
        self.in_group(group, lambda i, peer: self.copy(i, peer, self.seq).start())

    def received_group(self, group):
        self.in_group(group, lambda i, peer: self.copy(i, peer, peer).wait_recv())


def coefficients(seq, drecv, coef):
    decays = jnp.concatenate([drecv[k, 0:1, :] for k in range(SEQ)], axis=0)
    head = (seq // BANDS) * (HEADS // GROUPS) + iota((128, SPREAD), 1) // HEAD_DIM
    into = (iota((128, SPREAD), 0) == head).astype(F32)
    wide = lax.dot_general(
        decays, into, (NN, ((), ())), preferred_element_type=F32, precision=lax.Precision.HIGHEST
    )
    for k in range(SEQ):
        coef[k] = wide[k : k + 1, :]


def scan_chunks(reverse, recv, outgoing, coef):
    def scan(j, state):
        k = SEQ - 1 - j if reverse else j
        outgoing[k] = state.astype(outgoing.dtype)
        return coef[k] * state + recv[k].astype(F32)

    lax.fori_loop(0, SEQ, scan, jnp.zeros((BAND, SPREAD), F32))


def place():
    seq, dp = lax.axis_index("seq"), lax.axis_index("dp")
    partner = dp + 1 - 2 * lax.rem(dp, 2)
    across = lax.rem(dp + 2, DP)
    return seq, dp, partner, across


def kernel(
    x_ref, gate_ref, taps_ref, fbias_ref, weight_ref, heads_ref, step_ref, cot_ref, w_ref,
    gin_ref, ggate_ref, gstep_ref, gfilt_ref, gnorm_ref, ghead_ref, gweight_ref,
    table_ref, edge_ref, halo_ref, ext_ref, dfilt_ref, act_ref, scan_ref, ng_ref, stepx_ref, expx_ref, col_ref, cum_ref,
    scores_ref, turn_ref, dsc_ref, acc_ref, dq_ref, dk_ref, dcum_ref, dskip_ref, dstep_ref, zsum_ref, ded_ref,
    drecv, down_ref, coef, pay_ref, recv, outgoing, ent_ref, pay2_ref, recv2, outgoing2, end_ref,
    wblocks, low_ref, lrecv, crecv, part_ref, wrecv, wall, wown, wacc,
    tail_ref, ret_ref, rrecv, small_ref, srecv, sall, sown, sdp, sems, wsems, dsems, hsems, xsems,
):
    seq, dp, partner, across = place()
    corner = DP - 1 - dp
    beside = seq + 4 - 8 * lax.rem(seq // 4, 2)
    after, before = lax.rem(seq + 1, SEQ), lax.rem(seq + SEQ - 1, SEQ)
    met = greet(seq, dp, [(seq, partner), (seq, across), (seq, corner), (beside, across), (beside, corner)])
    table_ref[0:TAPS, :] = taps_ref[...]
    for j in range(CHANNELS // 128):
        table_ref[TAPS : TAPS + 1, j * 128 : j * 128 + 128] = fbias_ref[j * 128 : j * 128 + 128].reshape(1, 128)
    low_half = iota((1, 128), 1) < HEAD_DIM
    for p in range(PAIRS):
        at = slice(p * 128, p * 128 + 128)
        table_ref[5:6, at] = weight_ref[at].reshape(1, 128)
        skips = heads_ref[2:3, 2 * p : 2 * p + 2]
        table_ref[6:7, at] = jnp.where(low_half, skips[:, 0:1], skips[:, 1:2])
    raw, sizes, gain, rates, cums = rates_of(step_ref, heads_ref)
    cum_t = turned(cums)
    size_t = turned(sizes)
    decays = jnp.exp(cum_t[TOKENS - 1 :, :])
    down_ref[...] = jnp.broadcast_to(decays, (8, 128))
    met()
    last_rows = x_ref.at[pl.ds(TOKENS - EDGE, EDGE)]
    halo = to_peer(last_rows, edge_ref, hsems.at[0], hsems.at[1], (after, dp))
    halo.start()
    quarter = ROWS // 4

    def piece(q):
        return pl.ds(q * quarter, quarter)

    cross = [
        to_peer(w_ref.at[piece(q)], wblocks.at[1, piece(q)], wsems.at[0, q], wsems.at[1, q], (beside, across))
        for q in range(4)
    ]
    relay = [
        to_peer(wblocks.at[1, piece(q)], wblocks.at[2, piece(q)], wsems.at[2, q], wsems.at[3, q], (seq, partner))
        for q in range(4)
    ]
    near = to_peer(w_ref, wblocks.at[0], wsems.at[4, 0], wsems.at[5, 0], (seq, partner))
    for copy in cross:
        copy.start()
    near.start()
    decay_all = Scatter(seq, dp, down_ref, drecv, sems, 0, whole=True)
    decay_all.start()
    to_end = turned(jnp.exp(cums[:, TOKENS - 1 :] - cums))
    end_t = to_end * size_t
    halo.wait_recv()
    halo_ref[...] = jnp.where(seq > 0, edge_ref[...].astype(F32), 0.0)

    def activate(j, carry):
        cols = lanes(j)
        f = filtered_of(x_ref, table_ref, ext_ref, halo_ref[:, cols], cols)
        act_ref[:, cols] = f * sigmoid(f)
        return carry

    lax.fori_loop(0, CHANNELS // 128, activate, 0, unroll=2)
    key = act_ref[:, INNER : INNER + STATE]
    key_turned = split(jnp.transpose(key))
    out = Scatter(seq, dp, pay_ref, recv, sems, 2)
    for p in range(PAIRS):
        a = act_ref[:, p * 128 : p * 128 + 128] * widen(end_t, p)
        write_state(pay_ref, p, dot3(key_turned, split(a), NN))
        if p % EACH == EACH - 1:
            out.start_group(p // EACH)
    out.keep()

    exp_t = jnp.exp(cum_t)
    for h in range(HEADS):
        cum_ref[h] = cums[h : h + 1, :]
        col_ref[h] = jnp.broadcast_to(cum_t[:, h : h + 1], (TOKENS, 128))
    for p in range(PAIRS):
        stepx_ref[:, p * 128 : p * 128 + 128] = widen(size_t, p)
        expx_ref[:, p * 128 : p * 128 + 128] = widen(exp_t, p)
    query = act_ref[:, INNER + STATE :]
    key_s, query_s = split(key), split(query)
    query_turned = split(jnp.transpose(query))
    scores_ref[...] = dot3(query_s, key_s, NT)
    first = iota((TOKENS, 128), 1) < HEAD_DIM
    rows, columns = iota((TOKENS, TOKENS), 0), iota((TOKENS, TOKENS), 1)

    def inside(p, carry):
        cols = lanes(p)
        high, low = split(act_ref[:, cols] * stepx_ref[:, cols])
        both = jnp.concatenate([high, low], axis=1)
        parts = []
        for i in range(2):
            h = 2 * p + i
            c = col_ref[h]
            e = jnp.exp(jnp.where(rows >= columns, jnp.concatenate([c, c], axis=1) - cum_ref[h], MASKED))
            wh, wl = split(scores_ref[...] * e)
            r = mm(wh, both, NN)
            parts.append(r[:, :128] + r[:, 128:] + mm(wl, high, NN))
        scan_ref[:, cols] = jnp.where(first, parts[0], parts[1])
        return carry

    def normed_grad(block, weights):
        at = pl.multiple_of(block * ROWS, 128)
        ng_ref[:, pl.ds(at, ROWS)] = mm(cot_ref[...], weights[...], NT)

    lax.fori_loop(0, PAIRS, inside, 0)
    normed_grad(dp, w_ref)
    decay_all.received()
    coefficients(seq, drecv, coef)
    out.received()
    scan_chunks(False, recv, outgoing, coef)
    back = Scatter(seq, dp, outgoing, ent_ref, sems, 4)
    back.start()
    near.wait_recv()
    normed_grad(partner, wblocks.at[0])
    for q in range(4):
        cross[q].wait_recv()
        relay[q].start()
    cot_near = to_peer(cot_ref, crecv.at[0], dsems.at[0, 0], dsems.at[1, 0], (seq, partner))
    cot_cross = to_peer(cot_ref, crecv.at[1], dsems.at[0, 1], dsems.at[1, 1], (beside, across))
    cot_relay = to_peer(crecv.at[1], crecv.at[2], dsems.at[0, 2], dsems.at[1, 2], (seq, partner))
    cot_near.start()
    cot_cross.start()
    normed_grad(across, wblocks.at[1])
    turn_ref[...] = dot3(key_s, query_s, NT)
    for copy in relay:
        copy.wait_recv()
    normed_grad(corner, wblocks.at[2])
    for ref in (acc_ref, dsc_ref, dq_ref, dcum_ref, dskip_ref, dstep_ref, zsum_ref, ded_ref, small_ref):
        ref[...] = jnp.zeros_like(ref)
    decay_all.sent()
    out.sent()

    def forward(p, carry):
        cols = lanes(p)
        carried = dot3(query_s, split(read_state(ent_ref, p)), NN) * expx_ref[:, cols]
        scanned = scan_ref[:, cols] + carried + table_ref[6:7, cols] * act_ref[:, cols]
        scan_ref[:, cols] = scanned
        gate = gate_ref[:, cols].astype(F32)
        gated = scanned * (gate * sigmoid(gate))
        acc_ref[...] += gated * gated
        return carry

    for turn in (0, 1, 3, 2):
        group = lax.rem(seq // BANDS + turn, GROUPS)
        back.received_group(group)
        lax.fori_loop(0, EACH, lambda i, carry: forward(group * EACH + i, carry), 0, unroll=EACH)
    inverse = lax.rsqrt(jnp.sum(acc_ref[...], axis=1, keepdims=True) / INNER + EPSILON)
    acc_ref[...] = jnp.zeros_like(acc_ref)

    def norm(p, carry):
        cols = lanes(p)
        gate = gate_ref[:, cols].astype(F32)
        gated = scan_ref[:, cols] * (gate * sigmoid(gate))
        weight = table_ref[5:6, cols]
        unit = gated * inverse
        block = p // 5
        low_ref[block, :, lanes(p - block * 5)] = (unit * weight).astype(BF16)
        ng = ng_ref[:, cols]
        small_ref[p, 5:6, :] = jnp.sum(ng * unit, axis=0, keepdims=True)
        acc_ref[...] += ng * weight * gated
        return carry

    lax.fori_loop(0, PAIRS, norm, 0, unroll=2)
    lows = [
        to_peer(low_ref.at[other], lrecv.at[k], dsems.at[2, k], dsems.at[3, k], (at, other))
        for k, (at, other) in enumerate(((seq, partner), (beside, across), (beside, corner)))
    ]
    for copy in lows:
        copy.start()
    lean = jnp.sum(acc_ref[...], axis=1, keepdims=True) * (inverse * inverse * inverse) / INNER

    def cotangents(p, carry):
        cols = lanes(p)
        gate = gate_ref[:, cols].astype(F32)
        sloped = sigmoid(gate)
        silu = gate * sloped
        scanned = scan_ref[:, cols]
        dgated = inverse * (ng_ref[:, cols] * table_ref[5:6, cols]) - scanned * silu * lean
        ggate_ref[:, cols] = (dgated * scanned * (sloped * (1.0 + gate * (1.0 - sloped)))).astype(BF16)
        dy = dgated * silu
        ng_ref[:, cols] = dy
        write_state(pay2_ref, p, dot3(query_turned, split(dy * expx_ref[:, cols]), NN))
        return carry

    out2 = Scatter(seq, dp, pay2_ref, recv2, sems, 6)
    for turn in (2, 1, 3, 0):
        group = lax.rem(seq // BANDS + turn, GROUPS)
        lax.fori_loop(0, EACH, lambda i, carry: cotangents(group * EACH + i, carry), 0, unroll=EACH)
        out2.start_group(group)
    out2.keep()

    def backward(p, carry):
        cols = lanes(p)
        dy = ng_ref[:, cols]
        dh, dl = split(dy)
        both = jnp.concatenate([dh, dl], axis=1)
        twice = jnp.concatenate([dh, dh], axis=1)
        values = act_ref[:, cols]
        scaled = values * stepx_ref[:, cols]
        parts = []
        for i in range(2):
            h = 2 * p + i
            c = col_ref[h]
            e = jnp.exp(jnp.where(columns >= rows, cum_ref[h] - jnp.concatenate([c, c], axis=1), MASKED))
            wh, wl = split(turn_ref[...] * e)
            r = mm(wh, both, NN)
            parts.append(r[:, :128] + r[:, 128:] + mm(wl, dh, NN))
            own = first if i == 0 else jnp.logical_not(first)
            xh, xl = split(jnp.where(own, scaled, 0.0))
            dw = mm(jnp.concatenate([xh, xl], axis=1), twice, NT) + mm(xh, dl, NT)
            dsc_ref[...] += dw * e
        dx = jnp.where(first, parts[0], parts[1])
        dq_ref[...] += dot3(split(dy * expx_ref[:, cols]), split(read_state(ent_ref, p)), NT)
        skipped = dy * values
        dcum_ref[...] += head_sum(dy * scan_ref[:, cols] - skipped * table_ref[6:7, cols] - scaled * dx, p)
        dskip_ref[...] += head_sum(jnp.sum(skipped.reshape(TOKENS // 8, 8, 128), axis=0), p)
        scan_ref[:, cols] = dx
        return carry

    lax.fori_loop(0, PAIRS, backward, 0)
    for p in range(PAIRS):
        expx_ref[:, p * 128 : p * 128 + 128] = widen(to_end, p)
    cot_cross.wait_recv()
    cot_relay.start()
    back.sent()
    out2.received()
    scan_chunks(True, recv2, outgoing2, coef)
    back2 = Scatter(seq, dp, outgoing2, end_ref, sems, 8)
    back2.start()
    dsc = dsc_ref[...]
    dk_ref[...] = dot3(split(dsc), query_s, NN)
    dq_ref[...] += dot3(split(jnp.transpose(dsc)), key_s, NN)
    cot_near.wait_recv()
    for copy in lows:
        copy.wait_recv()
    cot_relay.wait_recv()
    left = [jnp.transpose(block) for block in (low_ref[dp], lrecv[0], lrecv[1], lrecv[2])]
    right = [cot_ref, crecv.at[0], crecv.at[1], crecv.at[2]]
    for j in range(WIDTH // 256):
        total = mm(left[0], right[0][:, j * 256 : j * 256 + 256], NN)
        for k in range(1, DP):
            total = total + mm(left[k], right[k][:, j * 256 : j * 256 + 256], NN)
        for i in range(2):
            for c in range(ROWS // 16):
                chunk, at = divmod((2 * j + i) * ROWS + c * 16, PIECE)
                part_ref[chunk, at : at + 16, :] = total[c * 16 : c * 16 + 16, i * 128 : i * 128 + 128].astype(BF16)
    for c in range(10 * ROWS, SEQ * PIECE, 16):
        chunk, at = divmod(c, PIECE)
        part_ref[chunk, at : at + 16, :] = jnp.zeros((16, 128), BF16)
    spread = Scatter(seq, dp, part_ref, wrecv, sems, 10)
    out2.sent()
    back2.received()
    spread.start()

    def pair(p, carry):
        cols = lanes(p)
        values = act_ref[:, cols]
        step = stepx_ref[:, cols]
        ending = expx_ref[:, cols]
        end = read_state(end_ref, p)
        end_s = split(end)
        z = dot3(key_s, end_s, NN) * ending
        dx = scan_ref[:, cols] + z
        act_ref[:, cols] = dx * step + table_ref[6:7, cols] * ng_ref[:, cols]
        dstep_ref[...] += head_sum(dx * values, p)
        scaled = values * step
        zsum_ref[...] += head_sum(scaled * z, p)
        dk_ref[...] += dot3(split(scaled * ending), end_s, NT)
        both = end * read_state(ent_ref, p)
        ded_ref[...] += head_sum(jnp.sum(both.reshape(STATE // 8, 8, 128), axis=0), p)
        return carry

    lax.fori_loop(0, PAIRS, pair, 0, unroll=2)
    act_ref[:, INNER : INNER + STATE] = dk_ref[...]
    act_ref[:, INNER + STATE :] = dq_ref[...]
    dfilt_ref[0:8, :] = jnp.zeros((8, 128), F32)
    dfilt_ref[8 + TOKENS :, :] = jnp.zeros((8, 128), F32)

    def filters(j, carry):
        cols = lanes(j)
        f = filtered_of(x_ref, table_ref, ext_ref, halo_ref[:, cols], cols)
        s = sigmoid(f)
        dfilt = act_ref[:, cols] * (s * (1.0 + f * (1.0 - s)))
        dfilt_ref[8 : 8 + TOKENS, :] = dfilt
        dx = table_ref[TAPS - 1 : TAPS, cols] * dfilt
        lead = table_ref[0:1, cols] * dfilt_ref[8:16, :]
        for k in range(TAPS):
            at = EDGE - TAPS + 1 + k
            small_ref[j, k : k + 1, :] = jnp.sum(dfilt * ext_ref[at : at + TOKENS, :], axis=0, keepdims=True)
            if k < TAPS - 1:
                dx = dx + table_ref[k : k + 1, cols] * dfilt_ref[11 - k : 11 - k + TOKENS, :]
            if 0 < k < TAPS - 1:
                lead = lead + table_ref[k : k + 1, cols] * dfilt_ref[8 - k : 16 - k, :]
        small_ref[j, TAPS : TAPS + 1, :] = jnp.sum(dfilt, axis=0, keepdims=True)
        gin_ref[:, cols] = dx.astype(BF16)
        tail_ref[:, cols] = dx[TOKENS - EDGE :, :]
        ret_ref[:, cols] = lead
        return carry

    lax.fori_loop(0, CHANNELS // 128, filters, 0, unroll=2)
    returned = to_peer(ret_ref, rrecv, hsems.at[2], hsems.at[3], (before, dp))
    returned.start()
    zsum = zsum_ref[...]
    final = jnp.sum(zsum, axis=0, keepdims=True) + decays * jnp.sum(ded_ref[...], axis=0, keepdims=True)
    row = iota((TOKENS, 128), 0)
    dcum = dcum_ref[...] - zsum + jnp.where(row == TOKENS - 1, final, 0.0)
    shift = 1
    while shift < TOKENS:
        dcum = dcum + jnp.where(row < TOKENS - shift, pltpu.roll(dcum, TOKENS - shift, 0), 0.0)
        shift *= 2
    gain_t = turned(jnp.broadcast_to(gain, (HEADS, TOKENS)))
    draw = (dstep_ref[...] + dcum * gain_t) * turned(sigmoid(raw))
    gstep_ref[...] = jnp.transpose(draw)[:HEADS, :]
    tiles = CHANNELS // 128
    small_ref[tiles, 0:1, :] = jnp.sum(draw, axis=0, keepdims=True)
    small_ref[tiles, 1:2, :] = jnp.sum(dcum * turned(rates), axis=0, keepdims=True)
    small_ref[tiles, 2:3, :] = jnp.sum(dskip_ref[...], axis=0, keepdims=True)
    def pick(peer):
        return peer + (4 - 8 * lax.rem(peer // 4, 2)) * (dp // 2)

    narrow = Scatter(seq, dp, small_ref, srecv, sems, 14, pick=pick)
    narrow.start()

    spread.received()
    wacc[...] = jnp.zeros_like(wacc)

    def add(k, carry):
        wacc[...] += wrecv[k].astype(F32)
        return carry

    lax.fori_loop(0, SEQ, add, 0)
    wown[...] = wacc[...].astype(BF16)
    wide_all = Scatter(seq, dp, wown, wall, sems, 12, whole=True)
    wide_all.start()

    back2.sent()
    spread.sent()
    narrow.received()
    sdp[dp] = lax.fori_loop(0, SEQ, lambda k, total: total + srecv[k], jnp.zeros((8, 128), F32))

    others = ((seq, partner), (beside, across), (beside, corner))

    def exchange(k, slot):
        return to_peer(sdp.at[dp], sdp.at[slot], xsems.at[0, k], xsems.at[1, slot], others[k])

    for k in range(DP - 1):
        exchange(k, dp).start()
    for k in range(DP - 1):
        exchange(k, others[k][1]).wait_recv()
    sown[...] = sdp[0] + sdp[1] + sdp[2] + sdp[3]
    narrow_all = Scatter(seq, dp, sown, sall, sems, 16, whole=True)
    narrow_all.start()
    returned.wait_recv()
    fix = jnp.where(seq < SEQ - 1, rrecv[...], 0.0)
    zeros = jnp.zeros((EDGE - TAPS + 1, CHANNELS), F32)
    fix = jnp.concatenate([zeros, fix[: TAPS - 1, :]], axis=0)
    gin_ref[TOKENS - EDGE :, :] = (tail_ref[...] + fix).astype(BF16)
    narrow_all.received()
    for j in range(tiles):
        gfilt_ref[:, j * 128 : j * 128 + 128] = sall[pick(j), 0 : TAPS + 1, :]
    for p in range(PAIRS):
        gnorm_ref[p * 128 : p * 128 + 128] = sall[pick(p), 5, :]
    ghead_ref[...] = sall[pick(tiles), 0:3, 0:HEADS]
    wide_all.received()
    for j in range(WIDTH // 128):
        for c in range(ROWS // 16):
            chunk, at = divmod(j * ROWS + c * 16, PIECE)
            gweight_ref[c * 16 : c * 16 + 16, j * 128 : j * 128 + 128] = wall[chunk, at : at + 16, :].astype(F32)
    for copy in [halo, near, *cross, *relay, cot_near, cot_cross, cot_relay, *lows, returned]:
        copy.wait_send()
    for k in range(DP - 1):
        exchange(k, dp).wait_send()
    for scatter in (narrow, wide_all, narrow_all):
        scatter.sent()


VMEM = pl.BlockSpec(memory_space=pltpu.VMEM)


def vmem(*shape, kind=F32):
    return pltpu.VMEM(shape, kind)


SENT = F32


def body(
    conv_input, gate_input, step_input, filter_taps, filter_bias, step_bias, decay_log, skip_gain, norm_weight,
    output_weight, output_grad,
):
    heads = jnp.stack([step_bias, decay_log, skip_gain])
    args = (conv_input[0], gate_input[0], filter_taps, filter_bias, norm_weight, heads, step_input[0], output_grad[0], output_weight)
    dma = pltpu.SemaphoreType.DMA
    wide, small, square = (TOKENS, INNER), (TOKENS, STATE), (TOKENS, TOKENS)
    states, pieces, tiles = (SEQ, BAND, SPREAD), (SEQ, PIECE, 128), (SEQ, 8, 128)
    scan = [vmem(*states, kind=SENT)] * 4
    outs = [
        ((TOKENS, CHANNELS), BF16), (wide, BF16), ((HEADS, TOKENS), F32), ((TAPS + 1, CHANNELS), F32),
        ((INNER,), F32), ((3, HEADS), F32), ((ROWS, WIDTH), F32),
    ]
    gin, ggate, gstep, gfilt, gnorm, ghead, gweight = pl.pallas_call(
        kernel,
        out_shape=[jax.ShapeDtypeStruct(shape, kind) for shape, kind in outs],
        in_specs=[VMEM] * len(args),
        out_specs=[VMEM] * len(outs),
        scratch_shapes=[
            vmem(8, CHANNELS), vmem(EDGE, CHANNELS, kind=BF16), vmem(EDGE, CHANNELS), vmem(TOKENS + EDGE, 128), vmem(TOKENS + 16, 128),
            vmem(TOKENS, CHANNELS), vmem(*wide), vmem(*wide), vmem(*wide), vmem(*wide),
            vmem(HEADS, TOKENS, 128), vmem(HEADS, 1, TOKENS), vmem(*square), vmem(*square), vmem(*square),
            *[vmem(*small)] * 4, vmem(8, 128), *[vmem(*small)] * 2, vmem(8, 128),
            vmem(*tiles), vmem(8, 128), vmem(SEQ, 1, SPREAD), *scan, *scan,
            vmem(DP - 1, ROWS, WIDTH, kind=BF16), vmem(DP, TOKENS, ROWS, kind=BF16),
            vmem(DP - 1, TOKENS, ROWS, kind=BF16), vmem(DP - 1, TOKENS, WIDTH, kind=BF16),
            *[vmem(*pieces, kind=BF16)] * 3, vmem(PIECE, 128, kind=BF16), vmem(PIECE, 128),
            vmem(EDGE, CHANNELS), *[vmem(8, CHANNELS)] * 2, *[vmem(*tiles)] * 3, vmem(8, 128), vmem(DP, 8, 128),
            dma((18, SEQ)), dma((6, 4)), dma((4, DP - 1)), dma((4,)), dma((2, DP)),
        ],
        compiler_params=pltpu.CompilerParams(
            vmem_limit_bytes=63 * 2**20, collective_id=0, has_side_effects=True
        ),
        name="layer_backward",
    )(*args)
    return gin[None], ggate[None], gstep[None], gweight, gfilt, gnorm, ghead


def solution(mesh):
    tokens, by_head, rows = P("dp", "seq", None), P("dp", None, "seq"), P("dp", None)
    return jax.shard_map(
        body,
        mesh=mesh,
        in_specs=(tokens, tokens, by_head, P(), P(), P(), P(), P(), P(), rows, tokens),
        out_specs=(tokens, tokens, by_head, rows, P(), P(), P()),
        check_vma=False,
    )
```

```python
import jax
import jax.numpy as jnp
from jax import lax
from jax.experimental import pallas as pl
from jax.experimental.pallas import tpu as pltpu
from jax.sharding import PartitionSpec as P

HEADS = 40
HEAD_DIM = 64
STATE = 128
INNER = 2560
CHANNELS = 2816
WIDTH = 1280
TOKENS = 256
TAPS = 4
PAIRS = 20
GROUPS = 4
EACH = PAIRS // GROUPS
SPREAD = INNER // GROUPS
BAND = 16
BANDS = STATE // BAND
SEQ = 32
DP = 4
ROWS = INNER // DP
EDGE = 16
FIRST = 112
PIECE = 208
MASKED = -1e30
EPSILON = 1e-05

F32 = jnp.float32
BF16 = jnp.bfloat16
MESH = pl.DeviceIdType.MESH
NN = ((1,), (0,))
NT = ((1,), (1,))
TN = ((0,), (0,))


def mm(a, b, dims):
    return lax.dot_general(a, b, (dims, ((), ())), preferred_element_type=F32)


def split(x):
    high = x.astype(BF16)
    return high, (x - high.astype(F32)).astype(BF16)


def dot3(a, b, dims):
    return mm(a[0], b[0], dims) + mm(a[0], b[1], dims) + mm(a[1], b[0], dims)


def iota(shape, dim):
    return lax.broadcasted_iota(jnp.int32, shape, dim)


def lanes(p):
    return pl.ds(pl.multiple_of(p * 128, 128), 128)


def turned(x):
    return jnp.transpose(jnp.concatenate([x, jnp.zeros((128 - HEADS, TOKENS), F32)], axis=0))


def rates_of(step_ref, heads_ref):
    columns = jnp.transpose(jnp.pad(heads_ref[...], ((0, 125), (0, 128 - HEADS))))
    raw = step_ref[...] + columns[:HEADS, 0:1]
    sizes = jnp.maximum(raw, 0.0) + jnp.log1p(jnp.exp(-jnp.abs(raw)))
    gain = -jnp.exp(columns[:HEADS, 1:2])
    rates = sizes * gain
    lane = iota(rates.shape, 1)
    cums = rates
    shift = 1
    while shift < TOKENS:
        cums = cums + jnp.where(lane >= shift, pltpu.roll(cums, shift, 1), 0.0)
        shift *= 2
    return raw, sizes, gain, rates, cums


def widen(columns, p):
    first = iota((TOKENS, 128), 1) < HEAD_DIM
    return jnp.where(first, columns[:, 2 * p : 2 * p + 1], columns[:, 2 * p + 1 : 2 * p + 2])


def head_sum(v, p):
    into = (iota((128, 128), 1) == 2 * p + iota((128, 128), 0) // HEAD_DIM).astype(BF16)
    high, low = split(v)
    return mm(high, into, NN) + mm(low, into, NN)


def sigmoid(x):
    return 1.0 / (1.0 + jnp.exp(-x))


def filtered_of(x_ref, table_ref, ext_ref, edge, cols, count=TOKENS):
    ext_ref[0:EDGE, :] = jnp.broadcast_to(edge, (EDGE, 128))
    ext_ref[EDGE : EDGE + count, :] = x_ref[0:count, cols].astype(F32)
    total = table_ref[TAPS : TAPS + 1, cols]
    for k in range(TAPS):
        at = EDGE - TAPS + 1 + k
        total = total + table_ref[k : k + 1, cols] * ext_ref[at : at + count, :]
    return total


def write_state(pay_ref, p, state):
    group = p // EACH
    at = lanes(p - group * EACH)
    for c in range(BANDS):
        pay_ref[group * BANDS + c, :, at] = state[c * BAND : c * BAND + BAND, :]


def read_state(ref, p):
    group = p // EACH
    at = lanes(p - group * EACH)
    return jnp.concatenate([ref[group * BANDS + c, :, at] for c in range(BANDS)], axis=0)


def to_peer(src, dst, send, recv, device):
    return pltpu.make_async_remote_copy(
        src_ref=src, dst_ref=dst, send_sem=send, recv_sem=recv, device_id=device, device_id_type=MESH
    )


def greet(seq, dp, others):
    barrier = pltpu.get_barrier_semaphore()

    def hello(i, carry):
        peer = lax.rem(seq + i, SEQ)
        pl.semaphore_signal(barrier, inc=1, device_id=(peer, dp), device_id_type=MESH)
        return carry

    lax.fori_loop(1, SEQ, hello, 0)
    for other in others:
        pl.semaphore_signal(barrier, inc=1, device_id=other, device_id_type=MESH)
    return lambda: pl.semaphore_wait(barrier, SEQ - 1 + len(others))


def each_peer(seq, act):
    def step(i, carry):
        act(i, lax.rem(seq + i, SEQ))
        return carry

    lax.fori_loop(1, SEQ, step, 0)


class Scatter:
    def __init__(self, seq, dp, src, dst, sems, row, whole=False, pick=lambda peer: peer):
        self.seq, self.dp, self.src, self.dst, self.sems, self.row = seq, dp, src, dst, sems, row
        self.whole, self.pick = whole, pick

    def copy(self, i, peer, slot):
        src = self.src if self.whole else self.src.at[self.pick(peer)]
        sems = self.sems
        return to_peer(src, self.dst.at[slot], sems.at[self.row, i], sems.at[self.row + 1, slot], (peer, self.dp))

    def keep(self):
        self.dst[self.seq] = self.src[...] if self.whole else self.src[self.pick(self.seq)]

    def start(self):
        each_peer(self.seq, lambda i, peer: self.copy(i, peer, self.seq).start())
        self.keep()

    def received(self):
        each_peer(self.seq, lambda i, peer: self.copy(i, peer, peer).wait_recv())

    def sent(self):
        each_peer(self.seq, lambda i, peer: self.copy(i, peer, self.seq).wait_send())

    def in_group(self, group, act):
        def step(c, carry):
            peer = group * BANDS + c

            @pl.when(peer != self.seq)
            def _():
                act(lax.rem(peer - self.seq + SEQ, SEQ), peer)

            return carry

        lax.fori_loop(0, BANDS, step, 0)

    def start_group(self, group):
        self.in_group(group, lambda i, peer: self.copy(i, peer, self.seq).start())

    def received_group(self, group):
        self.in_group(group, lambda i, peer: self.copy(i, peer, peer).wait_recv())


class Tree:
    def __init__(self, a, y, c, dp, device_of, buf, sems):
        self.a, self.y, self.c, self.dp, self.device_of, self.buf, self.sems = a, y, c, dp, device_of, buf, sems

    def copy(self, leg, k, arriving):
        a, y, c = self.a, self.y, self.c
        if leg == 0:
            other, mine = lax.rem(a + k, 4), a
            device, base, size = self.device_of(other, y, c), c * 8 + y * 4 + (other if arriving else mine), 1
        elif leg == 1:
            other, mine = 1 - y, y
            device, base, size = self.device_of(a, other, c), c * 8 + (other if arriving else mine) * 4, 4
        else:
            other, mine = lax.rem(c + k, 4), c
            device, base, size = self.device_of(a, y, other), (other if arriving else mine) * 8, 8
        part = self.buf.at[pl.ds(base, size)]
        recv = self.sems.at[2 * leg + 1, other if arriving else mine]
        return to_peer(part, part, self.sems.at[2 * leg, k], recv, (device, self.dp))

    def counts(self, leg):
        return (1,) if leg == 1 else (1, 2, 3)

    def start(self, leg):
        for k in self.counts(leg):
            self.copy(leg, k, False).start()

    def received(self, leg):
        for k in self.counts(leg):
            self.copy(leg, k, True).wait_recv()

    def sent(self):
        for leg in range(3):
            for k in self.counts(leg):
                self.copy(leg, k, False).wait_send()


def coefficients(seq, drecv, coef):
    decays = jnp.concatenate([drecv[k, 0:1, :] for k in range(SEQ)], axis=0)
    head = (seq // BANDS) * (HEADS // GROUPS) + iota((128, SPREAD), 1) // HEAD_DIM
    into = (iota((128, SPREAD), 0) == head).astype(F32)
    wide = lax.dot_general(
        decays, into, (NN, ((), ())), preferred_element_type=F32, precision=lax.Precision.HIGHEST
    )
    for k in range(SEQ):
        coef[k] = wide[k : k + 1, :]


def scan_chunks(reverse, recv, outgoing, coef):
    def scan(j, state):
        k = SEQ - 1 - j if reverse else j
        outgoing[k] = state.astype(outgoing.dtype)
        return coef[k] * state + recv[k].astype(F32)

    lax.fori_loop(0, SEQ, scan, jnp.zeros((BAND, SPREAD), F32))


def place():
    seq, dp = lax.axis_index("seq"), lax.axis_index("dp")
    partner = dp + 1 - 2 * lax.rem(dp, 2)
    across = lax.rem(dp + 2, DP)
    return seq, dp, partner, across


def kernel(
    x_ref, gate_ref, taps_ref, fbias_ref, weight_ref, heads_ref, step_ref, cot_ref, w_ref,
    gin_ref, ggate_ref, gstep_ref, gfilt_ref, gnorm_ref, ghead_ref, wall, wall2,
    table_ref, edge_ref, halo_ref, ext_ref, dfilt_ref, act_ref, scan_ref, ng_ref, stepx_ref, expx_ref, col_ref, cum_ref,
    scores_ref, turn_ref, dsc_ref, acc_ref, dq_ref, dk_ref, dcum_ref, dskip_ref, dstep_ref, zsum_ref, ded_ref,
    drecv, down_ref, coef, pay_ref, recv, outgoing, ent_ref, pay2_ref, recv2, outgoing2, end_ref,
    wblocks, low_ref, lrecv, crecv, part_ref, wrecv, wacc,
    tail_ref, ret_ref, rrecv, small_ref, srecv, sall, sown, sdp, sems, wsems, dsems, hsems, xsems, tsems,
):
    seq, dp, partner, across = place()
    corner = DP - 1 - dp
    beside = seq + 4 - 8 * lax.rem(seq // 4, 2)
    after, before = lax.rem(seq + 1, SEQ), lax.rem(seq + SEQ - 1, SEQ)
    met = greet(seq, dp, [(seq, partner), (seq, across), (seq, corner), (beside, across), (beside, corner)])
    table_ref[0:TAPS, :] = taps_ref[...]
    for j in range(CHANNELS // 128):
        table_ref[TAPS : TAPS + 1, j * 128 : j * 128 + 128] = fbias_ref[j * 128 : j * 128 + 128].reshape(1, 128)
    low_half = iota((1, 128), 1) < HEAD_DIM
    for p in range(PAIRS):
        at = slice(p * 128, p * 128 + 128)
        table_ref[5:6, at] = weight_ref[at].reshape(1, 128)
        skips = heads_ref[2:3, 2 * p : 2 * p + 2]
        table_ref[6:7, at] = jnp.where(low_half, skips[:, 0:1], skips[:, 1:2])
    raw, sizes, gain, rates, cums = rates_of(step_ref, heads_ref)
    cum_t = turned(cums)
    size_t = turned(sizes)
    decays = jnp.exp(cum_t[TOKENS - 1 :, :])
    down_ref[...] = jnp.broadcast_to(decays, (8, 128))
    met()
    last_rows = x_ref.at[pl.ds(TOKENS - EDGE, EDGE)]
    halo = to_peer(last_rows, edge_ref, hsems.at[0], hsems.at[1], (after, dp))
    halo.start()
    quarter = ROWS // 4

    def piece(q):
        return pl.ds(q * quarter, quarter)

    cross = [
        to_peer(w_ref.at[piece(q)], wblocks.at[1, piece(q)], wsems.at[0, q], wsems.at[1, q], (beside, across))
        for q in range(4)
    ]
    relay = [
        to_peer(wblocks.at[1, piece(q)], wblocks.at[2, piece(q)], wsems.at[2, q], wsems.at[3, q], (seq, partner))
        for q in range(4)
    ]
    near = to_peer(w_ref, wblocks.at[0], wsems.at[4, 0], wsems.at[5, 0], (seq, partner))
    for copy in cross:
        copy.start()
    near.start()
    decay_all = Scatter(seq, dp, down_ref, drecv, sems, 0, whole=True)
    decay_all.start()
    to_end = turned(jnp.exp(cums[:, TOKENS - 1 :] - cums))
    end_t = to_end * size_t

    def activate(j, carry):
        cols = lanes(j)
        f = filtered_of(x_ref, table_ref, ext_ref, 0.0, cols)
        act_ref[:, cols] = f * sigmoid(f)
        return carry

    def mend(j, carry):
        cols = lanes(j)
        f = filtered_of(x_ref, table_ref, ext_ref, halo_ref[:, cols], cols, EDGE)
        act_ref[0:EDGE, cols] = f * sigmoid(f)
        return carry

    lax.fori_loop(0, CHANNELS // 128, activate, 0, unroll=2)
    halo.wait_recv()
    halo_ref[...] = jnp.where(seq > 0, edge_ref[...].astype(F32), 0.0)
    lax.fori_loop(0, CHANNELS // 128, mend, 0, unroll=11)
    key = act_ref[:, INNER : INNER + STATE]
    key_turned = split(jnp.transpose(key))
    out = Scatter(seq, dp, pay_ref, recv, sems, 2)
    for p in range(PAIRS):
        a = act_ref[:, p * 128 : p * 128 + 128] * widen(end_t, p)
        write_state(pay_ref, p, dot3(key_turned, split(a), NN))
        if p % EACH == EACH - 1:
            out.start_group(p // EACH)
    out.keep()

    exp_t = jnp.exp(cum_t)
    for h in range(HEADS):
        cum_ref[h] = cums[h : h + 1, :]
        col_ref[h] = jnp.broadcast_to(cum_t[:, h : h + 1], (TOKENS, 128))
    for p in range(PAIRS):
        stepx_ref[:, p * 128 : p * 128 + 128] = widen(size_t, p)
        expx_ref[:, p * 128 : p * 128 + 128] = widen(exp_t, p)
    query = act_ref[:, INNER + STATE :]
    key_s, query_s = split(key), split(query)
    query_turned = split(jnp.transpose(query))
    scores_ref[...] = dot3(query_s, key_s, NT)
    first = iota((TOKENS, 128), 1) < HEAD_DIM
    rows, columns = iota((TOKENS, TOKENS), 0), iota((TOKENS, TOKENS), 1)

    def inside(p, carry):
        cols = lanes(p)
        high, low = split(act_ref[:, cols] * stepx_ref[:, cols])
        both = jnp.concatenate([high, low], axis=1)
        parts = []
        for i in range(2):
            h = 2 * p + i
            c = col_ref[h]
            e = jnp.exp(jnp.where(rows >= columns, jnp.concatenate([c, c], axis=1) - cum_ref[h], MASKED))
            wh, wl = split(scores_ref[...] * e)
            r = mm(wh, both, NN)
            parts.append(r[:, :128] + r[:, 128:] + mm(wl, high, NN))
        scan_ref[:, cols] = jnp.where(first, parts[0], parts[1])
        return carry

    def normed_grad(block, weights):
        at = pl.multiple_of(block * ROWS, 128)
        ng_ref[:, pl.ds(at, ROWS)] = mm(cot_ref[...], weights[...], NT)

    lax.fori_loop(0, PAIRS, inside, 0)
    normed_grad(dp, w_ref)
    decay_all.received()
    coefficients(seq, drecv, coef)
    out.received()
    scan_chunks(False, recv, outgoing, coef)
    back = Scatter(seq, dp, outgoing, ent_ref, sems, 4)
    back.start()
    near.wait_recv()
    normed_grad(partner, wblocks.at[0])
    for q in range(4):
        cross[q].wait_recv()
        relay[q].start()
    cot_near = to_peer(cot_ref, crecv.at[0], dsems.at[0, 0], dsems.at[1, 0], (seq, partner))
    cot_cross = to_peer(cot_ref, crecv.at[1], dsems.at[0, 1], dsems.at[1, 1], (beside, across))
    cot_relay = to_peer(crecv.at[1], crecv.at[2], dsems.at[0, 2], dsems.at[1, 2], (seq, partner))
    cot_near.start()
    cot_cross.start()
    normed_grad(across, wblocks.at[1])
    turn_ref[...] = dot3(key_s, query_s, NT)
    for copy in relay:
        copy.wait_recv()
    normed_grad(corner, wblocks.at[2])
    for ref in (acc_ref, dsc_ref, dq_ref, dcum_ref, dskip_ref, dstep_ref, zsum_ref, ded_ref, small_ref):
        ref[...] = jnp.zeros_like(ref)
    decay_all.sent()
    out.sent()

    def forward(p, carry):
        cols = lanes(p)
        carried = dot3(query_s, split(read_state(ent_ref, p)), NN) * expx_ref[:, cols]
        scanned = scan_ref[:, cols] + carried + table_ref[6:7, cols] * act_ref[:, cols]
        scan_ref[:, cols] = scanned
        gate = gate_ref[:, cols].astype(F32)
        gated = scanned * (gate * sigmoid(gate))
        acc_ref[...] += gated * gated
        return carry

    for turn in (0, 1, 3, 2):
        group = lax.rem(seq // BANDS + turn, GROUPS)
        back.received_group(group)
        lax.fori_loop(0, EACH, lambda i, carry: forward(group * EACH + i, carry), 0, unroll=EACH)
    inverse = lax.rsqrt(jnp.sum(acc_ref[...], axis=1, keepdims=True) / INNER + EPSILON)
    acc_ref[...] = jnp.zeros_like(acc_ref)

    def norm(p, carry):
        cols = lanes(p)
        gate = gate_ref[:, cols].astype(F32)
        gated = scan_ref[:, cols] * (gate * sigmoid(gate))
        weight = table_ref[5:6, cols]
        unit = gated * inverse
        block = p // 5
        low_ref[block, :, lanes(p - block * 5)] = (unit * weight).astype(BF16)
        ng = ng_ref[:, cols]
        small_ref[p, 5:6, :] = jnp.sum(ng * unit, axis=0, keepdims=True)
        acc_ref[...] += ng * weight * gated
        return carry

    lax.fori_loop(0, PAIRS, norm, 0, unroll=2)
    lows = [
        to_peer(low_ref.at[other], lrecv.at[k], dsems.at[2, k], dsems.at[3, k], (at, other))
        for k, (at, other) in enumerate(((seq, partner), (beside, across), (beside, corner)))
    ]
    for copy in lows:
        copy.start()
    lean = jnp.sum(acc_ref[...], axis=1, keepdims=True) * (inverse * inverse * inverse) / INNER

    def cotangents(p, carry):
        cols = lanes(p)
        gate = gate_ref[:, cols].astype(F32)
        sloped = sigmoid(gate)
        silu = gate * sloped
        scanned = scan_ref[:, cols]
        dgated = inverse * (ng_ref[:, cols] * table_ref[5:6, cols]) - scanned * silu * lean
        ggate_ref[:, cols] = (dgated * scanned * (sloped * (1.0 + gate * (1.0 - sloped)))).astype(BF16)
        dy = dgated * silu
        ng_ref[:, cols] = dy
        write_state(pay2_ref, p, dot3(query_turned, split(dy * expx_ref[:, cols]), NN))
        return carry

    out2 = Scatter(seq, dp, pay2_ref, recv2, sems, 6)
    for turn in (2, 1, 3, 0):
        group = lax.rem(seq // BANDS + turn, GROUPS)
        lax.fori_loop(0, EACH, lambda i, carry: cotangents(group * EACH + i, carry), 0, unroll=EACH)
        out2.start_group(group)
    out2.keep()

    def backward(p, carry):
        cols = lanes(p)
        dy = ng_ref[:, cols]
        dh, dl = split(dy)
        both = jnp.concatenate([dh, dl], axis=1)
        twice = jnp.concatenate([dh, dh], axis=1)
        values = act_ref[:, cols]
        scaled = values * stepx_ref[:, cols]
        parts = []
        for i in range(2):
            h = 2 * p + i
            c = col_ref[h]
            e = jnp.exp(jnp.where(columns >= rows, cum_ref[h] - jnp.concatenate([c, c], axis=1), MASKED))
            wh, wl = split(turn_ref[...] * e)
            r = mm(wh, both, NN)
            parts.append(r[:, :128] + r[:, 128:] + mm(wl, dh, NN))
            own = first if i == 0 else jnp.logical_not(first)
            xh, xl = split(jnp.where(own, scaled, 0.0))
            dw = mm(jnp.concatenate([xh, xl], axis=1), twice, NT) + mm(xh, dl, NT)
            dsc_ref[...] += dw * e
        dx = jnp.where(first, parts[0], parts[1])
        dq_ref[...] += dot3(split(dy * expx_ref[:, cols]), split(read_state(ent_ref, p)), NT)
        skipped = dy * values
        dcum_ref[...] += head_sum(dy * scan_ref[:, cols] - skipped * table_ref[6:7, cols] - scaled * dx, p)
        dskip_ref[...] += head_sum(jnp.sum(skipped.reshape(TOKENS // 8, 8, 128), axis=0), p)
        scan_ref[:, cols] = dx
        return carry

    lax.fori_loop(0, PAIRS, backward, 0)
    for p in range(PAIRS):
        expx_ref[:, p * 128 : p * 128 + 128] = widen(to_end, p)
    cot_cross.wait_recv()
    cot_relay.start()
    back.sent()
    out2.received()
    scan_chunks(True, recv2, outgoing2, coef)
    back2 = Scatter(seq, dp, outgoing2, end_ref, sems, 8)
    back2.start()
    dsc = dsc_ref[...]
    dk_ref[...] = dot3(split(dsc), query_s, NN)
    dq_ref[...] += dot3(split(jnp.transpose(dsc)), key_s, NN)
    cot_near.wait_recv()
    for copy in lows:
        copy.wait_recv()
    cot_relay.wait_recv()
    left = [jnp.transpose(block) for block in (low_ref[dp], lrecv[0], lrecv[1], lrecv[2])]
    right = [cot_ref, crecv.at[0], crecv.at[1], crecv.at[2]]
    for j in range(WIDTH // 256):
        total = mm(left[0], right[0][:, j * 256 : j * 256 + 256], NN)
        for k in range(1, DP):
            total = total + mm(left[k], right[k][:, j * 256 : j * 256 + 256], NN)
        for i in range(2):
            for c in range(ROWS // 16):
                chunk, at = divmod((2 * j + i) * ROWS + c * 16, PIECE)
                part_ref[chunk, at : at + 16, :] = total[c * 16 : c * 16 + 16, i * 128 : i * 128 + 128].astype(BF16)
    for c in range(10 * ROWS, SEQ * PIECE, 16):
        chunk, at = divmod(c, PIECE)
        part_ref[chunk, at : at + 16, :] = jnp.zeros((16, 128), BF16)
    spread = Scatter(seq, dp, part_ref, wrecv, sems, 10)
    out2.sent()
    back2.received()
    spread.start()

    def pair(p, carry):
        cols = lanes(p)
        values = act_ref[:, cols]
        step = stepx_ref[:, cols]
        ending = expx_ref[:, cols]
        end = read_state(end_ref, p)
        end_s = split(end)
        z = dot3(key_s, end_s, NN) * ending
        dx = scan_ref[:, cols] + z
        act_ref[:, cols] = dx * step + table_ref[6:7, cols] * ng_ref[:, cols]
        dstep_ref[...] += head_sum(dx * values, p)
        scaled = values * step
        zsum_ref[...] += head_sum(scaled * z, p)
        dk_ref[...] += dot3(split(scaled * ending), end_s, NT)
        both = end * read_state(ent_ref, p)
        ded_ref[...] += head_sum(jnp.sum(both.reshape(STATE // 8, 8, 128), axis=0), p)
        return carry

    lax.fori_loop(0, PAIRS, pair, 0, unroll=2)
    act_ref[:, INNER : INNER + STATE] = dk_ref[...]
    act_ref[:, INNER + STATE :] = dq_ref[...]
    dfilt_ref[0:8, :] = jnp.zeros((8, 128), F32)
    dfilt_ref[8 + TOKENS :, :] = jnp.zeros((8, 128), F32)

    def filters(j, carry):
        cols = lanes(j)
        f = filtered_of(x_ref, table_ref, ext_ref, halo_ref[:, cols], cols)
        s = sigmoid(f)
        dfilt = act_ref[:, cols] * (s * (1.0 + f * (1.0 - s)))
        dfilt_ref[8 : 8 + TOKENS, :] = dfilt
        dx = table_ref[TAPS - 1 : TAPS, cols] * dfilt
        lead = table_ref[0:1, cols] * dfilt_ref[8:16, :]
        for k in range(TAPS):
            at = EDGE - TAPS + 1 + k
            small_ref[j, k : k + 1, :] = jnp.sum(dfilt * ext_ref[at : at + TOKENS, :], axis=0, keepdims=True)
            if k < TAPS - 1:
                dx = dx + table_ref[k : k + 1, cols] * dfilt_ref[11 - k : 11 - k + TOKENS, :]
            if 0 < k < TAPS - 1:
                lead = lead + table_ref[k : k + 1, cols] * dfilt_ref[8 - k : 16 - k, :]
        small_ref[j, TAPS : TAPS + 1, :] = jnp.sum(dfilt, axis=0, keepdims=True)
        gin_ref[:, cols] = dx.astype(BF16)
        tail_ref[:, cols] = dx[TOKENS - EDGE :, :]
        ret_ref[:, cols] = lead
        return carry

    lax.fori_loop(0, CHANNELS // 128, filters, 0, unroll=2)
    returned = to_peer(ret_ref, rrecv, hsems.at[2], hsems.at[3], (before, dp))
    returned.start()
    zsum = zsum_ref[...]
    final = jnp.sum(zsum, axis=0, keepdims=True) + decays * jnp.sum(ded_ref[...], axis=0, keepdims=True)
    row = iota((TOKENS, 128), 0)
    dcum = dcum_ref[...] - zsum + jnp.where(row == TOKENS - 1, final, 0.0)
    shift = 1
    while shift < TOKENS:
        dcum = dcum + jnp.where(row < TOKENS - shift, pltpu.roll(dcum, TOKENS - shift, 0), 0.0)
        shift *= 2
    gain_t = turned(jnp.broadcast_to(gain, (HEADS, TOKENS)))
    draw = (dstep_ref[...] + dcum * gain_t) * turned(sigmoid(raw))
    gstep_ref[...] = jnp.transpose(draw)[:HEADS, :]
    tiles = CHANNELS // 128
    small_ref[tiles, 0:1, :] = jnp.sum(draw, axis=0, keepdims=True)
    small_ref[tiles, 1:2, :] = jnp.sum(dcum * turned(rates), axis=0, keepdims=True)
    small_ref[tiles, 2:3, :] = jnp.sum(dskip_ref[...], axis=0, keepdims=True)
    def pick(peer):
        return peer + (4 - 8 * lax.rem(peer // 4, 2)) * (dp // 2)

    narrow = Scatter(seq, dp, small_ref, srecv, sems, 14, pick=pick)
    narrow.start()

    spread.received()
    wacc[...] = jnp.zeros_like(wacc)

    def add(k, carry):
        wacc[...] += wrecv[k].astype(F32)
        return carry

    lax.fori_loop(0, SEQ, add, 0)
    x, y, z = seq // 8, lax.rem(seq // 4, 2), lax.rem(seq, 4)
    trees = [
        Tree(z, y, x, dp, lambda a, y, c: c * 8 + y * 4 + a, wall, tsems.at[0]),
        Tree(x, y, z, dp, lambda a, y, c: a * 8 + y * 4 + c, wall2, tsems.at[1]),
    ]
    wall[seq] = wacc[0:FIRST, :].astype(BF16)
    wall2[z * 8 + y * 4 + x] = wacc[FIRST:, :].astype(BF16)
    for tree in trees:
        tree.start(0)

    back2.sent()
    spread.sent()
    narrow.received()
    sdp[dp] = lax.fori_loop(0, SEQ, lambda k, total: total + srecv[k], jnp.zeros((8, 128), F32))

    others = ((seq, partner), (beside, across), (beside, corner))

    def exchange(k, slot):
        return to_peer(sdp.at[dp], sdp.at[slot], xsems.at[0, k], xsems.at[1, slot], others[k])

    for k in range(DP - 1):
        exchange(k, dp).start()
    for tree in trees:
        tree.received(0)
        tree.start(1)
    for k in range(DP - 1):
        exchange(k, others[k][1]).wait_recv()
    sown[...] = sdp[0] + sdp[1] + sdp[2] + sdp[3]
    narrow_all = Scatter(seq, dp, sown, sall, sems, 16, whole=True)
    narrow_all.start()
    for tree in trees:
        tree.received(1)
        tree.start(2)
    returned.wait_recv()
    fix = jnp.where(seq < SEQ - 1, rrecv[...], 0.0)
    zeros = jnp.zeros((EDGE - TAPS + 1, CHANNELS), F32)
    fix = jnp.concatenate([zeros, fix[: TAPS - 1, :]], axis=0)
    gin_ref[TOKENS - EDGE :, :] = (tail_ref[...] + fix).astype(BF16)
    narrow_all.received()
    for j in range(tiles):
        gfilt_ref[:, j * 128 : j * 128 + 128] = sall[pick(j), 0 : TAPS + 1, :]
    for p in range(PAIRS):
        gnorm_ref[p * 128 : p * 128 + 128] = sall[pick(p), 5, :]
    ghead_ref[...] = sall[pick(tiles), 0:3, 0:HEADS]
    for tree in trees:
        tree.received(2)
    for tree in trees:
        tree.sent()
    for copy in [halo, near, *cross, *relay, cot_near, cot_cross, cot_relay, *lows, returned]:
        copy.wait_send()
    for k in range(DP - 1):
        exchange(k, dp).wait_send()
    for scatter in (narrow, narrow_all):
        scatter.sent()


def part_of(walls, chunk, at):
    if at < FIRST:
        return walls[0][chunk, at : at + 16, :]
    x, y, z = chunk // 8, chunk // 4 % 2, chunk % 4
    return walls[1][z * 8 + y * 4 + x, at - FIRST : at - FIRST + 16, :]


def finish_kernel(*refs):
    half = len(refs) - 7
    for src, dst in zip(refs[:6], refs[half : half + 6]):
        dst[...] = src[...]
    walls, gweight_ref = refs[6:half], refs[-1]
    for j in range(WIDTH // 128):
        for c in range(ROWS // 16):
            chunk, at = divmod(j * ROWS + c * 16, PIECE)
            gweight_ref[c * 16 : c * 16 + 16, j * 128 : j * 128 + 128] = part_of(walls, chunk, at).astype(F32)


VMEM = pl.BlockSpec(memory_space=pltpu.VMEM)


def vmem(*shape, kind=F32):
    return pltpu.VMEM(shape, kind)


SENT = F32


def body(
    conv_input, gate_input, step_input, filter_taps, filter_bias, step_bias, decay_log, skip_gain, norm_weight,
    output_weight, output_grad,
):
    heads = jnp.stack([step_bias, decay_log, skip_gain])
    args = (conv_input[0], gate_input[0], filter_taps, filter_bias, norm_weight, heads, step_input[0], output_grad[0], output_weight)
    dma = pltpu.SemaphoreType.DMA
    wide, small, square = (TOKENS, INNER), (TOKENS, STATE), (TOKENS, TOKENS)
    states, pieces, tiles = (SEQ, BAND, SPREAD), (SEQ, PIECE, 128), (SEQ, 8, 128)
    scan = [vmem(*states, kind=SENT)] * 4
    walls = [((SEQ, FIRST, 128), BF16), ((SEQ, PIECE - FIRST, 128), BF16)]
    outs = [
        ((TOKENS, CHANNELS), BF16), (wide, BF16), ((HEADS, TOKENS), F32), ((TAPS + 1, CHANNELS), F32),
        ((INNER,), F32), ((3, HEADS), F32), *walls,
    ]
    results = pl.pallas_call(
        kernel,
        out_shape=[jax.ShapeDtypeStruct(shape, kind) for shape, kind in outs],
        in_specs=[VMEM] * len(args),
        out_specs=[VMEM] * len(outs),
        scratch_shapes=[
            vmem(8, CHANNELS), vmem(EDGE, CHANNELS, kind=BF16), vmem(EDGE, CHANNELS), vmem(TOKENS + EDGE, 128), vmem(TOKENS + 16, 128),
            vmem(TOKENS, CHANNELS), vmem(*wide), vmem(*wide), vmem(*wide), vmem(*wide),
            vmem(HEADS, TOKENS, 128), vmem(HEADS, 1, TOKENS), vmem(*square), vmem(*square), vmem(*square),
            *[vmem(*small)] * 4, vmem(8, 128), *[vmem(*small)] * 2, vmem(8, 128),
            vmem(*tiles), vmem(8, 128), vmem(SEQ, 1, SPREAD), *scan, *scan,
            vmem(DP - 1, ROWS, WIDTH, kind=BF16), vmem(DP, TOKENS, ROWS, kind=BF16),
            vmem(DP - 1, TOKENS, ROWS, kind=BF16), vmem(DP - 1, TOKENS, WIDTH, kind=BF16),
            *[vmem(*pieces, kind=BF16)] * 2, vmem(PIECE, 128),
            vmem(EDGE, CHANNELS), *[vmem(8, CHANNELS)] * 2, *[vmem(*tiles)] * 3, vmem(8, 128), vmem(DP, 8, 128),
            dma((18, SEQ)), dma((6, 4)), dma((4, DP - 1)), dma((4,)), dma((2, DP)), dma((2, 6, 4)),
        ],
        compiler_params=pltpu.CompilerParams(
            vmem_limit_bytes=63 * 2**20, collective_id=0, has_side_effects=True
        ),
        name="layer_backward",
    )(*args)
    finals = [*outs[:6], ((ROWS, WIDTH), F32)]
    gin, ggate, gstep, gfilt, gnorm, ghead, gweight = pl.pallas_call(
        finish_kernel,
        out_shape=[jax.ShapeDtypeStruct(shape, kind) for shape, kind in finals],
        in_specs=[VMEM] * len(outs),
        out_specs=[VMEM] * len(finals),
        compiler_params=pltpu.CompilerParams(vmem_limit_bytes=62 * 2**20),
        name="finish",
    )(*results)
    return gin[None], ggate[None], gstep[None], gweight, gfilt, gnorm, ghead


def solution(mesh):
    tokens, by_head, rows = P("dp", "seq", None), P("dp", None, "seq"), P("dp", None)
    return jax.shard_map(
        body,
        mesh=mesh,
        in_specs=(tokens, tokens, by_head, P(), P(), P(), P(), P(), P(), rows, tokens),
        out_specs=(tokens, tokens, by_head, rows, P(), P(), P()),
        check_vma=False,
    )
```

```python
import jax
import jax.numpy as jnp
from jax import lax
from jax.experimental import pallas as pl
from jax.experimental.pallas import tpu as pltpu
from jax.sharding import PartitionSpec as P

HEADS = 40
HEAD_DIM = 64
STATE = 128
INNER = 2560
CHANNELS = 2816
WIDTH = 1280
TOKENS = 256
TAPS = 4
PAIRS = 20
GROUPS = 4
EACH = PAIRS // GROUPS
SPREAD = INNER // GROUPS
BAND = 16
BANDS = STATE // BAND
SEQ = 32
DP = 4
ROWS = INNER // DP
EDGE = 16
FIRST = 112
PIECE = 208
MASKED = -1e30
EPSILON = 1e-05

F32 = jnp.float32
BF16 = jnp.bfloat16
MESH = pl.DeviceIdType.MESH
NN = ((1,), (0,))
NT = ((1,), (1,))
TN = ((0,), (0,))


def mm(a, b, dims):
    return lax.dot_general(a, b, (dims, ((), ())), preferred_element_type=F32)


def split(x):
    high = x.astype(BF16)
    return high, (x - high.astype(F32)).astype(BF16)


def dot3(a, b, dims):
    return mm(a[0], b[0], dims) + mm(a[0], b[1], dims) + mm(a[1], b[0], dims)


def iota(shape, dim):
    return lax.broadcasted_iota(jnp.int32, shape, dim)


def lanes(p):
    return pl.ds(pl.multiple_of(p * 128, 128), 128)


def turned(x):
    return jnp.transpose(jnp.concatenate([x, jnp.zeros((128 - HEADS, TOKENS), F32)], axis=0))


def rates_of(step_ref, heads_ref):
    columns = jnp.transpose(jnp.pad(heads_ref[...], ((0, 125), (0, 128 - HEADS))))
    raw = step_ref[...] + columns[:HEADS, 0:1]
    sizes = jnp.maximum(raw, 0.0) + jnp.log1p(jnp.exp(-jnp.abs(raw)))
    gain = -jnp.exp(columns[:HEADS, 1:2])
    rates = sizes * gain
    lane = iota(rates.shape, 1)
    cums = rates
    shift = 1
    while shift < TOKENS:
        cums = cums + jnp.where(lane >= shift, pltpu.roll(cums, shift, 1), 0.0)
        shift *= 2
    return raw, sizes, gain, rates, cums


def widen(columns, p):
    first = iota((TOKENS, 128), 1) < HEAD_DIM
    return jnp.where(first, columns[:, 2 * p : 2 * p + 1], columns[:, 2 * p + 1 : 2 * p + 2])


def head_sum(v, p):
    into = (iota((128, 128), 1) == 2 * p + iota((128, 128), 0) // HEAD_DIM).astype(BF16)
    high, low = split(v)
    return mm(high, into, NN) + mm(low, into, NN)


def sigmoid(x):
    return 1.0 / (1.0 + jnp.exp(-x))


def filtered_of(x_ref, table_ref, ext_ref, edge, cols, count=TOKENS):
    ext_ref[0:EDGE, :] = jnp.broadcast_to(edge, (EDGE, 128))
    ext_ref[EDGE : EDGE + count, :] = x_ref[0:count, cols].astype(F32)
    total = table_ref[TAPS : TAPS + 1, cols]
    for k in range(TAPS):
        at = EDGE - TAPS + 1 + k
        total = total + table_ref[k : k + 1, cols] * ext_ref[at : at + count, :]
    return total


def write_state(pay_ref, p, state):
    group = p // EACH
    at = lanes(p - group * EACH)
    for c in range(BANDS):
        pay_ref[group * BANDS + c, :, at] = state[c * BAND : c * BAND + BAND, :]


def read_state(ref, p):
    group = p // EACH
    at = lanes(p - group * EACH)
    return jnp.concatenate([ref[group * BANDS + c, :, at] for c in range(BANDS)], axis=0)


def to_peer(src, dst, send, recv, device):
    return pltpu.make_async_remote_copy(
        src_ref=src, dst_ref=dst, send_sem=send, recv_sem=recv, device_id=device, device_id_type=MESH
    )


def greet(seq, dp, others):
    barrier = pltpu.get_barrier_semaphore()

    def hello(i, carry):
        peer = lax.rem(seq + i, SEQ)
        pl.semaphore_signal(barrier, inc=1, device_id=(peer, dp), device_id_type=MESH)
        return carry

    lax.fori_loop(1, SEQ, hello, 0)
    for other in others:
        pl.semaphore_signal(barrier, inc=1, device_id=other, device_id_type=MESH)
    return lambda: pl.semaphore_wait(barrier, SEQ - 1 + len(others))


def each_peer(seq, act):
    def step(i, carry):
        act(i, lax.rem(seq + i, SEQ))
        return carry

    lax.fori_loop(1, SEQ, step, 0)


class Scatter:
    def __init__(self, seq, dp, src, dst, sems, row, whole=False, pick=lambda peer: peer):
        self.seq, self.dp, self.src, self.dst, self.sems, self.row = seq, dp, src, dst, sems, row
        self.whole, self.pick = whole, pick

    def copy(self, i, peer, slot):
        src = self.src if self.whole else self.src.at[self.pick(peer)]
        sems = self.sems
        return to_peer(src, self.dst.at[slot], sems.at[self.row, i], sems.at[self.row + 1, slot], (peer, self.dp))

    def keep(self):
        self.dst[self.seq] = self.src[...] if self.whole else self.src[self.pick(self.seq)]

    def start(self):
        each_peer(self.seq, lambda i, peer: self.copy(i, peer, self.seq).start())
        self.keep()

    def received(self):
        each_peer(self.seq, lambda i, peer: self.copy(i, peer, peer).wait_recv())

    def sent(self):
        each_peer(self.seq, lambda i, peer: self.copy(i, peer, self.seq).wait_send())

    def in_group(self, group, act):
        def step(c, carry):
            peer = group * BANDS + c

            @pl.when(peer != self.seq)
            def _():
                act(lax.rem(peer - self.seq + SEQ, SEQ), peer)

            return carry

        lax.fori_loop(0, BANDS, step, 0)

    def start_group(self, group):
        self.in_group(group, lambda i, peer: self.copy(i, peer, self.seq).start())

    def received_group(self, group):
        self.in_group(group, lambda i, peer: self.copy(i, peer, peer).wait_recv())


class Tree:
    def __init__(self, a, y, c, dp, device_of, buf, sems):
        self.a, self.y, self.c, self.dp, self.device_of, self.buf, self.sems = a, y, c, dp, device_of, buf, sems

    def copy(self, leg, k, arriving):
        a, y, c = self.a, self.y, self.c
        if leg == 0:
            other, mine = lax.rem(a + k, 4), a
            device, base, size = self.device_of(other, y, c), c * 8 + y * 4 + (other if arriving else mine), 1
        elif leg == 1:
            other, mine = 1 - y, y
            device, base, size = self.device_of(a, other, c), c * 8 + (other if arriving else mine) * 4, 4
        else:
            other, mine = lax.rem(c + k, 4), c
            device, base, size = self.device_of(a, y, other), (other if arriving else mine) * 8, 8
        part = self.buf.at[pl.ds(base, size)]
        recv = self.sems.at[2 * leg + 1, other if arriving else mine]
        return to_peer(part, part, self.sems.at[2 * leg, k], recv, (device, self.dp))

    def counts(self, leg):
        return (1,) if leg == 1 else (1, 2, 3)

    def start(self, leg):
        for k in self.counts(leg):
            self.copy(leg, k, False).start()

    def received(self, leg):
        for k in self.counts(leg):
            self.copy(leg, k, True).wait_recv()

    def sent(self):
        for leg in range(3):
            for k in self.counts(leg):
                self.copy(leg, k, False).wait_send()


class Fold:
    def __init__(self, a, y, c, dp, device_of, src, r0, s0, r1, s1, r2, sems):
        self.a, self.y, self.c, self.dp, self.device_of = a, y, c, dp, device_of
        self.src, self.r0, self.s0, self.r1, self.s1, self.r2, self.sems = src, r0, s0, r1, s1, r2, sems

    def copy(self, leg, k, arriving):
        a, y, c = self.a, self.y, self.c
        if leg == 0:
            other, mine = lax.rem(c + k, 4), c
            device, src, dst = self.device_of(a, y, other), self.src.at[pl.ds(other * 8, 8)], self.r0
            dst = dst.at[other if arriving else mine]
        elif leg == 1:
            other, mine = 1 - y, y
            device, src, dst = self.device_of(a, other, c), self.s0.at[pl.ds(other * 4, 4)], self.r1
        else:
            other, mine = lax.rem(a + k, 4), a
            device, src, dst = self.device_of(other, y, c), self.s1.at[other], self.r2
            dst = dst.at[other if arriving else mine]
        recv = self.sems.at[2 * leg + 1, other if arriving else mine]
        return to_peer(src, dst, self.sems.at[2 * leg, k], recv, (device, self.dp))

    def counts(self, leg):
        return (1,) if leg == 1 else (1, 2, 3)

    def start(self, leg):
        for k in self.counts(leg):
            self.copy(leg, k, False).start()

    def received(self, leg):
        for k in self.counts(leg):
            self.copy(leg, k, True).wait_recv()

    def first(self):
        self.received(0)
        c = self.c

        def add(i, carry):
            total = self.src[c * 8 + i].astype(F32)
            for k in (1, 2, 3):
                total = total + self.r0[lax.rem(c + k, 4), i].astype(F32)
            self.s0[i] = total
            return carry

        lax.fori_loop(0, 8, add, 0)
        self.start(1)

    def second(self):
        self.received(1)
        for i in range(4):
            self.s1[i] = self.s0[self.y * 4 + i] + self.r1[i]
        self.start(2)

    def third(self):
        self.received(2)
        total = self.s1[self.a]
        for k in (1, 2, 3):
            total = total + self.r2[lax.rem(self.a + k, 4)]
        return total

    def sent(self):
        for leg in range(3):
            for k in self.counts(leg):
                self.copy(leg, k, False).wait_send()


def coefficients(seq, drecv, coef):
    decays = jnp.concatenate([drecv[k, 0:1, :] for k in range(SEQ)], axis=0)
    head = (seq // BANDS) * (HEADS // GROUPS) + iota((128, SPREAD), 1) // HEAD_DIM
    into = (iota((128, SPREAD), 0) == head).astype(F32)
    wide = lax.dot_general(
        decays, into, (NN, ((), ())), preferred_element_type=F32, precision=lax.Precision.HIGHEST
    )
    for k in range(SEQ):
        coef[k] = wide[k : k + 1, :]


def scan_chunks(reverse, recv, outgoing, coef):
    def scan(j, state):
        k = SEQ - 1 - j if reverse else j
        outgoing[k] = state.astype(outgoing.dtype)
        return coef[k] * state + recv[k].astype(F32)

    lax.fori_loop(0, SEQ, scan, jnp.zeros((BAND, SPREAD), F32))


def turned_slot(chunk):
    return chunk % 4 * 8 + chunk // 4 % 2 * 4 + chunk // 8


def place_part(parts, chunk, at, value):
    if at < FIRST:
        parts[0][chunk, at : at + 16, :] = value
    else:
        parts[1][turned_slot(chunk), at - FIRST : at - FIRST + 16, :] = value


def part_of(parts, chunk, at):
    if at < FIRST:
        return parts[0][chunk, at : at + 16, :]
    return parts[1][turned_slot(chunk), at - FIRST : at - FIRST + 16, :]


def place():
    seq, dp = lax.axis_index("seq"), lax.axis_index("dp")
    partner = dp + 1 - 2 * lax.rem(dp, 2)
    across = lax.rem(dp + 2, DP)
    return seq, dp, partner, across


def kernel(
    x_ref, gate_ref, taps_ref, fbias_ref, weight_ref, heads_ref, step_ref, cot_ref, w_ref,
    gin_ref, ggate_ref, gstep_ref, gfilt_ref, gnorm_ref, ghead_ref, wall, wall2,
    table_ref, edge_ref, halo_ref, ext_ref, dfilt_ref, act_ref, scan_ref, ng_ref, stepx_ref, expx_ref, col_ref, cum_ref,
    scores_ref, turn_ref, dsc_ref, acc_ref, dq_ref, dk_ref, dcum_ref, dskip_ref, dstep_ref, zsum_ref, ded_ref,
    drecv, down_ref, coef, pay_ref, recv, outgoing, ent_ref, pay2_ref, recv2, outgoing2, end_ref,
    wblocks, low_ref, lrecv, crecv, part_ref, part2_ref, *rest,
):
    folding, rest = rest[:10], rest[10:]
    tail_ref, ret_ref, rrecv, small_ref, srecv, sall, sown, sdp, sems, wsems, dsems, hsems, xsems, tsems = rest
    parts = (part_ref, part2_ref)
    seq, dp, partner, across = place()
    corner = DP - 1 - dp
    beside = seq + 4 - 8 * lax.rem(seq // 4, 2)
    after, before = lax.rem(seq + 1, SEQ), lax.rem(seq + SEQ - 1, SEQ)
    met = greet(seq, dp, [(seq, partner), (seq, across), (seq, corner), (beside, across), (beside, corner)])
    table_ref[0:TAPS, :] = taps_ref[...]
    for j in range(CHANNELS // 128):
        table_ref[TAPS : TAPS + 1, j * 128 : j * 128 + 128] = fbias_ref[j * 128 : j * 128 + 128].reshape(1, 128)
    low_half = iota((1, 128), 1) < HEAD_DIM
    for p in range(PAIRS):
        at = slice(p * 128, p * 128 + 128)
        table_ref[5:6, at] = weight_ref[at].reshape(1, 128)
        skips = heads_ref[2:3, 2 * p : 2 * p + 2]
        table_ref[6:7, at] = jnp.where(low_half, skips[:, 0:1], skips[:, 1:2])
    raw, sizes, gain, rates, cums = rates_of(step_ref, heads_ref)
    cum_t = turned(cums)
    size_t = turned(sizes)
    decays = jnp.exp(cum_t[TOKENS - 1 :, :])
    down_ref[...] = jnp.broadcast_to(decays, (8, 128))
    met()
    last_rows = x_ref.at[pl.ds(TOKENS - EDGE, EDGE)]
    halo = to_peer(last_rows, edge_ref, hsems.at[0], hsems.at[1], (after, dp))
    halo.start()
    quarter = ROWS // 4

    def piece(q):
        return pl.ds(q * quarter, quarter)

    cross = [
        to_peer(w_ref.at[piece(q)], wblocks.at[1, piece(q)], wsems.at[0, q], wsems.at[1, q], (beside, across))
        for q in range(4)
    ]
    relay = [
        to_peer(wblocks.at[1, piece(q)], wblocks.at[2, piece(q)], wsems.at[2, q], wsems.at[3, q], (seq, partner))
        for q in range(4)
    ]
    near = to_peer(w_ref, wblocks.at[0], wsems.at[4, 0], wsems.at[5, 0], (seq, partner))
    for copy in cross:
        copy.start()
    near.start()
    decay_all = Scatter(seq, dp, down_ref, drecv, sems, 0, whole=True)
    decay_all.start()
    to_end = turned(jnp.exp(cums[:, TOKENS - 1 :] - cums))
    end_t = to_end * size_t

    def activate(j, carry):
        cols = lanes(j)
        f = filtered_of(x_ref, table_ref, ext_ref, 0.0, cols)
        act_ref[:, cols] = f * sigmoid(f)
        return carry

    def mend(j, carry):
        cols = lanes(j)
        f = filtered_of(x_ref, table_ref, ext_ref, halo_ref[:, cols], cols, EDGE)
        act_ref[0:EDGE, cols] = f * sigmoid(f)
        return carry

    lax.fori_loop(0, CHANNELS // 128, activate, 0, unroll=2)
    halo.wait_recv()
    halo_ref[...] = jnp.where(seq > 0, edge_ref[...].astype(F32), 0.0)
    lax.fori_loop(0, CHANNELS // 128, mend, 0, unroll=11)
    key = act_ref[:, INNER : INNER + STATE]
    key_turned = split(jnp.transpose(key))
    out = Scatter(seq, dp, pay_ref, recv, sems, 2)
    for p in range(PAIRS):
        a = act_ref[:, p * 128 : p * 128 + 128] * widen(end_t, p)
        write_state(pay_ref, p, dot3(key_turned, split(a), NN))
        if p % EACH == EACH - 1:
            out.start_group(p // EACH)
    out.keep()

    exp_t = jnp.exp(cum_t)
    for h in range(HEADS):
        cum_ref[h] = cums[h : h + 1, :]
        col_ref[h] = jnp.broadcast_to(cum_t[:, h : h + 1], (TOKENS, 128))
    for p in range(PAIRS):
        stepx_ref[:, p * 128 : p * 128 + 128] = widen(size_t, p)
        expx_ref[:, p * 128 : p * 128 + 128] = widen(exp_t, p)
    query = act_ref[:, INNER + STATE :]
    key_s, query_s = split(key), split(query)
    query_turned = split(jnp.transpose(query))
    scores_ref[...] = dot3(query_s, key_s, NT)
    first = iota((TOKENS, 128), 1) < HEAD_DIM
    rows, columns = iota((TOKENS, TOKENS), 0), iota((TOKENS, TOKENS), 1)

    def inside(p, carry):
        cols = lanes(p)
        high, low = split(act_ref[:, cols] * stepx_ref[:, cols])
        both = jnp.concatenate([high, low], axis=1)
        parts = []
        for i in range(2):
            h = 2 * p + i
            c = col_ref[h]
            e = jnp.exp(jnp.where(rows >= columns, jnp.concatenate([c, c], axis=1) - cum_ref[h], MASKED))
            wh, wl = split(scores_ref[...] * e)
            r = mm(wh, both, NN)
            parts.append(r[:, :128] + r[:, 128:] + mm(wl, high, NN))
        scan_ref[:, cols] = jnp.where(first, parts[0], parts[1])
        return carry

    def normed_grad(block, weights):
        at = pl.multiple_of(block * ROWS, 128)
        ng_ref[:, pl.ds(at, ROWS)] = mm(cot_ref[...], weights[...], NT)

    lax.fori_loop(0, PAIRS, inside, 0)
    normed_grad(dp, w_ref)
    decay_all.received()
    coefficients(seq, drecv, coef)
    out.received()
    scan_chunks(False, recv, outgoing, coef)
    back = Scatter(seq, dp, outgoing, ent_ref, sems, 4)
    back.start()
    near.wait_recv()
    normed_grad(partner, wblocks.at[0])
    for q in range(4):
        cross[q].wait_recv()
        relay[q].start()
    cot_near = to_peer(cot_ref, crecv.at[0], dsems.at[0, 0], dsems.at[1, 0], (seq, partner))
    cot_cross = to_peer(cot_ref, crecv.at[1], dsems.at[0, 1], dsems.at[1, 1], (beside, across))
    cot_relay = to_peer(crecv.at[1], crecv.at[2], dsems.at[0, 2], dsems.at[1, 2], (seq, partner))
    cot_near.start()
    cot_cross.start()
    normed_grad(across, wblocks.at[1])
    turn_ref[...] = dot3(key_s, query_s, NT)
    for copy in relay:
        copy.wait_recv()
    normed_grad(corner, wblocks.at[2])
    for ref in (acc_ref, dsc_ref, dq_ref, dcum_ref, dskip_ref, dstep_ref, zsum_ref, ded_ref, small_ref):
        ref[...] = jnp.zeros_like(ref)
    decay_all.sent()
    out.sent()

    def forward(p, carry):
        cols = lanes(p)
        carried = dot3(query_s, split(read_state(ent_ref, p)), NN) * expx_ref[:, cols]
        scanned = scan_ref[:, cols] + carried + table_ref[6:7, cols] * act_ref[:, cols]
        scan_ref[:, cols] = scanned
        gate = gate_ref[:, cols].astype(F32)
        gated = scanned * (gate * sigmoid(gate))
        acc_ref[...] += gated * gated
        return carry

    for turn in (0, 1, 3, 2):
        group = lax.rem(seq // BANDS + turn, GROUPS)
        back.received_group(group)
        lax.fori_loop(0, EACH, lambda i, carry: forward(group * EACH + i, carry), 0, unroll=EACH)
    inverse = lax.rsqrt(jnp.sum(acc_ref[...], axis=1, keepdims=True) / INNER + EPSILON)
    acc_ref[...] = jnp.zeros_like(acc_ref)

    def norm(p, carry):
        cols = lanes(p)
        gate = gate_ref[:, cols].astype(F32)
        gated = scan_ref[:, cols] * (gate * sigmoid(gate))
        weight = table_ref[5:6, cols]
        unit = gated * inverse
        block = p // 5
        low_ref[block, :, lanes(p - block * 5)] = (unit * weight).astype(BF16)
        ng = ng_ref[:, cols]
        small_ref[p, 5:6, :] = jnp.sum(ng * unit, axis=0, keepdims=True)
        acc_ref[...] += ng * weight * gated
        return carry

    lax.fori_loop(0, PAIRS, norm, 0, unroll=2)
    lows = [
        to_peer(low_ref.at[other], lrecv.at[k], dsems.at[2, k], dsems.at[3, k], (at, other))
        for k, (at, other) in enumerate(((seq, partner), (beside, across), (beside, corner)))
    ]
    for copy in lows:
        copy.start()
    lean = jnp.sum(acc_ref[...], axis=1, keepdims=True) * (inverse * inverse * inverse) / INNER

    def cotangents(p, carry):
        cols = lanes(p)
        gate = gate_ref[:, cols].astype(F32)
        sloped = sigmoid(gate)
        silu = gate * sloped
        scanned = scan_ref[:, cols]
        dgated = inverse * (ng_ref[:, cols] * table_ref[5:6, cols]) - scanned * silu * lean
        ggate_ref[:, cols] = (dgated * scanned * (sloped * (1.0 + gate * (1.0 - sloped)))).astype(BF16)
        dy = dgated * silu
        ng_ref[:, cols] = dy
        write_state(pay2_ref, p, dot3(query_turned, split(dy * expx_ref[:, cols]), NN))
        return carry

    out2 = Scatter(seq, dp, pay2_ref, recv2, sems, 6)
    for turn in (2, 1, 3, 0):
        group = lax.rem(seq // BANDS + turn, GROUPS)
        lax.fori_loop(0, EACH, lambda i, carry: cotangents(group * EACH + i, carry), 0, unroll=EACH)
        out2.start_group(group)
    out2.keep()

    def backward(p, carry):
        cols = lanes(p)
        dy = ng_ref[:, cols]
        dh, dl = split(dy)
        both = jnp.concatenate([dh, dl], axis=1)
        twice = jnp.concatenate([dh, dh], axis=1)
        values = act_ref[:, cols]
        scaled = values * stepx_ref[:, cols]
        parts = []
        for i in range(2):
            h = 2 * p + i
            c = col_ref[h]
            e = jnp.exp(jnp.where(columns >= rows, cum_ref[h] - jnp.concatenate([c, c], axis=1), MASKED))
            wh, wl = split(turn_ref[...] * e)
            r = mm(wh, both, NN)
            parts.append(r[:, :128] + r[:, 128:] + mm(wl, dh, NN))
            own = first if i == 0 else jnp.logical_not(first)
            xh, xl = split(jnp.where(own, scaled, 0.0))
            dw = mm(jnp.concatenate([xh, xl], axis=1), twice, NT) + mm(xh, dl, NT)
            dsc_ref[...] += dw * e
        dx = jnp.where(first, parts[0], parts[1])
        dq_ref[...] += dot3(split(dy * expx_ref[:, cols]), split(read_state(ent_ref, p)), NT)
        skipped = dy * values
        dcum_ref[...] += head_sum(dy * scan_ref[:, cols] - skipped * table_ref[6:7, cols] - scaled * dx, p)
        dskip_ref[...] += head_sum(jnp.sum(skipped.reshape(TOKENS // 8, 8, 128), axis=0), p)
        scan_ref[:, cols] = dx
        return carry

    lax.fori_loop(0, PAIRS, backward, 0)
    for p in range(PAIRS):
        expx_ref[:, p * 128 : p * 128 + 128] = widen(to_end, p)
    cot_cross.wait_recv()
    cot_relay.start()
    back.sent()
    out2.received()
    scan_chunks(True, recv2, outgoing2, coef)
    back2 = Scatter(seq, dp, outgoing2, end_ref, sems, 8)
    back2.start()
    dsc = dsc_ref[...]
    dk_ref[...] = dot3(split(dsc), query_s, NN)
    dq_ref[...] += dot3(split(jnp.transpose(dsc)), key_s, NN)
    cot_near.wait_recv()
    for copy in lows:
        copy.wait_recv()
    cot_relay.wait_recv()
    left = [jnp.transpose(block) for block in (low_ref[dp], lrecv[0], lrecv[1], lrecv[2])]
    right = [cot_ref, crecv.at[0], crecv.at[1], crecv.at[2]]
    for j in range(WIDTH // 256):
        total = mm(left[0], right[0][:, j * 256 : j * 256 + 256], NN)
        for k in range(1, DP):
            total = total + mm(left[k], right[k][:, j * 256 : j * 256 + 256], NN)
        for i in range(2):
            for c in range(ROWS // 16):
                chunk, at = divmod((2 * j + i) * ROWS + c * 16, PIECE)
                place_part(parts, chunk, at, total[c * 16 : c * 16 + 16, i * 128 : i * 128 + 128].astype(BF16))
    for c in range(10 * ROWS, SEQ * PIECE, 16):
        chunk, at = divmod(c, PIECE)
        place_part(parts, chunk, at, jnp.zeros((16, 128), BF16))
    x, y, z = seq // 8, lax.rem(seq // 4, 2), lax.rem(seq, 4)
    ways = (
        (z, y, x, dp, lambda a, y, c: c * 8 + y * 4 + a),
        (x, y, z, dp, lambda a, y, c: a * 8 + y * 4 + c),
    )
    folds = [Fold(*ways[i], parts[i], *folding[5 * i : 5 * i + 5], tsems.at[2 + i]) for i in range(2)]
    out2.sent()

    def pair(p, carry):
        cols = lanes(p)
        values = act_ref[:, cols]
        step = stepx_ref[:, cols]
        ending = expx_ref[:, cols]
        end = read_state(end_ref, p)
        end_s = split(end)
        z = dot3(key_s, end_s, NN) * ending
        dx = scan_ref[:, cols] + z
        act_ref[:, cols] = dx * step + table_ref[6:7, cols] * ng_ref[:, cols]
        dstep_ref[...] += head_sum(dx * values, p)
        scaled = values * step
        zsum_ref[...] += head_sum(scaled * z, p)
        dk_ref[...] += dot3(split(scaled * ending), end_s, NT)
        both = end * read_state(ent_ref, p)
        ded_ref[...] += head_sum(jnp.sum(both.reshape(STATE // 8, 8, 128), axis=0), p)
        return carry

    back2.received()
    for fold in folds:
        fold.start(0)
    lax.fori_loop(0, PAIRS, pair, 0, unroll=2)
    for fold in folds:
        fold.first()
    act_ref[:, INNER : INNER + STATE] = dk_ref[...]
    act_ref[:, INNER + STATE :] = dq_ref[...]
    dfilt_ref[0:8, :] = jnp.zeros((8, 128), F32)
    dfilt_ref[8 + TOKENS :, :] = jnp.zeros((8, 128), F32)

    def filters(j, carry):
        cols = lanes(j)
        f = filtered_of(x_ref, table_ref, ext_ref, halo_ref[:, cols], cols)
        s = sigmoid(f)
        dfilt = act_ref[:, cols] * (s * (1.0 + f * (1.0 - s)))
        dfilt_ref[8 : 8 + TOKENS, :] = dfilt
        dx = table_ref[TAPS - 1 : TAPS, cols] * dfilt
        lead = table_ref[0:1, cols] * dfilt_ref[8:16, :]
        for k in range(TAPS):
            at = EDGE - TAPS + 1 + k
            small_ref[j, k : k + 1, :] = jnp.sum(dfilt * ext_ref[at : at + TOKENS, :], axis=0, keepdims=True)
            if k < TAPS - 1:
                dx = dx + table_ref[k : k + 1, cols] * dfilt_ref[11 - k : 11 - k + TOKENS, :]
            if 0 < k < TAPS - 1:
                lead = lead + table_ref[k : k + 1, cols] * dfilt_ref[8 - k : 16 - k, :]
        small_ref[j, TAPS : TAPS + 1, :] = jnp.sum(dfilt, axis=0, keepdims=True)
        gin_ref[:, cols] = dx.astype(BF16)
        tail_ref[:, cols] = dx[TOKENS - EDGE :, :]
        ret_ref[:, cols] = lead
        return carry

    lax.fori_loop(0, CHANNELS // 128, filters, 0, unroll=2)
    returned = to_peer(ret_ref, rrecv, hsems.at[2], hsems.at[3], (before, dp))
    returned.start()
    for fold in folds:
        fold.second()
    zsum = zsum_ref[...]
    final = jnp.sum(zsum, axis=0, keepdims=True) + decays * jnp.sum(ded_ref[...], axis=0, keepdims=True)
    row = iota((TOKENS, 128), 0)
    dcum = dcum_ref[...] - zsum + jnp.where(row == TOKENS - 1, final, 0.0)
    shift = 1
    while shift < TOKENS:
        dcum = dcum + jnp.where(row < TOKENS - shift, pltpu.roll(dcum, TOKENS - shift, 0), 0.0)
        shift *= 2
    gain_t = turned(jnp.broadcast_to(gain, (HEADS, TOKENS)))
    draw = (dstep_ref[...] + dcum * gain_t) * turned(sigmoid(raw))
    gstep_ref[...] = jnp.transpose(draw)[:HEADS, :]
    tiles = CHANNELS // 128
    small_ref[tiles, 0:1, :] = jnp.sum(draw, axis=0, keepdims=True)
    small_ref[tiles, 1:2, :] = jnp.sum(dcum * turned(rates), axis=0, keepdims=True)
    small_ref[tiles, 2:3, :] = jnp.sum(dskip_ref[...], axis=0, keepdims=True)
    def pick(peer):
        return peer + (4 - 8 * lax.rem(peer // 4, 2)) * (dp // 2)

    narrow = Scatter(seq, dp, small_ref, srecv, sems, 14, pick=pick)
    narrow.start()

    trees = [Tree(*ways[i], (wall, wall2)[i], tsems.at[i]) for i in range(2)]
    wall[seq] = folds[0].third().astype(BF16)
    wall2[z * 8 + y * 4 + x] = folds[1].third().astype(BF16)
    for tree in trees:
        tree.start(0)

    back2.sent()
    for fold in folds:
        fold.sent()
    narrow.received()
    sdp[dp] = lax.fori_loop(0, SEQ, lambda k, total: total + srecv[k], jnp.zeros((8, 128), F32))

    others = ((seq, partner), (beside, across), (beside, corner))

    def exchange(k, slot):
        return to_peer(sdp.at[dp], sdp.at[slot], xsems.at[0, k], xsems.at[1, slot], others[k])

    for k in range(DP - 1):
        exchange(k, dp).start()
    for tree in trees:
        tree.received(0)
        tree.start(1)
    for k in range(DP - 1):
        exchange(k, others[k][1]).wait_recv()
    sown[...] = sdp[0] + sdp[1] + sdp[2] + sdp[3]
    narrow_all = Scatter(seq, dp, sown, sall, sems, 16, whole=True)
    narrow_all.start()
    for tree in trees:
        tree.received(1)
        tree.start(2)
    returned.wait_recv()
    fix = jnp.where(seq < SEQ - 1, rrecv[...], 0.0)
    zeros = jnp.zeros((EDGE - TAPS + 1, CHANNELS), F32)
    fix = jnp.concatenate([zeros, fix[: TAPS - 1, :]], axis=0)
    gin_ref[TOKENS - EDGE :, :] = (tail_ref[...] + fix).astype(BF16)
    narrow_all.received()
    for j in range(tiles):
        gfilt_ref[:, j * 128 : j * 128 + 128] = sall[pick(j), 0 : TAPS + 1, :]
    for p in range(PAIRS):
        gnorm_ref[p * 128 : p * 128 + 128] = sall[pick(p), 5, :]
    ghead_ref[...] = sall[pick(tiles), 0:3, 0:HEADS]
    for tree in trees:
        tree.received(2)
    for tree in trees:
        tree.sent()
    for copy in [halo, near, *cross, *relay, cot_near, cot_cross, cot_relay, *lows, returned]:
        copy.wait_send()
    for k in range(DP - 1):
        exchange(k, dp).wait_send()
    for scatter in (narrow, narrow_all):
        scatter.sent()


def finish_kernel(*refs):
    half = len(refs) - 7
    for src, dst in zip(refs[:6], refs[half : half + 6]):
        dst[...] = src[...]
    walls, gweight_ref = refs[6:half], refs[-1]
    for j in range(WIDTH // 128):
        for c in range(ROWS // 16):
            chunk, at = divmod(j * ROWS + c * 16, PIECE)
            gweight_ref[c * 16 : c * 16 + 16, j * 128 : j * 128 + 128] = part_of(walls, chunk, at).astype(F32)


VMEM = pl.BlockSpec(memory_space=pltpu.VMEM)


def vmem(*shape, kind=F32):
    return pltpu.VMEM(shape, kind)


SENT = F32


def body(
    conv_input, gate_input, step_input, filter_taps, filter_bias, step_bias, decay_log, skip_gain, norm_weight,
    output_weight, output_grad,
):
    heads = jnp.stack([step_bias, decay_log, skip_gain])
    args = (conv_input[0], gate_input[0], filter_taps, filter_bias, norm_weight, heads, step_input[0], output_grad[0], output_weight)
    dma = pltpu.SemaphoreType.DMA
    wide, small, square = (TOKENS, INNER), (TOKENS, STATE), (TOKENS, TOKENS)
    states, tiles = (SEQ, BAND, SPREAD), (SEQ, 8, 128)
    scan = [vmem(*states, kind=SENT)] * 4
    walls = [((SEQ, FIRST, 128), BF16), ((SEQ, PIECE - FIRST, 128), BF16)]
    halves = [vmem(*shape, kind=kind) for shape, kind in walls]

    def folding(n):
        return [vmem(4, 8, n, 128, kind=BF16), vmem(8, n, 128), *[vmem(4, n, 128)] * 3]

    outs = [
        ((TOKENS, CHANNELS), BF16), (wide, BF16), ((HEADS, TOKENS), F32), ((TAPS + 1, CHANNELS), F32),
        ((INNER,), F32), ((3, HEADS), F32), *walls,
    ]
    results = pl.pallas_call(
        kernel,
        out_shape=[jax.ShapeDtypeStruct(shape, kind) for shape, kind in outs],
        in_specs=[VMEM] * len(args),
        out_specs=[VMEM] * len(outs),
        scratch_shapes=[
            vmem(8, CHANNELS), vmem(EDGE, CHANNELS, kind=BF16), vmem(EDGE, CHANNELS), vmem(TOKENS + EDGE, 128), vmem(TOKENS + 16, 128),
            vmem(TOKENS, CHANNELS), vmem(*wide), vmem(*wide), vmem(*wide), vmem(*wide),
            vmem(HEADS, TOKENS, 128), vmem(HEADS, 1, TOKENS), vmem(*square), vmem(*square), vmem(*square),
            *[vmem(*small)] * 4, vmem(8, 128), *[vmem(*small)] * 2, vmem(8, 128),
            vmem(*tiles), vmem(8, 128), vmem(SEQ, 1, SPREAD), *scan, *scan,
            vmem(DP - 1, ROWS, WIDTH, kind=BF16), vmem(DP, TOKENS, ROWS, kind=BF16),
            vmem(DP - 1, TOKENS, ROWS, kind=BF16), vmem(DP - 1, TOKENS, WIDTH, kind=BF16),
            *halves, *folding(FIRST), *folding(PIECE - FIRST),
            vmem(EDGE, CHANNELS), *[vmem(8, CHANNELS)] * 2, *[vmem(*tiles)] * 3, vmem(8, 128), vmem(DP, 8, 128),
            dma((18, SEQ)), dma((6, 4)), dma((4, DP - 1)), dma((4,)), dma((2, DP)), dma((4, 6, 4)),
        ],
        compiler_params=pltpu.CompilerParams(
            vmem_limit_bytes=63 * 2**20, collective_id=0, has_side_effects=True
        ),
        name="layer_backward",
    )(*args)
    finals = [*outs[:6], ((ROWS, WIDTH), F32)]
    gin, ggate, gstep, gfilt, gnorm, ghead, gweight = pl.pallas_call(
        finish_kernel,
        out_shape=[jax.ShapeDtypeStruct(shape, kind) for shape, kind in finals],
        in_specs=[VMEM] * len(outs),
        out_specs=[VMEM] * len(finals),
        compiler_params=pltpu.CompilerParams(vmem_limit_bytes=62 * 2**20),
        name="finish",
    )(*results)
    return gin[None], ggate[None], gstep[None], gweight, gfilt, gnorm, ghead


def solution(mesh):
    tokens, by_head, rows = P("dp", "seq", None), P("dp", None, "seq"), P("dp", None)
    return jax.shard_map(
        body,
        mesh=mesh,
        in_specs=(tokens, tokens, by_head, P(), P(), P(), P(), P(), P(), rows, tokens),
        out_specs=(tokens, tokens, by_head, rows, P(), P(), P()),
        check_vma=False,
    )
```
